128 devices in a mesh: src: 16 (over z, x), rcv: 8 (over y, core).
Axes of the slice: x: 4, y: 4, z: 4, core: 2. Of those that a mesh axis runs over, the one named last changes fastest.
Arguments:
- traces: bfloat16 [2, 2, 2048, 2048], P(None, None, 'src', 'rcv'), may hold values from -8 to 8
- wavelet: float32 [2, 2], replicated, may hold values from -0.3 to 0.3
Outputs:
- coeffs: float32 [2, 2, 2048, 2048], P(None, None, 'src', 'rcv')
- norms: float32 [2, 2], replicated
The draws below stay inside these ranges and needn't reach their ends.
All inputs are finite; a program needn't handle non-finite values.
Results may differ from the reference program's by a relative error of at most 0.006.
Values may be sent and summed in bfloat16 or wider, within the bound.
A program may use at most 128 MiB of HBM per device.

```python
import math
import jax
import jax.numpy as jnp
from jax import lax

N = 2048
NF = 2
ITERS = 2


def draw_traces(key, part):
    values = jax.random.normal(jax.random.fold_in(key, 11), (NF, 2, N, N), jnp.float32)
    position = jnp.arange(N, dtype=jnp.float32) / N
    trend = jnp.exp(-math.log(4.0) * position)[None, None, :, None]
    values = values * trend * 1.3
    return jnp.clip(values, -8.0, 8.0).astype(jnp.bfloat16)


def setup_inputs(seed: int = 0) -> dict:
    seeds = jax.random.split(jax.random.key(seed), 3)
    traces = draw_traces(jax.random.fold_in(seeds[2], 71), 0)
    wavelet = jnp.clip(jax.random.uniform(seeds[1], (NF, 2), jnp.float32, -0.3, 0.3), -0.3, 0.3)
    return dict(traces=traces, wavelet=wavelet)


step_length = 0.4
shrink_fraction = 0.2

def table_block(offset, height, second, breadth, length, direction):
    left_index = offset + jnp.arange(height, dtype=jnp.int32)
    right_index = second + jnp.arange(breadth, dtype=jnp.int32)
    phase = left_index[:, None] * right_index[None, :] % length
    angle = phase.astype(jnp.float32) * (2.0 * math.pi / length)
    scale = 1.0 / math.sqrt(length)
    return jnp.stack([jnp.cos(angle) * scale, direction * (jnp.sin(angle) * scale)]).astype(jnp.bfloat16)

def rounded(values):
    return lax.optimization_barrier(values.astype(jnp.bfloat16)).astype(jnp.float32)

def matmul_high(left_side, right_side):
    return jnp.matmul(left_side, right_side, precision=lax.Precision.HIGHEST)

def complex_matmul(left_side, right_side):
    left_re = left_side[..., 0, :, :]
    left_im = left_side[..., 1, :, :]
    right_re = right_side[..., 0, :, :]
    right_im = right_side[..., 1, :, :]
    real_part = matmul_high(left_re, right_re) - matmul_high(left_im, right_im)
    imag_part = matmul_high(left_re, right_im) + matmul_high(left_im, right_re)
    return jnp.stack([real_part, imag_part], axis=-3)

def complex_scale(real_part, imag_part, values):
    return jnp.stack([real_part * values[:, 0] - imag_part * values[:, 1], real_part * values[:, 1] + imag_part * values[:, 0]], axis=1)

def reference(traces, wavelet):
    extent = traces.shape[-1]
    forward = table_block(0, extent, 0, extent, extent, -1.0).astype(jnp.float32)
    inverse = table_block(0, extent, 0, extent, extent, 1.0).astype(jnp.float32)
    traces_f = traces.astype(jnp.float32)
    root_scale = 1.0 / math.sqrt(extent)
    wave_re = (wavelet[:, 0] * root_scale)[:, None, None]
    wave_im = (wavelet[:, 1] * root_scale)[:, None, None]
    traces_adj = jnp.stack([jnp.swapaxes(traces_f[:, 0], 1, 2), -jnp.swapaxes(traces_f[:, 1], 1, 2)], axis=1)
    coeffs = jnp.zeros(traces_f.shape, jnp.float32)
    norm_list = []
    for iteration in range(ITERS):
        if iteration == 0:
            misfit = traces_f
        else:
            halfway = rounded(complex_matmul(inverse, rounded(coeffs)))
            model = rounded(complex_matmul(halfway, inverse))
            product = complex_matmul(model, traces_f)
            misfit = traces_f - model + complex_scale(wave_re, wave_im, product)
        norm_list.append(jnp.sqrt(lax.optimization_barrier(jnp.sum(misfit * misfit, axis=(1, 2, 3)))))
        misfit_half = rounded(misfit)
        back_term = complex_matmul(misfit_half, traces_adj)
        gradient = misfit_half - complex_scale(wave_re, -wave_im, back_term)
        transformed = rounded(complex_matmul(rounded(gradient), forward))
        spectrum = complex_matmul(forward, transformed)
        trial = coeffs + step_length * spectrum
        magnitude = jnp.sqrt(trial[:, 0] * trial[:, 0] + trial[:, 1] * trial[:, 1])
        level = shrink_fraction * lax.optimization_barrier(jnp.max(magnitude, axis=(1, 2)))[:, None, None]
        factor = jnp.maximum(1.0 - level / jnp.maximum(magnitude, level), 0.0)
        coeffs = trial * factor[:, None]
    return (coeffs, jnp.stack(norm_list))
```

```python
import functools
import math

import jax
import jax.numpy as jnp
import numpy as np
from jax import lax
from jax.experimental import pallas as pl
from jax.experimental.pallas import tpu as pltpu
from jax.sharding import PartitionSpec as P

MESH = pl.DeviceIdType.MESH
N = 2048
BASE = 64
STEP = 0.4
SHRINK = 0.2
BF = jnp.bfloat16
F32 = jnp.float32


def table_parts():
    cols = np.arange(N)
    low = 2.0 * math.pi * ((np.arange(BASE)[:, None] * cols[None, :]) % N) / N
    high = 2.0 * math.pi * ((np.arange(0, N, BASE)[:, None] * cols[None, :]) % N) / N
    scale = 1.0 / math.sqrt(N)
    parts = (np.cos(low) * scale, np.sin(low) * scale, np.cos(high), np.sin(high))
    return [a.astype(np.float32) for a in parts]


def kernel(
    tr, wave, base_c, base_s, mul_c, mul_s, out, norms,
    tf, tab_c, tab_s, pg, sb, ra, rb, qa, qb, dl, dr, gb, yb, zz, zt, xt,
    trial, coef, cfo, cb, hb, wt, hh, mb, mf, ot, st1, st2, sr1, sr2, nt, nr,
    ssem, rsem,
):
    p = lax.axis_index("src")
    rcv = lax.axis_index("rcv")
    y = rcv // 2
    c = rcv % 2
    z = p // 4
    x = p % 4
    used = [0]
    pending = []

    def ids(n):
        used[0] += n
        return used[0] - n

    def dev(pp, yy, cc):
        return (pp, yy * 2 + cc)

    def rcopy(src, dst, s_id, r_id, where):
        return pltpu.make_async_remote_copy(
            src_ref=src, dst_ref=dst, send_sem=ssem.at[s_id], recv_sem=rsem.at[r_id],
            device_id=where, device_id_type=MESH,
        )

    def send(src, dst, s_id, where):
        copy = rcopy(src, dst, s_id, s_id, where)
        copy.start()
        pending.append(copy)

    def arrived(ref, r_id):
        rcopy(ref, ref, r_id, r_id, dev(p, y, 1 - c)).wait_recv()

    def sent():
        for copy in pending:
            copy.wait_send()
        pending.clear()

    def ds(start, size, unit):
        return pl.ds(pl.multiple_of(start, unit), size)

    barrier = pltpu.get_barrier_semaphore()
    me = p * 2 + c

    @pl.loop(1, 32)
    def _(k):
        other = (me + k) % 32
        pl.semaphore_signal(
            barrier, inc=1, device_id=dev(other // 2, y, other % 2), device_id_type=MESH
        )

    for d in (1, 2, 3):
        pl.semaphore_signal(
            barrier, inc=1, device_id=dev(p, (y + d) % 4, c), device_id_type=MESH
        )
    pl.semaphore_wait(barrier, 34)

    own_rows = ds(128 * p, 128, 128)
    swap = []
    for part in range(2):
        s_id = ids(1)
        where = tf.at[own_rows, ds(part * 512 + 256 * c, 256, 256)]
        send(tr.at[1 - c, part], where, s_id, dev(p, y, 1 - c))
        swap.append(s_id)
    for part in range(2):
        tf[own_rows, ds(part * 512 + 256 * c, 256, 256)] = tr[c, part]
    for part in range(2):
        arrived(tf.at[own_rows, ds(part * 512 + 256 * (1 - c), 256, 256)], swap[part])

    def shift(at, axis, d):
        zz_, xx_ = at
        return ((zz_ + d) % 4, xx_) if axis == 0 else (zz_, (xx_ + d) % 4)

    def neighbour(axis, d):
        a, b = shift((z, x), axis, d)
        return dev(a * 4 + b, y, c)

    def block(at, half, quarter=None):
        start = (at[0] * 4 + at[1]) * 128 + 64 * half
        if quarter is None:
            return tf.at[ds(start, 64, 32), :]
        return tf.at[ds(start + 32 * quarter, 32, 32), :]

    def ag_start(at, axis, half):
        s_id = ids(4)
        send(block(at, half), block(at, half), s_id, neighbour(axis, 1))
        send(block(at, half), block(at, half), s_id + 1, neighbour(axis, -1))
        return at, axis, half, s_id

    def ag_forward(item):
        at, axis, half, s_id = item
        left, right = shift(at, axis, -1), shift(at, axis, 1)
        arrived(block(left, half), s_id)
        send(block(left, half, 0), block(left, half, 0), s_id + 2, neighbour(axis, 1))
        arrived(block(right, half), s_id + 1)
        send(block(right, half, 1), block(right, half, 1), s_id + 3, neighbour(axis, -1))

    def ag_finish(item):
        at, axis, half, s_id = item
        far = shift(at, axis, 2)
        arrived(block(far, half, 0), s_id + 2)
        arrived(block(far, half, 1), s_id + 3)

    def make_table(first, last):
        @pl.loop(first, last)
        def _(m):
            for col in range(0, N, 512):
                here = pl.ds(col, 512)
                bc, bs = base_c[:, here], base_s[:, here]
                mc, ms = mul_c[pl.ds(m, 1), here], mul_s[pl.ds(m, 1), here]
                rows = ds(m * BASE, BASE, BASE)
                tab_c[rows, here] = (bc * mc - bs * ms).astype(BF)
                tab_s[rows, here] = (bs * mc + bc * ms).astype(BF)

    home = (z, x)
    first_x = ag_start(home, 1, 0)
    first_z = ag_start(home, 0, 1)
    second = [ag_start(home, 0, 0), ag_start(home, 1, 1)]
    make_table(0, 24)
    ag_forward(first_x)
    ag_forward(first_z)
    for d in (-1, 1):
        second.append(ag_start(shift(home, 1, d), 0, 0))
        second.append(ag_start(shift(home, 0, d), 1, 1))
    make_table(24, 32)
    ag_forward(second[0])
    ag_forward(second[1])
    ag_finish(first_x)
    ag_finish(first_z)
    second.append(ag_start(shift(home, 1, 2), 0, 0))
    second.append(ag_start(shift(home, 0, 2), 1, 1))
    for item in second[2:]:
        ag_forward(item)
    for item in second:
        ag_finish(item)

    root = 1.0 / math.sqrt(N)
    wr = wave[c, 0] * root
    wi = wave[c, 1] * root

    def dot(a, b):
        return lax.dot_general(a, b, (((1,), (0,)), ((), ())), preferred_element_type=F32)

    def dot_nt(a, b):
        return lax.dot_general(a, b, (((1,), (1,)), ((), ())), preferred_element_type=F32)

    def transform(rows_ref, half, sign, col):
        rows = rows_ref[...].reshape(2 * half, N)
        a = dot(rows, tab_c[:, ds(col, 256, 256)])
        b = dot(rows, tab_s[:, ds(col, 256, 256)])
        if sign > 0:
            return a[:half] + b[half:], a[half:] - b[:half]
        return a[:half] - b[half:], a[half:] + b[:half]

    def plane_exchange(source, landing, first_id):
        @pl.loop(1, 16)
        def _(k):
            q = (p + k) % 16
            rcopy(source(q), landing(p), first_id + k, first_id + k, dev(q, y, c)).start()

    def plane_wait(source, landing, first_id):
        @pl.loop(1, 16)
        def _(k):
            q = (p + 16 - k) % 16
            w = rcopy(source((p + k) % 16), landing(q), first_id + k, first_id + k, dev(q, y, c))
            w.wait_recv()
            w.wait_send()

    totals = []
    for it in range(2):
        if it == 0:
            re = tf[own_rows, 0:512]
            im = tf[own_rows, 512:1024]
            mf[0] = re
            mf[1] = im
            ref, imf = re.astype(F32), im.astype(F32)
            squares = jnp.sum(ref * ref + imf * imf)
        else:
            @pl.loop(0, 8)
            def _(n):
                a, b = transform(cb, 32, -1, n * 256)
                hb[0, :, ds(n * 256, 256, 256)] = a.astype(BF)
                hb[1, :, ds(n * 256, 256, 256)] = b.astype(BF)

            wid = ids(16)
            src_of = lambda q: hb.at[:, :, ds(128 * q, 128, 128)]
            dst_of = lambda q: wt.at[:, ds(32 * q, 32, 32), :]
            plane_exchange(src_of, dst_of, wid)
            wt[:, ds(32 * p, 32, 32), :] = hb[:, :, ds(128 * p, 128, 128)]
            plane_wait(src_of, dst_of, wid)
            for part in range(2):
                hh[part, :, ds(512 * y, 512, 512)] = wt[part].astype(F32).T.astype(BF)
            gid = ids(4)

            def col_block(yy, rows=None):
                if rows is None:
                    return hh.at[:, :, ds(512 * yy, 512, 512)]
                return hh.at[:, pl.ds(64 * rows, 64), ds(512 * yy, 512, 512)]

            up, down, far = (y + 1) % 4, (y + 3) % 4, (y + 2) % 4
            send(col_block(y), col_block(y), gid, dev(p, up, c))
            send(col_block(y), col_block(y), gid + 1, dev(p, down, c))
            arrived(col_block(down), gid)
            send(col_block(down, 0), col_block(down, 0), gid + 2, dev(p, up, c))
            arrived(col_block(up), gid + 1)
            send(col_block(up, 1), col_block(up, 1), gid + 3, dev(p, down, c))
            arrived(col_block(far, 0), gid + 2)
            arrived(col_block(far, 1), gid + 3)

            @pl.loop(0, 8)
            def _(n):
                a, b = transform(hh, 128, -1, n * 256)
                mb[0, :, ds(n * 256, 256, 256)] = a.astype(BF)
                mb[1, :, ds(n * 256, 256, 256)] = b.astype(BF)

            squares = 0.0
            for n in range(2):
                rows = mb[...].reshape(256, N)
                a = dot(rows, tf[:, n * 256 : n * 256 + 256])
                b = dot(rows, tf[:, 512 + n * 256 : 768 + n * 256])
                pr, pi = a[:128] - b[128:], b[:128] + a[128:]
                here = ds(512 * y + n * 256, 256, 256)
                mr = tf[own_rows, n * 256 : n * 256 + 256].astype(F32) - mb[0, :, here].astype(F32)
                mi = tf[own_rows, 512 + n * 256 : 768 + n * 256].astype(F32) - mb[1, :, here].astype(F32)
                mr = mr + (wr * pr - wi * pi)
                mi = mi + (wr * pi + wi * pr)
                squares = squares + jnp.sum(mr * mr + mi * mi)
                mf[0, :, n * 256 : n * 256 + 256] = mr.astype(BF)
                mf[1, :, n * 256 : n * 256 + 256] = mi.astype(BF)

        @pl.loop(0, 8)
        def _(n):
            rows = mf[...].reshape(256, 512)
            here = ds(n * 256, 256, 256)
            a = dot_nt(rows, tf[here, 0:512])
            b = dot_nt(rows, tf[here, 512:1024])
            br, bi = a[:128] + b[128:], a[128:] - b[:128]
            pg[0, :, here] = -(wr * br + wi * bi)
            pg[1, :, here] = -(wr * bi - wi * br)

        mine = ds(512 * y, 512, 512)
        pg[:, :, mine] = pg[:, :, mine] + mf[...].astype(F32)

        up, down, far = (y + 1) % 4, (y + 3) % 4, (y + 2) % 4
        lo, hi = pl.ds(0, 1024), pl.ds(1024, 1024)
        rows_of = lambda yy: ds(32 * yy, 32, 32)
        sb[it] = pg[...].astype(BF)
        sbi = sb.at[it]
        rid = ids(6)
        send(sbi.at[:, rows_of(far), lo], ra.at[it], rid, dev(p, up, c))
        send(sbi.at[:, rows_of(far), hi], rb.at[it], rid + 1, dev(p, down, c))
        send(sbi.at[:, rows_of(up), hi], dl.at[it, :, :, hi], rid + 2, dev(p, up, c))
        send(sbi.at[:, rows_of(down), lo], dr.at[it, :, :, lo], rid + 3, dev(p, down, c))
        arrived(ra.at[it], rid)
        qa[it] = (pg[:, rows_of(up), lo] + ra[it].astype(F32)).astype(BF)
        send(qa.at[it], dl.at[it, :, :, lo], rid + 4, dev(p, up, c))
        arrived(rb.at[it], rid + 1)
        qb[it] = (pg[:, rows_of(down), hi] + rb[it].astype(F32)).astype(BF)
        send(qb.at[it], dr.at[it, :, :, hi], rid + 5, dev(p, down, c))
        arrived(dl.at[it, :, :, hi], rid + 2)
        arrived(dr.at[it, :, :, lo], rid + 3)
        arrived(dl.at[it, :, :, lo], rid + 4)
        arrived(dr.at[it, :, :, hi], rid + 5)
        gb[...] = (pg[:, rows_of(y), :] + dl[it].astype(F32) + dr[it].astype(F32)).astype(BF)

        yid = ids(4)
        for d in (2, 1, 3, 0):
            yy = (y + d) % 4

            @pl.loop(0, 2)
            def _(n):
                a, b = transform(gb, 32, 1, yy * 512 + n * 256)
                yb[it, 0, :, ds(yy * 512 + n * 256, 256, 256)] = a.astype(BF)
                yb[it, 1, :, ds(yy * 512 + n * 256, 256, 256)] = b.astype(BF)

            if d:
                send(
                    yb.at[it, :, :, ds(512 * yy, 512, 512)],
                    zz.at[it, :, rows_of(y), :], yid + d, dev(p, yy, c),
                )
            else:
                zz[it, :, rows_of(y), :] = yb[it, :, :, ds(512 * yy, 512, 512)]
        for d in (1, 3, 2):
            arrived(zz.at[it, :, rows_of((y + 4 - d) % 4), :], yid + d)
        for part in range(2):
            zt[it, part] = zz[it, part].astype(F32).T.astype(BF)
        xid = ids(16)
        src_of = lambda q: zt.at[it, :, ds(32 * q, 32, 32), :]
        dst_of = lambda q: xt.at[it, :, :, ds(128 * q, 128, 128)]
        plane_exchange(src_of, dst_of, xid)
        xt[it, :, :, ds(128 * p, 128, 128)] = zt[it, :, ds(32 * p, 32, 32), :]
        plane_wait(src_of, dst_of, xid)

        def column_step(n, peak):
            here = ds(n * 256, 256, 256)
            a, b = transform(xt.at[it], 32, 1, n * 256)
            a, b = STEP * a, STEP * b
            if it:
                a, b = coef[0, :, here] + a, coef[1, :, here] + b
            trial[0, :, here] = a
            trial[1, :, here] = b
            return jnp.maximum(peak, jnp.sqrt(a * a + b * b))

        peak = jnp.max(lax.fori_loop(0, 8, column_step, jnp.zeros((32, 256), F32)))

        st1[it, 0] = jnp.full((8, 128), peak, F32)
        st1[it, 1] = jnp.full((8, 128), squares, F32)
        sid = ids(16)
        src_of = lambda q: st1.at[it]
        dst_of = lambda q: sr1.at[it, q]
        plane_exchange(src_of, dst_of, sid)
        sr1[it, p] = st1[it]
        plane_wait(src_of, dst_of, sid)
        peak_t, sum_t = sr1[it, 0, 0], sr1[it, 0, 1]
        for k in range(1, 16):
            peak_t = jnp.maximum(peak_t, sr1[it, k, 0])
            sum_t = sum_t + sr1[it, k, 1]
        st2[it, 0] = peak_t
        st2[it, 1] = sum_t
        tid = ids(4)
        for d in (1, 2, 3):
            send(st2.at[it], sr2.at[it, y], tid + d, dev(p, (y + d) % 4, c))
        sr2[it, y] = st2[it]
        for d in (1, 2, 3):
            arrived(sr2.at[it, (y + 4 - d) % 4], tid + d)
        peak_t, sum_t = sr2[it, 0, 0], sr2[it, 0, 1]
        for k in range(1, 4):
            peak_t = jnp.maximum(peak_t, sr2[it, k, 0])
            sum_t = sum_t + sr2[it, k, 1]
        totals.append(sum_t)
        level = SHRINK * jnp.max(peak_t)

        @pl.loop(0, 8)
        def _(n):
            here = ds(n * 256, 256, 256)
            a, b = trial[0, :, here], trial[1, :, here]
            size = jnp.sqrt(a * a + b * b)
            factor = jnp.maximum(1.0 - level / jnp.maximum(size, level), 0.0)
            a, b = a * factor, b * factor
            if it == 0:
                coef[0, :, here] = a
                coef[1, :, here] = b
                cb[0, :, here] = a.astype(BF)
                cb[1, :, here] = b.astype(BF)
            else:
                cfo[0, :, here] = a
                cfo[1, :, here] = b

    nid = ids(1)
    for it in range(2):
        nt[it] = jnp.sqrt(totals[it])
    send(nt, nr, nid, dev(p, y, 1 - c))
    oid = ids(16)
    co = p // 8
    lane = (p % 8) * 2 + c

    def out_copy(q):
        return rcopy(
            cfo.at[:, :, ds(128 * q, 128, 128)],
            ot.at[c, :, ds(32 * (p % 8), 32, 32), :],
            oid + (q + 16 - p) % 16, oid + lane, dev(q, y, co),
        )

    away = co != c

    @pl.loop(1, 16)
    def _(k):
        out_copy((p + k) % 16).start()

    @pl.when(away)
    def _():
        out_copy(p).start()

    @pl.when(jnp.logical_not(away))
    def _():
        ot[c, :, ds(32 * (p % 8), 32, 32), :] = cfo[:, :, ds(128 * p, 128, 128)]

    arrived(nr, nid)
    for it in range(2):
        norms[it, c] = jnp.max(nt[it])
        norms[it, 1 - c] = jnp.max(nr[it])

    @pl.loop(0, 16)
    def _(k):
        q, f = 8 * c + k // 2, k % 2

        @pl.when(jnp.logical_or(q != p, f != c))
        def _():
            there = ot.at[f, :, ds(32 * (q % 8), 32, 32), :]
            rcopy(there, there, oid + k, oid + k, dev(p, y, 1 - c)).wait_recv()

    for f in range(2):
        for part in range(2):
            out[f, part] = ot[f, part].T

    @pl.loop(1, 16)
    def _(k):
        out_copy((p + k) % 16).wait_send()

    @pl.when(away)
    def _():
        out_copy(p).wait_send()

    sent()


def scratch():
    v = lambda *shape, t=BF: pltpu.VMEM(shape, t)
    return [
        v(N, 1024), v(N, N), v(N, N), v(2, 128, N, t=F32), v(2, 2, 128, N),
        v(2, 2, 32, 1024), v(2, 2, 32, 1024), v(2, 2, 32, 1024), v(2, 2, 32, 1024),
        v(2, 2, 32, N), v(2, 2, 32, N), v(2, 32, N), v(2, 2, 32, N),
        v(2, 2, 128, 512), v(2, 2, 512, 128), v(2, 2, 32, N),
        v(2, 32, N, t=F32), v(2, 32, N, t=F32), v(2, 32, N, t=F32), v(2, 32, N),
        v(2, 32, N), v(2, 512, 128), v(2, 128, N), v(2, 128, N), v(2, 128, 512),
        v(2, 2, 256, 128, t=F32),
        v(2, 2, 8, 128, t=F32), v(2, 2, 8, 128, t=F32),
        v(2, 16, 2, 8, 128, t=F32), v(2, 4, 2, 8, 128, t=F32),
        v(2, 8, 128, t=F32), v(2, 8, 128, t=F32),
        pltpu.SemaphoreType.DMA((192,)), pltpu.SemaphoreType.DMA((192,)),
    ]


def per_device(traces, wavelet):
    vm = pl.BlockSpec(memory_space=pltpu.VMEM)
    sm = pl.BlockSpec(memory_space=pltpu.SMEM)
    return pl.pallas_call(
        kernel,
        out_shape=(
            jax.ShapeDtypeStruct((2, 2, 128, 256), F32),
            jax.ShapeDtypeStruct((2, 2), F32),
        ),
        in_specs=[vm, sm, vm, vm, vm, vm],
        out_specs=(vm, sm),
        scratch_shapes=scratch(),
        compiler_params=pltpu.CompilerParams(
            collective_id=0, has_side_effects=True, vmem_limit_bytes=60 * 1024 * 1024
        ),
        name="whole",
    )(traces, wavelet, *table_parts())


def solution(mesh):
    return jax.shard_map(
        per_device,
        mesh=mesh,
        in_specs=(P(None, None, "src", "rcv"), P()),
        out_specs=(P(None, None, "src", "rcv"), P()),
        check_vma=False,
    )
```

```python
import functools
import math

import jax
import jax.numpy as jnp
import numpy as np
from jax import lax
from jax.experimental import pallas as pl
from jax.experimental.pallas import tpu as pltpu
from jax.sharding import PartitionSpec as P

MESH = pl.DeviceIdType.MESH
N = 2048
BASE = 32
QUARTER = N // 4
STEP = 0.4
SHRINK = 0.2
BF = jnp.bfloat16
F32 = jnp.float32


def table_parts():
    def both(left, right, scale):
        angle = 2.0 * math.pi * ((left[:, None] * right[None, :]) % N) / N
        return [(f(angle) * scale).astype(np.float32) for f in (np.cos, np.sin)]

    scale = 1.0 / math.sqrt(N)
    quarter = np.arange(QUARTER)
    residue = np.arange(4)
    order = (4 * quarter[None, :] + residue[:, None]).reshape(-1)
    first = (4 * np.arange(BASE)[None, :] + residue[:, None]).reshape(-1)
    later = BASE * np.arange(QUARTER // BASE)
    return [
        *both(np.arange(BASE), order, scale), *both(later, order, 1.0),
        *both(first, quarter, scale), *both(4 * later, quarter, 1.0),
    ]


def kernel(
    tr, wave, base_c, base_s, mul_c, mul_s, ibase_c, ibase_s, imul_c, imul_s, out, norms,
    tf, tab_c, tab_s, inv_c, inv_s, perm, pg, sb, ra, rb, qa, qb, dl, dr, ub, yb, zz, zt, xt,
    trial, cfo, cb, hb, wt, hh, mb, mf, ot, nat, keep, got, st1, st2, sr1, sr2, nt, nr,
    ssem, rsem,
):
    p = lax.axis_index("src")
    rcv = lax.axis_index("rcv")
    y = rcv // 2
    c = rcv % 2
    z = p // 4
    x = p % 4
    used = [0]
    pending = []

    stage = [None]

    def mark(name):
        if stage[0] is not None:
            stage[0].__exit__(None, None, None)
        stage[0] = jax.named_scope(name) if name else None
        if name:
            stage[0].__enter__()

    def ids(n):
        used[0] += n
        return used[0] - n

    def dev(pp, yy, cc):
        return (pp, yy * 2 + cc)

    def rcopy(src, dst, s_id, r_id, where):
        return pltpu.make_async_remote_copy(
            src_ref=src, dst_ref=dst, send_sem=ssem.at[s_id], recv_sem=rsem.at[r_id],
            device_id=where, device_id_type=MESH,
        )

    def send(src, dst, s_id, where):
        copy = rcopy(src, dst, s_id, s_id, where)
        copy.start()
        pending.append(copy)

    def arrived(ref, r_id):
        rcopy(ref, ref, r_id, r_id, dev(p, y, 1 - c)).wait_recv()

    def sent():
        for copy in pending:
            copy.wait_send()
        pending.clear()

    def ds(start, size, unit):
        return pl.ds(pl.multiple_of(start, unit), size)

    mark("entry")
    barrier = pltpu.get_barrier_semaphore()
    me = p * 2 + c

    @pl.loop(1, 32)
    def _(k):
        other = (me + k) % 32
        pl.semaphore_signal(
            barrier, inc=1, device_id=dev(other // 2, y, other % 2), device_id_type=MESH
        )

    for d in (1, 2, 3):
        pl.semaphore_signal(
            barrier, inc=1, device_id=dev(p, (y + d) % 4, c), device_id_type=MESH
        )
    pl.semaphore_wait(barrier, 34)

    mark("swap")
    own_rows = ds(128 * p, 128, 128)
    swap = []
    for part in range(2):
        s_id = ids(1)
        where = tf.at[own_rows, ds(part * 512 + 256 * c, 256, 256)]
        send(tr.at[1 - c, part], where, s_id, dev(p, y, 1 - c))
        swap.append(s_id)
    for part in range(2):
        tf[own_rows, ds(part * 512 + 256 * c, 256, 256)] = tr[c, part]
    for part in range(2):
        arrived(tf.at[own_rows, ds(part * 512 + 256 * (1 - c), 256, 256)], swap[part])

    def shift(at, axis, d):
        zz_, xx_ = at
        return ((zz_ + d) % 4, xx_) if axis == 0 else (zz_, (xx_ + d) % 4)

    def neighbour(axis, d):
        a, b = shift((z, x), axis, d)
        return dev(a * 4 + b, y, c)

    def block(at, half, quarter=None):
        start = (at[0] * 4 + at[1]) * 128 + 64 * half
        if quarter is None:
            return tf.at[ds(start, 64, 32), :]
        return tf.at[ds(start + 32 * quarter, 32, 32), :]

    def ag_start(at, axis, half):
        s_id = ids(4)
        send(block(at, half), block(at, half), s_id, neighbour(axis, 1))
        send(block(at, half), block(at, half), s_id + 1, neighbour(axis, -1))
        return at, axis, half, s_id

    def ag_forward(item):
        at, axis, half, s_id = item
        left, right = shift(at, axis, -1), shift(at, axis, 1)
        arrived(block(left, half), s_id)
        send(block(left, half, 0), block(left, half, 0), s_id + 2, neighbour(axis, 1))
        arrived(block(right, half), s_id + 1)
        send(block(right, half, 1), block(right, half, 1), s_id + 3, neighbour(axis, -1))

    def ag_finish(item):
        at, axis, half, s_id = item
        far = shift(at, axis, 2)
        arrived(block(far, half, 0), s_id + 2)
        arrived(block(far, half, 1), s_id + 3)

    def make_table(first, last):
        @pl.loop(first, last)
        def _(m):
            rows = ds(m * BASE, BASE, BASE)
            for col in range(0, N, 512):
                here = pl.ds(col, 512)
                bc, bs = base_c[:, here], base_s[:, here]
                mc, ms = mul_c[pl.ds(m, 1), here], mul_s[pl.ds(m, 1), here]
                tab_c[rows, here] = (bc * mc - bs * ms).astype(BF)
                tab_s[rows, here] = (bs * mc + bc * ms).astype(BF)
            mc, ms = imul_c[pl.ds(m, 1), :], imul_s[pl.ds(m, 1), :]
            for r in range(4):
                bc, bs = ibase_c[r * BASE : r * BASE + BASE], ibase_s[r * BASE : r * BASE + BASE]
                rows = ds(r * QUARTER + m * BASE, BASE, BASE)
                inv_c[rows, :] = (bc * mc - bs * ms).astype(BF)
                inv_s[rows, :] = (bs * mc + bc * ms).astype(BF)

    def make_order():
        row = lax.broadcasted_iota(jnp.int32, (512, 512), 0)
        col = lax.broadcasted_iota(jnp.int32, (512, 512), 1)
        perm[...] = jnp.where(col == 4 * (row % 128) + row // 128, 1.0, 0.0).astype(BF)

    mark("gather_a")
    home = (z, x)
    first_x = ag_start(home, 1, 0)
    first_z = ag_start(home, 0, 1)
    second = [ag_start(home, 0, 0), ag_start(home, 1, 1)]
    make_table(0, 12)
    mark("gather_b")
    ag_forward(first_x)
    ag_forward(first_z)
    for d in (-1, 1):
        second.append(ag_start(shift(home, 1, d), 0, 0))
        second.append(ag_start(shift(home, 0, d), 1, 1))
    mark("table_b")
    make_table(12, 16)
    make_order()
    mark("gather_c")
    ag_forward(second[0])
    ag_forward(second[1])
    ag_finish(first_x)
    ag_finish(first_z)
    second.append(ag_start(shift(home, 1, 2), 0, 0))
    second.append(ag_start(shift(home, 0, 2), 1, 1))
    for item in second[2:]:
        ag_forward(item)
    for item in second:
        ag_finish(item)

    root = 1.0 / math.sqrt(N)
    wr = wave[c, 0] * root
    wi = wave[c, 1] * root

    def dot(a, b):
        return lax.dot_general(a, b, (((1,), (0,)), ((), ())), preferred_element_type=F32)

    def dot_nt(a, b):
        return lax.dot_general(a, b, (((1,), (1,)), ((), ())), preferred_element_type=F32)

    def forward(load, store):
        x = [[load(part, q) for part in range(2)] for q in range(4)]
        plus = [[x[h][k] + x[h + 2][k] for k in range(2)] for h in range(2)]
        less = [[x[h][k] - x[h + 2][k] for k in range(2)] for h in range(2)]
        for k in range(2):
            ub[0, k] = (plus[0][k] + plus[1][k]).astype(BF)
            ub[2, k] = (plus[0][k] - plus[1][k]).astype(BF)
        ub[1, 0] = (less[0][0] + less[1][1]).astype(BF)
        ub[1, 1] = (less[0][1] - less[1][0]).astype(BF)
        ub[3, 0] = (less[0][0] - less[1][1]).astype(BF)
        ub[3, 1] = (less[0][1] + less[1][0]).astype(BF)
        for r in range(4):
            rows = ub[r].reshape(64, QUARTER)
            here = pl.ds(r * QUARTER, QUARTER)
            a, b = dot(rows, tab_c[:, here]), dot(rows, tab_s[:, here])
            store(r, a[:32] + b[32:], a[32:] - b[:32])

    def inverse(load, half, store):
        for col in range(0, QUARTER, 256):
            e = []
            for r in range(4):
                rows = load(r)
                there = pl.ds(r * QUARTER, QUARTER)
                a = dot(rows, inv_c[there, col : col + 256])
                b = dot(rows, inv_s[there, col : col + 256])
                e.append((a[:half] - b[half:], b[:half] + a[half:]))
            plus = [[e[h][k] + e[h + 2][k] for k in range(2)] for h in range(2)]
            less = [[e[h][k] - e[h + 2][k] for k in range(2)] for h in range(2)]
            store(col, plus[0][0] + plus[1][0], plus[0][1] + plus[1][1])
            store(QUARTER + col, less[0][0] - less[1][1], less[0][1] + less[1][0])
            store(2 * QUARTER + col, plus[0][0] - plus[1][0], plus[0][1] - plus[1][1])
            store(3 * QUARTER + col, less[0][0] + less[1][1], less[0][1] - less[1][0])

    def residue(ref, q):
        return ref.at[:, q % 4, ds(32 * (q // 4), 32, 32), :]

    def plane_exchange(source, landing, first_id):
        @pl.loop(1, 16)
        def _(k):
            q = (p + k) % 16
            rcopy(source(q), landing(p), first_id + k, first_id + k, dev(q, y, c)).start()

    def plane_wait(source, landing, first_id):
        @pl.loop(1, 16)
        def _(k):
            q = (p + 16 - k) % 16
            w = rcopy(source((p + k) % 16), landing(q), first_id + k, first_id + k, dev(q, y, c))
            w.wait_recv()
            w.wait_send()

    totals = []
    for it in range(2):
        if it == 0:
            re = tf[own_rows, 0:512]
            im = tf[own_rows, 512:1024]
            mf[0] = re
            mf[1] = im
            ref, imf = re.astype(F32), im.astype(F32)
            squares = jnp.sum(ref * ref + imf * imf)
        else:
            mark("g_left")
            def put_half(col, a, b):
                hb[0, :, col : col + 256] = a.astype(BF)
                hb[1, :, col : col + 256] = b.astype(BF)

            inverse(lambda r: cb[:, r].reshape(64, QUARTER), 32, put_half)

            mark("g_plane")
            wid = ids(16)
            src_of = lambda q: hb.at[:, :, ds(128 * q, 128, 128)]
            dst_of = lambda q: residue(wt, q)
            plane_exchange(src_of, dst_of, wid)
            residue(wt, p)[...] = hb[:, :, ds(128 * p, 128, 128)]
            plane_wait(src_of, dst_of, wid)
            for part in range(2):
                for r in range(4):
                    hh[part, r, :, ds(128 * y, 128, 128)] = wt[part, r].astype(F32).T.astype(BF)
            mark("g_gather")
            gid = ids(4)

            def col_block(yy, rows=None):
                if rows is None:
                    return hh.at[:, :, :, ds(128 * yy, 128, 128)]
                return hh.at[rows, :, :, ds(128 * yy, 128, 128)]

            up, down, far = (y + 1) % 4, (y + 3) % 4, (y + 2) % 4
            send(col_block(y), col_block(y), gid, dev(p, up, c))
            send(col_block(y), col_block(y), gid + 1, dev(p, down, c))
            arrived(col_block(down), gid)
            send(col_block(down, 0), col_block(down, 0), gid + 2, dev(p, up, c))
            arrived(col_block(up), gid + 1)
            send(col_block(up, 1), col_block(up, 1), gid + 3, dev(p, down, c))
            arrived(col_block(far, 0), gid + 2)
            arrived(col_block(far, 1), gid + 3)

            mark("g_right")
            def put_model(col, a, b):
                mb[0, :, col : col + 256] = a.astype(BF)
                mb[1, :, col : col + 256] = b.astype(BF)

            inverse(lambda r: hh[:, r].reshape(256, QUARTER), 128, put_model)

            mark("misfit")
            squares = 0.0
            for n in range(2):
                rows = mb[...].reshape(256, N)
                a = dot(rows, tf[:, n * 256 : n * 256 + 256])
                b = dot(rows, tf[:, 512 + n * 256 : 768 + n * 256])
                pr, pi = a[:128] - b[128:], b[:128] + a[128:]
                here = ds(512 * y + n * 256, 256, 256)
                mr = tf[own_rows, n * 256 : n * 256 + 256].astype(F32) - mb[0, :, here].astype(F32)
                mi = tf[own_rows, 512 + n * 256 : 768 + n * 256].astype(F32) - mb[1, :, here].astype(F32)
                mr = mr + (wr * pr - wi * pi)
                mi = mi + (wr * pi + wi * pr)
                squares = squares + jnp.sum(mr * mr + mi * mi)
                mf[0, :, n * 256 : n * 256 + 256] = mr.astype(BF)
                mf[1, :, n * 256 : n * 256 + 256] = mi.astype(BF)

        mark("back")
        @pl.loop(0, 8)
        def _(n):
            rows = mf[...].reshape(256, 512)
            here = ds(n * 256, 256, 256)
            a = dot_nt(rows, tf[here, 0:512])
            b = dot_nt(rows, tf[here, 512:1024])
            br, bi = a[:128] + b[128:], a[128:] - b[:128]
            pg[0, :, here] = -(wr * br + wi * bi)
            pg[1, :, here] = -(wr * bi - wi * br)

        mine = ds(512 * y, 512, 512)
        pg[:, :, mine] = pg[:, :, mine] + mf[...].astype(F32)

        up, down, far = (y + 1) % 4, (y + 3) % 4, (y + 2) % 4
        lo, hi = pl.ds(0, 1024), pl.ds(1024, 1024)
        rows_of = lambda yy: ds(32 * yy, 32, 32)
        sb[it] = pg[...].astype(BF)
        sbi = sb.at[it]
        mark("scatter")
        rid = ids(6)
        send(sbi.at[:, rows_of(far), lo], ra.at[it], rid, dev(p, up, c))
        send(sbi.at[:, rows_of(far), hi], rb.at[it], rid + 1, dev(p, down, c))
        send(sbi.at[:, rows_of(up), hi], dl.at[it, :, :, hi], rid + 2, dev(p, up, c))
        send(sbi.at[:, rows_of(down), lo], dr.at[it, :, :, lo], rid + 3, dev(p, down, c))
        arrived(ra.at[it], rid)
        qa[it] = (pg[:, rows_of(up), lo] + ra[it].astype(F32)).astype(BF)
        send(qa.at[it], dl.at[it, :, :, lo], rid + 4, dev(p, up, c))
        arrived(rb.at[it], rid + 1)
        qb[it] = (pg[:, rows_of(down), hi] + rb[it].astype(F32)).astype(BF)
        send(qb.at[it], dr.at[it, :, :, hi], rid + 5, dev(p, down, c))
        arrived(dl.at[it, :, :, hi], rid + 2)
        arrived(dr.at[it, :, :, lo], rid + 3)
        arrived(dl.at[it, :, :, lo], rid + 4)
        arrived(dr.at[it, :, :, hi], rid + 5)

        mark("f_right")
        yid = ids(4)

        def gradient(part, q):
            here = pl.ds(q * QUARTER, QUARTER)
            theirs = dl[it, part, :, here].astype(F32) + dr[it, part, :, here].astype(F32)
            return pg[part, rows_of(y), here] + theirs

        def put_transformed(r, a, b):
            yb[it, 0, r] = a.astype(BF)
            yb[it, 1, r] = b.astype(BF)

        forward(gradient, put_transformed)
        mark("f_y")
        to_y = lambda yy: yb.at[it, :, :, :, ds(128 * yy, 128, 128)]
        from_y = lambda yy: zz.at[it, :, :, rows_of(yy), :]
        for d in (2, 1, 3):
            yy = (y + d) % 4
            send(to_y(yy), from_y(y), yid + d, dev(p, yy, c))
        from_y(y)[...] = to_y(y)[...]
        for d in (1, 3, 2):
            arrived(from_y((y + 4 - d) % 4), yid + d)
        for part in range(2):
            for r in range(4):
                zt[it, part, r] = zz[it, part, r].astype(F32).T.astype(BF)
        mark("f_plane")
        xid = ids(16)
        src_of = lambda q: residue(zt.at[it], q)
        dst_of = lambda q: xt.at[it, :, :, ds(128 * q, 128, 128)]
        plane_exchange(src_of, dst_of, xid)
        dst_of(p)[...] = src_of(p)[...]
        plane_wait(src_of, dst_of, xid)

        mark("f_left")
        peaks = []

        def put_trial(r, a, b):
            a, b = STEP * a, STEP * b
            if it:
                a, b = trial[0, r] + a, trial[1, r] + b
            trial[0, r] = a
            trial[1, r] = b
            peaks.append(jnp.max(jnp.sqrt(a * a + b * b)))

        forward(lambda part, q: xt[it, part, :, q * QUARTER : q * QUARTER + QUARTER].astype(F32), put_trial)
        peak = jnp.maximum(jnp.maximum(peaks[0], peaks[1]), jnp.maximum(peaks[2], peaks[3]))

        mark("stats")
        st1[it, 0] = jnp.full((8, 128), peak, F32)
        st1[it, 1] = jnp.full((8, 128), squares, F32)
        sid = ids(16)
        src_of = lambda q: st1.at[it]
        dst_of = lambda q: sr1.at[it, q]
        plane_exchange(src_of, dst_of, sid)
        sr1[it, p] = st1[it]
        if it:
            mark("out_send")
            oid = ids(16)
            for b in range(4):
                x = [trial[part, r, :, 128 * b : 128 * b + 128] for r in range(4) for part in range(2)]
                x = jnp.concatenate([jnp.concatenate(x[k::2], axis=1) for k in range(2)], axis=0)
                hi = x.astype(BF)
                rest = x - hi.astype(F32)
                mid = rest.astype(BF)
                low = (rest - mid.astype(F32)).astype(BF)
                order = perm[...]
                x = dot(hi, order) + dot(mid, order) + dot(low, order)
                cfo[0, :, 512 * b : 512 * b + 512] = x[:32]
                cfo[1, :, 512 * b : 512 * b + 512] = x[32:]
            out_src = lambda q: cfo.at[:, :, ds(128 * q, 128, 128)]
            out_dst = lambda q: ot.at[:, q]
            plane_exchange(out_src, out_dst, oid)
            out_dst(p)[...] = out_src(p)[...]
            mark("stats_wait")
        plane_wait(src_of, dst_of, sid)
        peak_t, sum_t = sr1[it, 0, 0], sr1[it, 0, 1]
        for k in range(1, 16):
            peak_t = jnp.maximum(peak_t, sr1[it, k, 0])
            sum_t = sum_t + sr1[it, k, 1]
        st2[it, 0] = peak_t
        st2[it, 1] = sum_t
        tid = ids(4)
        for d in (1, 2, 3):
            send(st2.at[it], sr2.at[it, y], tid + d, dev(p, (y + d) % 4, c))
        sr2[it, y] = st2[it]
        for d in (1, 2, 3):
            arrived(sr2.at[it, (y + 4 - d) % 4], tid + d)
        peak_t, sum_t = sr2[it, 0, 0], sr2[it, 0, 1]
        for k in range(1, 4):
            peak_t = jnp.maximum(peak_t, sr2[it, k, 0])
            sum_t = sum_t + sr2[it, k, 1]
        totals.append(sum_t)
        mark("shrink")
        level = SHRINK * jnp.max(peak_t)

        def shrunk(a, b):
            size = jnp.sqrt(a * a + b * b)
            factor = jnp.maximum(1.0 - level / jnp.maximum(size, level), 0.0)
            return a * factor, b * factor

        if it == 0:
            for r in range(4):
                a, b = shrunk(trial[0, r], trial[1, r])
                trial[0, r] = a
                trial[1, r] = b
                cb[0, r] = a.astype(BF)
                cb[1, r] = b.astype(BF)

    mark("out_wait")
    nid = ids(1)
    for it in range(2):
        nt[it] = jnp.sqrt(totals[it])
    send(nt, nr, nid, dev(p, y, 1 - c))
    plane_wait(out_src, out_dst, oid)
    mark("out_turn")
    for b in range(4):
        for r in range(4):
            a, d = shrunk(ot[0, 4 * b + r], ot[1, 4 * b + r])
            nat[0, b, pl.ds(r, 32, stride=4), :] = a
            nat[1, b, pl.ds(r, 32, stride=4), :] = d
    halves = ids(2)

    def turned(part, half):
        return jnp.concatenate([nat[part, 2 * half + k].T for k in range(2)], axis=1)

    for part in range(2):
        keep[part] = turned(part, 1 - c)
    send(keep, got, halves, dev(p, y, 1 - c))
    for part in range(2):
        out[c, part] = turned(part, c)
    mark("out_swap")
    arrived(nr, nid)
    for it in range(2):
        norms[it, c] = jnp.max(nt[it])
        norms[it, 1 - c] = jnp.max(nr[it])
    arrived(got, halves)
    out[1 - c] = got[...]
    sent()
    mark(None)


def scratch():
    v = lambda *shape, t=BF: pltpu.VMEM(shape, t)
    pair = pltpu.SemaphoreType.DMA((192,))
    return [
        v(N, 1024), v(QUARTER, N), v(QUARTER, N), v(N, QUARTER), v(N, QUARTER), v(512, 512),
        v(2, 128, N, t=F32), v(2, 2, 128, N),
        v(2, 2, 32, 1024), v(2, 2, 32, 1024), v(2, 2, 32, 1024), v(2, 2, 32, 1024),
        v(2, 2, 32, N), v(2, 2, 32, N), v(4, 2, 32, QUARTER), v(2, 2, 4, 32, QUARTER),
        v(2, 2, 4, 128, 128), v(2, 2, 4, 128, 128), v(2, 2, 32, N),
        v(2, 4, 32, QUARTER, t=F32), v(2, 32, N, t=F32), v(2, 4, 32, QUARTER),
        v(2, 32, N), v(2, 4, 128, 128), v(2, 4, 128, QUARTER), v(2, 128, N), v(2, 128, 512),
        v(2, 16, 32, 128, t=F32), v(2, 4, 128, 128, t=F32),
        v(2, 128, 256, t=F32), v(2, 128, 256, t=F32),
        v(2, 2, 8, 128, t=F32), v(2, 2, 8, 128, t=F32),
        v(2, 16, 2, 8, 128, t=F32), v(2, 4, 2, 8, 128, t=F32),
        v(2, 8, 128, t=F32), v(2, 8, 128, t=F32),
        pair, pair,
    ]


def per_device(traces, wavelet):
    vm = pl.BlockSpec(memory_space=pltpu.VMEM)
    sm = pl.BlockSpec(memory_space=pltpu.SMEM)
    return pl.pallas_call(
        kernel,
        out_shape=(
            jax.ShapeDtypeStruct((2, 2, 128, 256), F32),
            jax.ShapeDtypeStruct((2, 2), F32),
        ),
        in_specs=[vm, sm] + [vm] * 8,
        out_specs=(vm, sm),
        scratch_shapes=scratch(),
        compiler_params=pltpu.CompilerParams(
            collective_id=0, has_side_effects=True, vmem_limit_bytes=60 * 1024 * 1024
        ),
        name="whole",
    )(traces, wavelet, *table_parts())


def solution(mesh):
    return jax.shard_map(
        per_device,
        mesh=mesh,
        in_specs=(P(None, None, "src", "rcv"), P()),
        out_specs=(P(None, None, "src", "rcv"), P()),
        check_vma=False,
    )
```

```python
import functools
import math

import jax
import jax.numpy as jnp
import numpy as np
from jax import lax
from jax.experimental import pallas as pl
from jax.experimental.pallas import tpu as pltpu
from jax.sharding import PartitionSpec as P

MESH = pl.DeviceIdType.MESH
N = 2048
BASE = 32
QUARTER = N // 4
STEP = 0.4
SHRINK = 0.2
BF = jnp.bfloat16
F32 = jnp.float32


def table_parts():
    def both(left, right, scale):
        angle = 2.0 * math.pi * ((left[:, None] * right[None, :]) % N) / N
        return [(f(angle) * scale).astype(np.float32) for f in (np.cos, np.sin)]

    scale = 1.0 / math.sqrt(N)
    quarter = np.arange(QUARTER)
    residue = np.arange(4)
    order = (4 * quarter[None, :] + residue[:, None]).reshape(-1)
    first = (4 * np.arange(BASE)[None, :] + residue[:, None]).reshape(-1)
    later = BASE * np.arange(QUARTER // BASE)
    return [
        *both(np.arange(BASE), order, scale), *both(later, order, 1.0),
        *both(first, quarter, scale), *both(4 * later, quarter, 1.0),
    ]


def kernel(
    tr, wave, base_c, base_s, mul_c, mul_s, ibase_c, ibase_s, imul_c, imul_s, out, norms,
    tf, tab_c, tab_s, inv_c, inv_s, perm, pg, ubt, tp, sb, ra, rb, qa, qb, dl, dr, ub, zt, xt,
    trial, cfo, cb, hb, wt, hh, mb, mf, ot, nat, keep, got, st1, st2, sr1, sr2, nt, nr,
    ssem, rsem,
):
    src = lax.axis_index("src")
    rcv = lax.axis_index("rcv")
    y = rcv // 2
    c = rcv % 2
    z = src // 4
    x = src % 4
    lane2 = (1 - c) * x + c * y
    g = (1 - c) * y + c * x
    p = z * 4 + lane2
    used = [0]
    pending = []

    stage = [None]

    def mark(name):
        if stage[0] is not None:
            stage[0].__exit__(None, None, None)
        stage[0] = jax.named_scope(name) if name else None
        if name:
            stage[0].__enter__()

    def ids(n):
        used[0] += n
        return used[0] - n

    def chip(zz_, xx_, yy_, cc_):
        return (zz_ * 4 + xx_, yy_ * 2 + cc_)

    def dev(q, gg):
        second = q % 4
        return chip(q // 4, (1 - c) * second + c * gg, (1 - c) * gg + c * second, c)

    partner = chip(z, x, y, 1 - c)

    def rcopy(src, dst, s_id, r_id, where):
        return pltpu.make_async_remote_copy(
            src_ref=src, dst_ref=dst, send_sem=ssem.at[s_id], recv_sem=rsem.at[r_id],
            device_id=where, device_id_type=MESH,
        )

    def send(src, dst, s_id, where):
        copy = rcopy(src, dst, s_id, s_id, where)
        copy.start()
        pending.append(copy)

    def arrived(ref, r_id):
        rcopy(ref, ref, r_id, r_id, partner).wait_recv()

    def sent():
        for copy in pending:
            copy.wait_send()
        pending.clear()

    def ds(start, size, unit):
        return pl.ds(pl.multiple_of(start, unit), size)

    mark("entry")
    barrier = pltpu.get_barrier_semaphore()

    def greet(where):
        pl.semaphore_signal(barrier, inc=1, device_id=where, device_id_type=MESH)

    greet(partner)
    for d in (1, 2, 3):
        greet(dev(p, (g + d) % 4))
    for d in (1, 3):
        greet(dev((z + d) % 4 * 4 + lane2, g))
        greet(dev(z * 4 + (lane2 + d) % 4, g))
    crossed = jnp.logical_and(c == 1, x != y)

    @pl.when(crossed)
    def _():
        greet(chip(z, y, x, 0))
        greet(chip(z, y, x, 1))

    @pl.when(x != y)
    def _():
        pl.semaphore_wait(barrier, 9)

    @pl.when(x == y)
    def _():
        pl.semaphore_wait(barrier, 8)

    mark("swap")
    own_rows = ds(128 * p, 128, 128)
    swap = ids(2)
    landing = tf.at[:, ds(128 * src, 128, 128), ds(256 * c, 256, 256)]
    to_first = rcopy(tr.at[0], landing, swap, swap + c, chip(z, x, y, 0))
    to_second = rcopy(tr.at[1], landing, swap + 1, swap + c, chip(z, y, x, 1))
    stays = jnp.logical_and(c == 1, x == y)

    @pl.when(jnp.logical_not(stays))
    def _():
        to_second.start()

    @pl.when(c == 1)
    def _():
        to_first.start()

    @pl.when(c == 0)
    def _():
        landing[...] = tr[0]

    @pl.when(stays)
    def _():
        landing[...] = tr[1]

    @pl.when(c == 1)
    def _():
        arrived(tf.at[:, own_rows, 0:256], swap)

    @pl.when(jnp.logical_not(stays))
    def _():
        arrived(tf.at[:, own_rows, 256:512], swap + 1)

    def shift(at, axis, d):
        zz_, xx_ = at
        return ((zz_ + d + 4) % 4, xx_) if axis == 0 else (zz_, (xx_ + d + 4) % 4)

    def neighbour(axis, d):
        a, b = shift((z, lane2), axis, d)
        return dev(a * 4 + b, g)

    def block(at, kind, part=None):
        start = (at[0] * 4 + at[1]) * 128 + 96 * kind
        rows = 32 if kind else 96
        if part is not None:
            rows = rows // 2
            start = start + rows * part
        return tf.at[:, ds(start, rows, 16), :]

    def ag_start(at, axis, half):
        s_id = ids(4)
        send(block(at, half), block(at, half), s_id, neighbour(axis, 1))
        send(block(at, half), block(at, half), s_id + 1, neighbour(axis, -1))
        return at, axis, half, s_id

    def ag_forward(item):
        at, axis, half, s_id = item
        left, right = shift(at, axis, -1), shift(at, axis, 1)
        arrived(block(left, half), s_id)
        send(block(left, half, 0), block(left, half, 0), s_id + 2, neighbour(axis, 1))
        arrived(block(right, half), s_id + 1)
        send(block(right, half, 1), block(right, half, 1), s_id + 3, neighbour(axis, -1))

    def ag_finish(item):
        at, axis, half, s_id = item
        far = shift(at, axis, 2)
        arrived(block(far, half, 0), s_id + 2)
        arrived(block(far, half, 1), s_id + 3)

    def make_table(first, last):
        @pl.loop(first, last)
        def _(m):
            rows = ds(m * BASE, BASE, BASE)
            for col in range(0, N, 512):
                here = pl.ds(col, 512)
                bc, bs = base_c[:, here], base_s[:, here]
                mc, ms = mul_c[pl.ds(m, 1), here], mul_s[pl.ds(m, 1), here]
                tab_c[rows, here] = (bc * mc - bs * ms).astype(BF)
                tab_s[rows, here] = (bs * mc + bc * ms).astype(BF)
            mc, ms = imul_c[pl.ds(m, 1), :], imul_s[pl.ds(m, 1), :]
            for r in range(4):
                bc, bs = ibase_c[r * BASE : r * BASE + BASE], ibase_s[r * BASE : r * BASE + BASE]
                rows = ds(r * QUARTER + m * BASE, BASE, BASE)
                inv_c[rows, :] = (bc * mc - bs * ms).astype(BF)
                inv_s[rows, :] = (bs * mc + bc * ms).astype(BF)

    def make_order():
        row = lax.broadcasted_iota(jnp.int32, (512, 512), 0)
        col = lax.broadcasted_iota(jnp.int32, (512, 512), 1)
        perm[...] = jnp.where(col == 4 * (row % 128) + row // 128, 1.0, 0.0).astype(BF)

    mark("gather_a")
    home = (z, lane2)
    first = [ag_start(home, 0, 0), ag_start(home, 1, 1)]
    second = [ag_start(home, 1, 0), ag_start(home, 0, 1)]
    make_table(0, 12)
    mark("gather_b")
    for item in first:
        ag_forward(item)
    for d in (-1, 1):
        second.append(ag_start(shift(home, 0, d), 1, 0))
        second.append(ag_start(shift(home, 1, d), 0, 1))
    mark("table_b")
    make_table(12, 16)
    make_order()
    mark("gather_c")
    for item in second[:2]:
        ag_forward(item)
    for item in first:
        ag_finish(item)
    second.append(ag_start(shift(home, 0, 2), 1, 0))
    second.append(ag_start(shift(home, 1, 2), 0, 1))
    for item in second[2:]:
        ag_forward(item)
    for item in second:
        ag_finish(item)

    root = 1.0 / math.sqrt(N)
    wr = wave[c, 0] * root
    wi = wave[c, 1] * root

    def dot(a, b):
        return lax.dot_general(a, b, (((1,), (0,)), ((), ())), preferred_element_type=F32)

    def dot_nt(a, b):
        return lax.dot_general(a, b, (((1,), (1,)), ((), ())), preferred_element_type=F32)

    def quarters(load, ub):
        x = [[load(part, q) for part in range(2)] for q in range(4)]
        plus = [[x[h][k] + x[h + 2][k] for k in range(2)] for h in range(2)]
        less = [[x[h][k] - x[h + 2][k] for k in range(2)] for h in range(2)]
        for k in range(2):
            ub(0, k)[...] = (plus[0][k] + plus[1][k]).astype(BF)
            ub(2, k)[...] = (plus[0][k] - plus[1][k]).astype(BF)
        ub(1, 0)[...] = (less[0][0] + less[1][1]).astype(BF)
        ub(1, 1)[...] = (less[0][1] - less[1][0]).astype(BF)
        ub(3, 0)[...] = (less[0][0] - less[1][1]).astype(BF)
        ub(3, 1)[...] = (less[0][1] + less[1][0]).astype(BF)

    def forward(load, store):
        quarters(load, lambda r, part: ub.at[r, part])
        for r in range(4):
            rows = ub[r].reshape(64, QUARTER)
            here = pl.ds(r * QUARTER, QUARTER)
            a, b = dot(rows, tab_c[:, here]), dot(rows, tab_s[:, here])
            store(r, a[:32] + b[32:], a[32:] - b[:32])

    def inverse(load, half, store):
        for col in range(0, QUARTER, 256):
            e = []
            for r in range(4):
                rows = load(r)
                there = pl.ds(r * QUARTER, QUARTER)
                a = dot(rows, inv_c[there, col : col + 256])
                b = dot(rows, inv_s[there, col : col + 256])
                e.append((a[:half] - b[half:], b[:half] + a[half:]))
            plus = [[e[h][k] + e[h + 2][k] for k in range(2)] for h in range(2)]
            less = [[e[h][k] - e[h + 2][k] for k in range(2)] for h in range(2)]
            store(col, plus[0][0] + plus[1][0], plus[0][1] + plus[1][1])
            store(QUARTER + col, less[0][0] - less[1][1], less[0][1] + less[1][0])
            store(2 * QUARTER + col, plus[0][0] - plus[1][0], plus[0][1] - plus[1][1])
            store(3 * QUARTER + col, less[0][0] + less[1][1], less[0][1] - less[1][0])

    def residue(ref, q):
        return ref.at[:, q % 4, ds(32 * (q // 4), 32, 32), :]

    def plane_exchange(source, landing, first_id):
        @pl.loop(1, 16)
        def _(k):
            q = (p + k) % 16
            rcopy(source(q), landing(p), first_id + k, first_id + k, dev(q, g)).start()

    def plane_wait(source, landing, first_id):
        @pl.loop(1, 16)
        def _(k):
            q = (p + 16 - k) % 16
            w = rcopy(source((p + k) % 16), landing(q), first_id + k, first_id + k, dev(q, g))
            w.wait_recv()
            w.wait_send()

    totals = []
    for it in range(2):
        if it == 0:
            re = tf[0, own_rows, :]
            im = tf[1, own_rows, :]
            mf[0] = re
            mf[1] = im
            ref, imf = re.astype(F32), im.astype(F32)
            squares = jnp.sum(ref * ref + imf * imf)
        else:
            mark("g_left")
            def put_half(col, a, b):
                hb[0, :, col : col + 256] = a.astype(BF)
                hb[1, :, col : col + 256] = b.astype(BF)

            inverse(lambda r: cb[:, r].reshape(64, QUARTER), 32, put_half)

            mark("g_plane")
            wid = ids(16)
            src_of = lambda q: hb.at[:, :, ds(128 * q, 128, 128)]
            dst_of = lambda q: residue(wt, q)
            plane_exchange(src_of, dst_of, wid)
            residue(wt, p)[...] = hb[:, :, ds(128 * p, 128, 128)]
            plane_wait(src_of, dst_of, wid)
            for part in range(2):
                for r in range(4):
                    hh[part, r, :, ds(128 * g, 128, 128)] = wt[part, r].astype(F32).T.astype(BF)
            mark("g_gather")
            gid = ids(4)

            def col_block(yy, rows=None):
                if rows is None:
                    return hh.at[:, :, :, ds(128 * yy, 128, 128)]
                return hh.at[rows, :, :, ds(128 * yy, 128, 128)]

            up, down, far = (g + 1) % 4, (g + 3) % 4, (g + 2) % 4
            send(col_block(g), col_block(g), gid, dev(p, up))
            send(col_block(g), col_block(g), gid + 1, dev(p, down))
            arrived(col_block(down), gid)
            send(col_block(down, 0), col_block(down, 0), gid + 2, dev(p, up))
            arrived(col_block(up), gid + 1)
            send(col_block(up, 1), col_block(up, 1), gid + 3, dev(p, down))
            arrived(col_block(far, 0), gid + 2)
            arrived(col_block(far, 1), gid + 3)

            mark("g_right")
            def put_model(col, a, b):
                mb[0, :, col : col + 256] = a.astype(BF)
                mb[1, :, col : col + 256] = b.astype(BF)

            inverse(lambda r: hh[:, r].reshape(256, QUARTER), 128, put_model)

            mark("misfit")
            squares = 0.0
            for n in range(2):
                rows = mb[...].reshape(256, N)
                some = pl.ds(n * 256, 256)
                a, b = dot(rows, tf[0, :, some]), dot(rows, tf[1, :, some])
                pr, pi = a[:128] - b[128:], b[:128] + a[128:]
                here = ds(512 * g + n * 256, 256, 256)
                mr = tf[0, own_rows, some].astype(F32) - mb[0, :, here].astype(F32)
                mi = tf[1, own_rows, some].astype(F32) - mb[1, :, here].astype(F32)
                mr = mr + (wr * pr - wi * pi)
                mi = mi + (wr * pi + wi * pr)
                squares = squares + jnp.sum(mr * mr + mi * mi)
                mf[0, :, n * 256 : n * 256 + 256] = mr.astype(BF)
                mf[1, :, n * 256 : n * 256 + 256] = mi.astype(BF)

        mark("back")
        @pl.loop(0, 4)
        def _(n):
            errors = mf[...].reshape(256, 512)
            here = ds(n * 512, 512, 512)
            a, b = dot_nt(tf[0, here, :], errors), dot_nt(tf[1, here, :], errors)
            br, bi = a[:, :128] + b[:, 128:], a[:, 128:] - b[:, :128]
            pg[0, here, :] = -(wr * br + wi * bi)
            pg[1, here, :] = -(wr * bi - wi * br)

        mine = ds(512 * g, 512, 512)
        for part in range(2):
            pg[part, mine, :] = pg[part, mine, :] + mf[part].astype(F32).T

        mark("f_right")
        quarters(
            lambda part, q: pg[part, q * QUARTER : q * QUARTER + QUARTER, :],
            lambda r, part: ubt.at[r, :, pl.ds(128 * part, 128)],
        )
        for r in range(4):
            there = pl.ds(r * QUARTER, QUARTER)
            a, b = dot(inv_c[there, :], ubt[r]), dot(inv_s[there, :], ubt[r])
            tr_, ti_ = a[:, :128] + b[:, 128:], a[:, 128:] - b[:, :128]
            tp[0, r] = tr_
            tp[1, r] = ti_
            sb[it, 0, r] = tr_.astype(BF)
            sb[it, 1, r] = ti_.astype(BF)

        mark("scatter")
        up, down, far = (g + 1) % 4, (g + 3) % 4, (g + 2) % 4
        cols_of = lambda gg: ds(128 * gg, 128, 128)
        rid = ids(6)
        send(sb.at[it, 0, :, cols_of(far), :], ra.at[it], rid, dev(p, up))
        send(sb.at[it, 1, :, cols_of(far), :], rb.at[it], rid + 1, dev(p, down))
        send(sb.at[it, 1, :, cols_of(up), :], dl.at[it, 1], rid + 2, dev(p, up))
        send(sb.at[it, 0, :, cols_of(down), :], dr.at[it, 0], rid + 3, dev(p, down))
        arrived(ra.at[it], rid)
        qa[it] = (tp[0, :, cols_of(up), :] + ra[it].astype(F32)).astype(BF)
        send(qa.at[it], dl.at[it, 0], rid + 4, dev(p, up))
        arrived(rb.at[it], rid + 1)
        qb[it] = (tp[1, :, cols_of(down), :] + rb[it].astype(F32)).astype(BF)
        send(qb.at[it], dr.at[it, 1], rid + 5, dev(p, down))
        arrived(dl.at[it, 1], rid + 2)
        arrived(dr.at[it, 0], rid + 3)
        arrived(dl.at[it, 0], rid + 4)
        arrived(dr.at[it, 1], rid + 5)
        zt[it] = (tp[:, :, cols_of(g), :] + dl[it].astype(F32) + dr[it].astype(F32)).astype(BF)
        mark("f_plane")
        xid = ids(16)
        src_of = lambda q: residue(zt.at[it], q)
        dst_of = lambda q: xt.at[it, :, :, ds(128 * q, 128, 128)]
        plane_exchange(src_of, dst_of, xid)
        dst_of(p)[...] = src_of(p)[...]
        plane_wait(src_of, dst_of, xid)

        mark("f_left")
        peaks = []

        def put_trial(r, a, b):
            a, b = STEP * a, STEP * b
            if it:
                a, b = trial[0, r] + a, trial[1, r] + b
            trial[0, r] = a
            trial[1, r] = b
            peaks.append(jnp.max(jnp.sqrt(a * a + b * b)))

        forward(lambda part, q: xt[it, part, :, q * QUARTER : q * QUARTER + QUARTER].astype(F32), put_trial)
        peak = jnp.maximum(jnp.maximum(peaks[0], peaks[1]), jnp.maximum(peaks[2], peaks[3]))

        mark("stats")
        lane = lax.broadcasted_iota(jnp.int32, (1, 128), 1)
        st1[it] = jnp.where(lane < 64, peak, squares)
        sid = ids(16)
        src_of = lambda q: st1.at[it]
        dst_of = lambda q: sr1.at[it, q]
        plane_exchange(src_of, dst_of, sid)
        sr1[it, p] = st1[it]
        if it:
            mark("out_send")
            oid = ids(16)
            for b in range(4):
                v = [trial[part, r, :, 128 * b : 128 * b + 128] for r in range(4) for part in range(2)]
                v = jnp.concatenate([jnp.concatenate(v[k::2], axis=1) for k in range(2)], axis=0)
                hi = v.astype(BF)
                rest = v - hi.astype(F32)
                mid = rest.astype(BF)
                low = (rest - mid.astype(F32)).astype(BF)
                order = perm[...]
                v = dot(hi, order) + dot(mid, order) + dot(low, order)
                cfo[0, :, 512 * b : 512 * b + 512] = v[:32]
                cfo[1, :, 512 * b : 512 * b + 512] = v[32:]
            out_src = lambda q: cfo.at[:, :, ds(128 * q, 128, 128)]
            out_dst = lambda q: ot.at[:, q]
            away = jnp.logical_and(c == 1, x != y)

            def out_copy(q):
                s_id = oid + (q + 16 - p) % 16
                return rcopy(out_src(q), out_dst(p), s_id, oid + p, chip(q // 4, q % 4, g, c))

            @pl.loop(1, 16)
            def _(k):
                out_copy((p + k) % 16).start()

            @pl.when(away)
            def _():
                out_copy(p).start()

            @pl.when(jnp.logical_not(away))
            def _():
                out_dst(p)[...] = out_src(p)[...]

            mark("stats_wait")
        plane_wait(src_of, dst_of, sid)
        def joined(all_of):
            return jnp.where(lane < 64, jnp.max(all_of, axis=0), jnp.sum(all_of, axis=0))

        st2[it] = joined(sr1[it])
        tid = ids(4)
        for d in (1, 2, 3):
            send(st2.at[it], sr2.at[it, g], tid + d, dev(p, (g + d) % 4))
        sr2[it, g] = st2[it]
        for d in (1, 2, 3):
            arrived(sr2.at[it, (g + 4 - d) % 4], tid + d)
        both = joined(sr2[it])
        totals.append(jnp.max(jnp.where(lane < 64, 0.0, both)))
        mark("shrink")
        level = SHRINK * jnp.max(jnp.where(lane < 64, both, 0.0))

        def shrunk(a, b):
            size = jnp.sqrt(a * a + b * b)
            factor = jnp.maximum(1.0 - level / jnp.maximum(size, level), 0.0)
            return a * factor, b * factor

        if it == 0:
            for r in range(4):
                a, b = shrunk(trial[0, r], trial[1, r])
                trial[0, r] = a
                trial[1, r] = b
                cb[0, r] = a.astype(BF)
                cb[1, r] = b.astype(BF)

    mark("out_wait")
    nid = ids(1)
    for it in range(2):
        nt[it] = jnp.sqrt(jnp.full((1, 128), totals[it], F32))
    send(nt, nr, nid, partner)

    @pl.loop(1, 16)
    def _(k):
        q = (p + k) % 16
        arrived(out_dst(q), oid + q)
        out_copy(q).wait_send()

    @pl.when(away)
    def _():
        arrived(out_dst(p), oid + p)
        out_copy(p).wait_send()

    mark("out_turn")
    for b in range(4):
        for r in range(4):
            a, d = shrunk(ot[0, 4 * b + r], ot[1, 4 * b + r])
            nat[0, b, pl.ds(r, 32, stride=4), :] = a
            nat[1, b, pl.ds(r, 32, stride=4), :] = d
    halves = ids(2)

    def turned(part, half):
        return jnp.concatenate([nat[part, 2 * half + k].T for k in range(2)], axis=1)

    for part in range(2):
        keep[part] = turned(part, 1 - c)
    send(keep, got, halves, partner)
    for part in range(2):
        out[c, part] = turned(part, c)
    mark("out_swap")
    arrived(nr, nid)
    for it in range(2):
        norms[it, c] = jnp.max(nt[it])
        norms[it, 1 - c] = jnp.max(nr[it])
    arrived(got, halves)
    out[1 - c] = got[...]
    sent()

    @pl.when(jnp.logical_not(stays))
    def _():
        to_second.wait_send()

    @pl.when(c == 1)
    def _():
        to_first.wait_send()

    mark(None)


def scratch():
    v = lambda *shape, t=BF: pltpu.VMEM(shape, t)
    pair = pltpu.SemaphoreType.DMA((192,))
    return [
        v(2, N, 512), v(QUARTER, N), v(QUARTER, N), v(N, QUARTER), v(N, QUARTER), v(512, 512),
        v(2, N, 128, t=F32), v(4, QUARTER, 256), v(2, 4, QUARTER, 128, t=F32),
        v(2, 2, 4, QUARTER, 128), v(2, 4, 128, 128), v(2, 4, 128, 128), v(2, 4, 128, 128),
        v(2, 4, 128, 128), v(2, 2, 4, 128, 128), v(2, 2, 4, 128, 128), v(4, 2, 32, QUARTER),
        v(2, 2, 4, 128, 128), v(2, 2, 32, N),
        v(2, 4, 32, QUARTER, t=F32), v(2, 32, N, t=F32), v(2, 4, 32, QUARTER),
        v(2, 32, N), v(2, 4, 128, 128), v(2, 4, 128, QUARTER), v(2, 128, N), v(2, 128, 512),
        v(2, 16, 32, 128, t=F32), v(2, 4, 128, 128, t=F32),
        v(2, 128, 256, t=F32), v(2, 128, 256, t=F32),
        v(2, 1, 128, t=F32), v(2, 1, 128, t=F32), v(2, 16, 1, 128, t=F32), v(2, 4, 1, 128, t=F32),
        v(2, 1, 128, t=F32), v(2, 1, 128, t=F32),
        pair, pair,
    ]


def per_device(traces, wavelet):
    vm = pl.BlockSpec(memory_space=pltpu.VMEM)
    sm = pl.BlockSpec(memory_space=pltpu.SMEM)
    return pl.pallas_call(
        kernel,
        out_shape=(
            jax.ShapeDtypeStruct((2, 2, 128, 256), F32),
            jax.ShapeDtypeStruct((2, 2), F32),
        ),
        in_specs=[vm, sm] + [vm] * 8,
        out_specs=(vm, sm),
        scratch_shapes=scratch(),
        compiler_params=pltpu.CompilerParams(
            collective_id=0, has_side_effects=True, vmem_limit_bytes=60 * 1024 * 1024
        ),
        name="whole",
    )(traces, wavelet, *table_parts())


def solution(mesh):
    return jax.shard_map(
        per_device,
        mesh=mesh,
        in_specs=(P(None, None, "src", "rcv"), P()),
        out_specs=(P(None, None, "src", "rcv"), P()),
        check_vma=False,
    )
```

```python
import functools
import math

import jax
import jax.numpy as jnp
import numpy as np
from jax import lax
from jax.experimental import pallas as pl
from jax.experimental.pallas import tpu as pltpu
from jax.sharding import PartitionSpec as P

MESH = pl.DeviceIdType.MESH
N = 2048
BASE = 32
QUARTER = N // 4
STEP = 0.4
SHRINK = 0.2
BF = jnp.bfloat16
F32 = jnp.float32


def table_parts():
    def both(left, right, scale):
        angle = 2.0 * math.pi * ((left[:, None] * right[None, :]) % N) / N
        return [(f(angle) * scale).astype(np.float32) for f in (np.cos, np.sin)]

    scale = 1.0 / math.sqrt(N)
    quarter = np.arange(QUARTER)
    residue = np.arange(4)
    order = (4 * quarter[None, :] + residue[:, None]).reshape(-1)
    first = (4 * np.arange(BASE)[None, :] + residue[:, None]).reshape(-1)
    later = BASE * np.arange(QUARTER // BASE)
    return [
        *both(np.arange(BASE), order, scale), *both(later, order, 1.0),
        *both(first, quarter, scale), *both(4 * later, quarter, 1.0),
    ]


def kernel(
    tr, wave, base_c, base_s, mul_c, mul_s, ibase_c, ibase_s, imul_c, imul_s, out, norms,
    tf, tab_c, tab_s, inv_c, inv_s, perm, pg, ubt, tp, sb, ra, rb, qa, qb, dl, dr, ub, zt, xt,
    trial, cfo, cb, hb, wt, hh, mb, mf, ot, nat, keep, got, st1, st2, sr1, sr2, nt, nr,
    ssem, rsem,
):
    src = lax.axis_index("src")
    rcv = lax.axis_index("rcv")
    y = rcv // 2
    c = rcv % 2
    z = src // 4
    x = src % 4
    lane2 = (1 - c) * x + c * y
    g = (1 - c) * y + c * x
    p = z * 4 + lane2
    used = [0]
    pending = []

    stage = [None]

    def mark(name):
        if stage[0] is not None:
            stage[0].__exit__(None, None, None)
        stage[0] = jax.named_scope(name) if name else None
        if name:
            stage[0].__enter__()

    def ids(n):
        used[0] += n
        return used[0] - n

    def chip(zz_, xx_, yy_, cc_):
        return (zz_ * 4 + xx_, yy_ * 2 + cc_)

    def dev(q, gg):
        second = q % 4
        return chip(q // 4, (1 - c) * second + c * gg, (1 - c) * gg + c * second, c)

    partner = chip(z, x, y, 1 - c)

    def rcopy(src, dst, s_id, r_id, where):
        return pltpu.make_async_remote_copy(
            src_ref=src, dst_ref=dst, send_sem=ssem.at[s_id], recv_sem=rsem.at[r_id],
            device_id=where, device_id_type=MESH,
        )

    def send(src, dst, s_id, where):
        copy = rcopy(src, dst, s_id, s_id, where)
        copy.start()
        pending.append(copy)

    def arrived(ref, r_id):
        rcopy(ref, ref, r_id, r_id, partner).wait_recv()

    def sent():
        for copy in pending:
            copy.wait_send()
        pending.clear()

    def ds(start, size, unit):
        return pl.ds(pl.multiple_of(start, unit), size)

    mark("entry")
    barrier = pltpu.get_barrier_semaphore()

    def greet(where):
        pl.semaphore_signal(barrier, inc=1, device_id=where, device_id_type=MESH)

    greet(partner)
    for d in (1, 2, 3):
        greet(dev(p, (g + d) % 4))
    for d in (1, 3):
        greet(dev((z + d) % 4 * 4 + lane2, g))
        greet(dev(z * 4 + (lane2 + d) % 4, g))
    crossed = jnp.logical_and(c == 1, x != y)

    @pl.when(crossed)
    def _():
        greet(chip(z, y, x, 0))
        greet(chip(z, y, x, 1))

    @pl.when(x != y)
    def _():
        pl.semaphore_wait(barrier, 9)

    @pl.when(x == y)
    def _():
        pl.semaphore_wait(barrier, 8)

    mark("swap")
    own_rows = ds(128 * p, 128, 128)
    swap = ids(2)
    landing = tf.at[:, ds(128 * src, 128, 128), ds(256 * c, 256, 256)]
    to_first = rcopy(tr.at[0], landing, swap, swap + c, chip(z, x, y, 0))
    to_second = rcopy(tr.at[1], landing, swap + 1, swap + c, chip(z, y, x, 1))
    stays = jnp.logical_and(c == 1, x == y)

    @pl.when(jnp.logical_not(stays))
    def _():
        to_second.start()

    @pl.when(c == 1)
    def _():
        to_first.start()

    @pl.when(c == 0)
    def _():
        landing[...] = tr[0]

    @pl.when(stays)
    def _():
        landing[...] = tr[1]

    @pl.when(c == 1)
    def _():
        arrived(tf.at[:, own_rows, 0:256], swap)

    @pl.when(jnp.logical_not(stays))
    def _():
        arrived(tf.at[:, own_rows, 256:512], swap + 1)

    root = 1.0 / math.sqrt(N)
    wr = wave[c, 0] * root
    wi = wave[c, 1] * root

    def dot(a, b):
        return lax.dot_general(a, b, (((1,), (0,)), ((), ())), preferred_element_type=F32)

    def dot_nt(a, b):
        return lax.dot_general(a, b, (((1,), (1,)), ((), ())), preferred_element_type=F32)

    def back_rows(n):
        errors = mf[...].reshape(256, 512)
        here = ds(n * 512, 512, 512)
        a, b = dot_nt(tf[0, here, :], errors), dot_nt(tf[1, here, :], errors)
        br, bi = a[:, :128] + b[:, 128:], a[:, 128:] - b[:, :128]
        pg[0, here, :] = -(wr * br + wi * bi)
        pg[1, here, :] = -(wr * bi - wi * br)

    def back_start():
        for part in range(2):
            mf[part] = tf[part, own_rows, :]

    def shift(at, axis, d):
        zz_, xx_ = at
        return ((zz_ + d + 4) % 4, xx_) if axis == 0 else (zz_, (xx_ + d + 4) % 4)

    def neighbour(axis, d):
        a, b = shift((z, lane2), axis, d)
        return dev(a * 4 + b, g)

    def block(at, kind, part=None):
        start = (at[0] * 4 + at[1]) * 128 + 32 * kind
        if part is not None:
            return tf.at[:, ds(start + 16 * part, 16, 16), :]
        return tf.at[:, ds(start, 32, 16), :]

    def ag_start(at, axis, half):
        s_id = ids(4)
        send(block(at, half), block(at, half), s_id, neighbour(axis, 1))
        send(block(at, half), block(at, half), s_id + 1, neighbour(axis, -1))
        return at, axis, half, s_id

    def ag_forward(item):
        at, axis, half, s_id = item
        left, right = shift(at, axis, -1), shift(at, axis, 1)
        arrived(block(left, half), s_id)
        send(block(left, half, 0), block(left, half, 0), s_id + 2, neighbour(axis, 1))
        arrived(block(right, half), s_id + 1)
        send(block(right, half, 1), block(right, half, 1), s_id + 3, neighbour(axis, -1))

    def ag_finish(item):
        at, axis, half, s_id = item
        far = shift(at, axis, 2)
        arrived(block(far, half, 0), s_id + 2)
        arrived(block(far, half, 1), s_id + 3)

    def make_table(first, last):
        @pl.loop(first, last)
        def _(m):
            rows = ds(m * BASE, BASE, BASE)
            for col in range(0, N, 512):
                here = pl.ds(col, 512)
                bc, bs = base_c[:, here], base_s[:, here]
                mc, ms = mul_c[pl.ds(m, 1), here], mul_s[pl.ds(m, 1), here]
                tab_c[rows, here] = (bc * mc - bs * ms).astype(BF)
                tab_s[rows, here] = (bs * mc + bc * ms).astype(BF)
            mc, ms = imul_c[pl.ds(m, 1), :], imul_s[pl.ds(m, 1), :]
            for r in range(4):
                bc, bs = ibase_c[r * BASE : r * BASE + BASE], ibase_s[r * BASE : r * BASE + BASE]
                rows = ds(r * QUARTER + m * BASE, BASE, BASE)
                inv_c[rows, :] = (bc * mc - bs * ms).astype(BF)
                inv_s[rows, :] = (bs * mc + bc * ms).astype(BF)

    def make_order():
        row = lax.broadcasted_iota(jnp.int32, (512, 512), 0)
        col = lax.broadcasted_iota(jnp.int32, (512, 512), 1)
        perm[...] = jnp.where(col == 4 * (row % 128) + row // 128, 1.0, 0.0).astype(BF)

    mark("gather_a")
    home = (z, lane2)
    kinds = (0, 1, 2, 3)
    first_axis = (0, 0, 0, 1)
    first = [ag_start(home, first_axis[k], k) for k in kinds]
    own = [ag_start(home, 1 - first_axis[k], k) for k in kinds]
    make_table(0, 16)
    make_order()
    mark("gather_b")
    near = {}

    def pass_on(k, hops):
        near[k, hops] = [ag_start(shift(home, first_axis[k], d), 1 - first_axis[k], k) for d in hops]

    for k in (3, 0, 1, 2):
        ag_forward(first[k])
        pass_on(k, (-1, 1))
        if k < 3:
            ag_forward(own[k])
    ag_forward(own[3])
    for k in kinds:
        ag_finish(first[k])
        pass_on(k, (2,))
    mark("gather_c")
    for k in kinds:
        for item in near[k, (-1, 1)]:
            ag_forward(item)
    for k in kinds:
        ag_finish(own[k])
    mark("gather_back")
    back_start()
    back_rows(z)
    mark("gather_d")
    for k in kinds:
        ag_forward(near[k, (2,)][0])
    for k in kinds:
        for item in near[k, (-1, 1)]:
            ag_finish(item)
    mark("gather_back")
    back_rows((z + 3) % 4)
    back_rows((z + 1) % 4)
    mark("gather_e")
    for k in kinds:
        ag_finish(near[k, (2,)][0])
    mark("gather_back")
    back_rows((z + 2) % 4)

    def quarters(load, ub):
        x = [[load(part, q) for part in range(2)] for q in range(4)]
        plus = [[x[h][k] + x[h + 2][k] for k in range(2)] for h in range(2)]
        less = [[x[h][k] - x[h + 2][k] for k in range(2)] for h in range(2)]
        for k in range(2):
            ub(0, k)[...] = (plus[0][k] + plus[1][k]).astype(BF)
            ub(2, k)[...] = (plus[0][k] - plus[1][k]).astype(BF)
        ub(1, 0)[...] = (less[0][0] + less[1][1]).astype(BF)
        ub(1, 1)[...] = (less[0][1] - less[1][0]).astype(BF)
        ub(3, 0)[...] = (less[0][0] - less[1][1]).astype(BF)
        ub(3, 1)[...] = (less[0][1] + less[1][0]).astype(BF)

    def forward(load, store):
        quarters(load, lambda r, part: ub.at[r, part])
        for r in range(4):
            rows = ub[r].reshape(64, QUARTER)
            here = pl.ds(r * QUARTER, QUARTER)
            a, b = dot(rows, tab_c[:, here]), dot(rows, tab_s[:, here])
            store(r, a[:32] + b[32:], a[32:] - b[:32])

    def inverse(load, half, store):
        for col in range(0, QUARTER, 256):
            e = []
            for r in range(4):
                rows = load(r)
                there = pl.ds(r * QUARTER, QUARTER)
                a = dot(rows, inv_c[there, col : col + 256])
                b = dot(rows, inv_s[there, col : col + 256])
                e.append((a[:half] - b[half:], b[:half] + a[half:]))
            plus = [[e[h][k] + e[h + 2][k] for k in range(2)] for h in range(2)]
            less = [[e[h][k] - e[h + 2][k] for k in range(2)] for h in range(2)]
            store(col, plus[0][0] + plus[1][0], plus[0][1] + plus[1][1])
            store(QUARTER + col, less[0][0] - less[1][1], less[0][1] + less[1][0])
            store(2 * QUARTER + col, plus[0][0] - plus[1][0], plus[0][1] - plus[1][1])
            store(3 * QUARTER + col, less[0][0] + less[1][1], less[0][1] - less[1][0])

    def residue(ref, q):
        return ref.at[:, q % 4, ds(32 * (q // 4), 32, 32), :]

    offsets = [(a, b) for a in range(4) for b in range(4) if a or b]
    offsets.sort(key=lambda o: -(min(o[0], 4 - o[0]) + min(o[1], 4 - o[1])))

    def place(a, b):
        return (z + a) % 4 * 4 + (lane2 + b) % 4

    def plane_exchange(source, landing, first_id):
        for k, (a, b) in enumerate(offsets):
            q = place(a, b)
            rcopy(source(q), landing(p), first_id + k, first_id + k, dev(q, g)).start()

    def plane_wait(source, landing, first_id):
        for k, (a, b) in reversed(list(enumerate(offsets))):
            q = place(4 - a, 4 - b)
            w = rcopy(source(place(a, b)), landing(q), first_id + k, first_id + k, dev(q, g))
            w.wait_recv()
            w.wait_send()

    totals = []
    for it in range(2):
        if it == 0:
            ref, imf = mf[0].astype(F32), mf[1].astype(F32)
            squares = jnp.sum(ref * ref + imf * imf)
        else:
            mark("g_left")
            def put_half(col, a, b):
                hb[0, :, col : col + 256] = a.astype(BF)
                hb[1, :, col : col + 256] = b.astype(BF)

            inverse(lambda r: cb[:, r].reshape(64, QUARTER), 32, put_half)

            mark("g_plane")
            wid = ids(16)
            src_of = lambda q: hb.at[:, :, ds(128 * q, 128, 128)]
            dst_of = lambda q: residue(wt, q)
            plane_exchange(src_of, dst_of, wid)
            residue(wt, p)[...] = hb[:, :, ds(128 * p, 128, 128)]
            plane_wait(src_of, dst_of, wid)
            for part in range(2):
                for r in range(4):
                    hh[part, r, :, ds(128 * g, 128, 128)] = wt[part, r].astype(F32).T.astype(BF)
            mark("g_gather")
            gid = ids(10)

            def held(gg, part, h=None):
                which = slice(None) if h is None else pl.ds(2 * h, 2)
                return hh.at[part, which, :, ds(128 * gg, 128, 128)]

            up, down, far = (g + 1) % 4, (g + 3) % 4, (g + 2) % 4
            for h in range(2):
                send(held(g, 0, h), held(g, 0, h), gid + h, dev(p, up))
                send(held(g, 1, h), held(g, 1, h), gid + 2 + h, dev(p, down))
            send(held(g, 1), held(g, 1), gid + 4, dev(p, up))
            send(held(g, 0), held(g, 0), gid + 5, dev(p, down))
            for h in range(2):
                arrived(held(down, 0, h), gid + h)
                send(held(down, 0, h), held(down, 0, h), gid + 6 + h, dev(p, up))
                arrived(held(up, 1, h), gid + 2 + h)
                send(held(up, 1, h), held(up, 1, h), gid + 8 + h, dev(p, down))
            arrived(held(down, 1), gid + 4)
            arrived(held(up, 0), gid + 5)
            for h in range(2):
                arrived(held(far, 0, h), gid + 6 + h)
                arrived(held(far, 1, h), gid + 8 + h)

            mark("g_right")
            def put_model(col, a, b):
                mb[0, :, col : col + 256] = a.astype(BF)
                mb[1, :, col : col + 256] = b.astype(BF)

            inverse(lambda r: hh[:, r].reshape(256, QUARTER), 128, put_model)

            mark("misfit")
            squares = 0.0
            for n in range(2):
                rows = mb[...].reshape(256, N)
                some = pl.ds(n * 256, 256)
                a, b = dot(rows, tf[0, :, some]), dot(rows, tf[1, :, some])
                pr, pi = a[:128] - b[128:], b[:128] + a[128:]
                here = ds(512 * g + n * 256, 256, 256)
                mr = tf[0, own_rows, some].astype(F32) - mb[0, :, here].astype(F32)
                mi = tf[1, own_rows, some].astype(F32) - mb[1, :, here].astype(F32)
                mr = mr + (wr * pr - wi * pi)
                mi = mi + (wr * pi + wi * pr)
                squares = squares + jnp.sum(mr * mr + mi * mi)
                mf[0, :, n * 256 : n * 256 + 256] = mr.astype(BF)
                mf[1, :, n * 256 : n * 256 + 256] = mi.astype(BF)

        if it:
            mark("back")

            @pl.loop(0, 4)
            def _(n):
                back_rows(n)

        mine = ds(512 * g, 512, 512)
        for part in range(2):
            pg[part, mine, :] = pg[part, mine, :] + mf[part].astype(F32).T

        mark("f_right")
        quarters(
            lambda part, q: pg[part, q * QUARTER : q * QUARTER + QUARTER, :],
            lambda r, part: ubt.at[r, :, pl.ds(128 * part, 128)],
        )
        up, down, far = (g + 1) % 4, (g + 3) % 4, (g + 2) % 4
        rid = ids(12)

        def piece(ref, gg, h, part):
            return ref.at[it, part, pl.ds(2 * h, 2), ds(128 * gg, 128, 128), :]

        def slot(ref, h, *part):
            return ref.at[(it, *part, pl.ds(2 * h, 2))]

        for r in range(4):
            there = pl.ds(r * QUARTER, QUARTER)
            a, b = dot(inv_c[there, :], ubt[r]), dot(inv_s[there, :], ubt[r])
            tr_, ti_ = a[:, :128] + b[:, 128:], a[:, 128:] - b[:, :128]
            tp[0, r] = tr_
            tp[1, r] = ti_
            sb[it, 0, r] = tr_.astype(BF)
            sb[it, 1, r] = ti_.astype(BF)
            if r % 2:
                h = r // 2
                send(piece(sb, far, h, 0), slot(ra, h), rid + h, dev(p, up))
                send(piece(sb, far, h, 1), slot(rb, h), rid + 2 + h, dev(p, down))

        mark("scatter")
        for h in range(2):
            send(piece(sb, up, h, 1), slot(dl, h, 1), rid + 4 + h, dev(p, up))
            send(piece(sb, down, h, 0), slot(dr, h, 0), rid + 6 + h, dev(p, down))
        for h in range(2):
            pair = pl.ds(2 * h, 2)
            arrived(slot(ra, h), rid + h)
            qa[it, pair] = (tp[0, pair, ds(128 * up, 128, 128), :] + ra[it, pair].astype(F32)).astype(BF)
            send(slot(qa, h), slot(dl, h, 0), rid + 8 + h, dev(p, up))
            arrived(slot(rb, h), rid + 2 + h)
            qb[it, pair] = (tp[1, pair, ds(128 * down, 128, 128), :] + rb[it, pair].astype(F32)).astype(BF)
            send(slot(qb, h), slot(dr, h, 1), rid + 10 + h, dev(p, down))
        for h in range(2):
            arrived(slot(dl, h, 1), rid + 4 + h)
            arrived(slot(dr, h, 0), rid + 6 + h)
        for h in range(2):
            pair = pl.ds(2 * h, 2)
            arrived(slot(dl, h, 0), rid + 8 + h)
            arrived(slot(dr, h, 1), rid + 10 + h)
            total = tp[:, pair, ds(128 * g, 128, 128), :] + dl[it, :, pair].astype(F32)
            zt[it, :, pair] = (total + dr[it, :, pair].astype(F32)).astype(BF)
        mark("f_plane")
        xid = ids(16)
        src_of = lambda q: residue(zt.at[it], q)
        dst_of = lambda q: xt.at[it, :, :, ds(128 * q, 128, 128)]
        plane_exchange(src_of, dst_of, xid)
        dst_of(p)[...] = src_of(p)[...]
        plane_wait(src_of, dst_of, xid)

        mark("f_left")
        peaks = []

        def put_trial(r, a, b):
            a, b = STEP * a, STEP * b
            if it:
                a, b = trial[0, r] + a, trial[1, r] + b
            trial[0, r] = a
            trial[1, r] = b
            peaks.append(jnp.max(jnp.sqrt(a * a + b * b)))

        forward(lambda part, q: xt[it, part, :, q * QUARTER : q * QUARTER + QUARTER].astype(F32), put_trial)
        peak = jnp.maximum(jnp.maximum(peaks[0], peaks[1]), jnp.maximum(peaks[2], peaks[3]))

        mark("stats")
        lane = lax.broadcasted_iota(jnp.int32, (1, 128), 1)
        st1[it] = jnp.where(lane < 64, peak, squares)
        sid = ids(16)
        src_of = lambda q: st1.at[it]
        dst_of = lambda q: sr1.at[it, q]
        plane_exchange(src_of, dst_of, sid)
        sr1[it, p] = st1[it]
        if it:
            mark("out_send")
            oid = ids(16)
            for b in range(4):
                v = [trial[part, r, :, 128 * b : 128 * b + 128] for r in range(4) for part in range(2)]
                v = jnp.concatenate([jnp.concatenate(v[k::2], axis=1) for k in range(2)], axis=0)
                hi = v.astype(BF)
                rest = v - hi.astype(F32)
                mid = rest.astype(BF)
                low = (rest - mid.astype(F32)).astype(BF)
                order = perm[...]
                v = dot(hi, order) + dot(mid, order) + dot(low, order)
                cfo[0, :, 512 * b : 512 * b + 512] = v[:32]
                cfo[1, :, 512 * b : 512 * b + 512] = v[32:]
            out_src = lambda q: cfo.at[:, :, ds(128 * q, 128, 128)]
            out_dst = lambda q: ot.at[:, q]
            away = jnp.logical_and(c == 1, x != y)

            def out_copy(q):
                s_id = oid + (q + 16 - p) % 16
                return rcopy(out_src(q), out_dst(p), s_id, oid + p, chip(q // 4, q % 4, g, c))

            for a, b in offsets:
                out_copy(place(a, b)).start()

            @pl.when(away)
            def _():
                out_copy(p).start()

            @pl.when(jnp.logical_not(away))
            def _():
                out_dst(p)[...] = out_src(p)[...]

            mark("stats_wait")
        plane_wait(src_of, dst_of, sid)
        def joined(all_of):
            return jnp.where(lane < 64, jnp.max(all_of, axis=0), jnp.sum(all_of, axis=0))

        st2[it] = joined(sr1[it])
        tid = ids(4)
        for d in (1, 2, 3):
            send(st2.at[it], sr2.at[it, g], tid + d, dev(p, (g + d) % 4))
        sr2[it, g] = st2[it]
        for d in (1, 2, 3):
            arrived(sr2.at[it, (g + 4 - d) % 4], tid + d)
        both = joined(sr2[it])
        totals.append(jnp.max(jnp.where(lane < 64, 0.0, both)))
        mark("shrink")
        level = SHRINK * jnp.max(jnp.where(lane < 64, both, 0.0))

        def shrunk(a, b):
            size = jnp.sqrt(a * a + b * b)
            factor = jnp.maximum(1.0 - level / jnp.maximum(size, level), 0.0)
            return a * factor, b * factor

        if it == 0:
            for r in range(4):
                a, b = shrunk(trial[0, r], trial[1, r])
                trial[0, r] = a
                trial[1, r] = b
                cb[0, r] = a.astype(BF)
                cb[1, r] = b.astype(BF)

    mark("out_wait")
    nid = ids(1)
    for it in range(2):
        nt[it] = jnp.sqrt(jnp.full((1, 128), totals[it], F32))
    send(nt, nr, nid, partner)

    @pl.loop(1, 16)
    def _(k):
        q = (p + k) % 16
        arrived(out_dst(q), oid + q)
        out_copy(q).wait_send()

    @pl.when(away)
    def _():
        arrived(out_dst(p), oid + p)
        out_copy(p).wait_send()

    mark("out_turn")
    for b in range(4):
        for r in range(4):
            a, d = shrunk(ot[0, 4 * b + r], ot[1, 4 * b + r])
            nat[0, b, pl.ds(r, 32, stride=4), :] = a
            nat[1, b, pl.ds(r, 32, stride=4), :] = d
    halves = ids(2)

    def turned(part, half):
        return jnp.concatenate([nat[part, 2 * half + k].T for k in range(2)], axis=1)

    for part in range(2):
        keep[part] = turned(part, 1 - c)
    send(keep, got, halves, partner)
    for part in range(2):
        out[c, part] = turned(part, c)
    mark("out_swap")
    arrived(nr, nid)
    for it in range(2):
        norms[it, c] = jnp.max(nt[it])
        norms[it, 1 - c] = jnp.max(nr[it])
    arrived(got, halves)
    out[1 - c] = got[...]
    sent()

    @pl.when(jnp.logical_not(stays))
    def _():
        to_second.wait_send()

    @pl.when(c == 1)
    def _():
        to_first.wait_send()

    mark(None)


def scratch():
    v = lambda *shape, t=BF: pltpu.VMEM(shape, t)
    pair = pltpu.SemaphoreType.DMA((320,))
    return [
        v(2, N, 512), v(QUARTER, N), v(QUARTER, N), v(N, QUARTER), v(N, QUARTER), v(512, 512),
        v(2, N, 128, t=F32), v(4, QUARTER, 256), v(2, 4, QUARTER, 128, t=F32),
        v(2, 2, 4, QUARTER, 128), v(2, 4, 128, 128), v(2, 4, 128, 128), v(2, 4, 128, 128),
        v(2, 4, 128, 128), v(2, 2, 4, 128, 128), v(2, 2, 4, 128, 128), v(4, 2, 32, QUARTER),
        v(2, 2, 4, 128, 128), v(2, 2, 32, N),
        v(2, 4, 32, QUARTER, t=F32), v(2, 32, N, t=F32), v(2, 4, 32, QUARTER),
        v(2, 32, N), v(2, 4, 128, 128), v(2, 4, 128, QUARTER), v(2, 128, N), v(2, 128, 512),
        v(2, 16, 32, 128, t=F32), v(2, 4, 128, 128, t=F32),
        v(2, 128, 256, t=F32), v(2, 128, 256, t=F32),
        v(2, 1, 128, t=F32), v(2, 1, 128, t=F32), v(2, 16, 1, 128, t=F32), v(2, 4, 1, 128, t=F32),
        v(2, 1, 128, t=F32), v(2, 1, 128, t=F32),
        pair, pair,
    ]


def per_device(traces, wavelet):
    vm = pl.BlockSpec(memory_space=pltpu.VMEM)
    sm = pl.BlockSpec(memory_space=pltpu.SMEM)
    return pl.pallas_call(
        kernel,
        out_shape=(
            jax.ShapeDtypeStruct((2, 2, 128, 256), F32),
            jax.ShapeDtypeStruct((2, 2), F32),
        ),
        in_specs=[vm, sm] + [vm] * 8,
        out_specs=(vm, sm),
        scratch_shapes=scratch(),
        compiler_params=pltpu.CompilerParams(
            collective_id=0, has_side_effects=True, vmem_limit_bytes=60 * 1024 * 1024
        ),
        name="whole",
    )(traces, wavelet, *table_parts())


def solution(mesh):
    return jax.shard_map(
        per_device,
        mesh=mesh,
        in_specs=(P(None, None, "src", "rcv"), P()),
        out_specs=(P(None, None, "src", "rcv"), P()),
        check_vma=False,
    )
```

```python
import functools
import math

import jax
import jax.numpy as jnp
import numpy as np
from jax import lax
from jax.experimental import pallas as pl
from jax.experimental.pallas import tpu as pltpu
from jax.sharding import PartitionSpec as P

MESH = pl.DeviceIdType.MESH
N = 2048
BASE = 32
RECEIVES = 92
SENDS = 16
QUARTER = N // 4
STEP = 0.4
SHRINK = 0.2
BF = jnp.bfloat16
F32 = jnp.float32


def table_parts():
    def both(left, right, scale):
        angle = 2.0 * math.pi * ((left[:, None] * right[None, :]) % N) / N
        return [(f(angle) * scale).astype(np.float32) for f in (np.cos, np.sin)]

    scale = 1.0 / math.sqrt(N)
    quarter = np.arange(QUARTER)
    residue = np.arange(4)
    order = (4 * quarter[None, :] + residue[:, None]).reshape(-1)
    first = (4 * np.arange(BASE)[None, :] + residue[:, None]).reshape(-1)
    later = BASE * np.arange(QUARTER // BASE)
    return [
        *both(np.arange(BASE), order, scale), *both(later, order, 1.0),
        *both(first, quarter, scale), *both(4 * later, quarter, 1.0),
    ]


def kernel(
    tr_any, wave, t0, t1, t2, t3, t4, t5, t6, t7, out, norms,
    tr, b0, b1, b2, b3, b4, b5, b6, b7,
    tf, tab_c, tab_s, inv_c, inv_s, perm, pg, ubt, tp, sb, ra, rb, qa, qb, dl, dr, ub, zt, xt,
    trial, cfo, cb, hb, wt, hh, mb, mf, ot, nat, keep, got, st1, st2, sr1, sr2, nt, nr,
    ssem, rsem, lsem,
):
    tables_any = (t0, t1, t2, t3, t4, t5, t6, t7)
    tables = (b0, b1, b2, b3, b4, b5, b6, b7)
    src = lax.axis_index("src")
    rcv = lax.axis_index("rcv")
    y = rcv // 2
    c = rcv % 2
    z = src // 4
    x = src % 4
    lane2 = (1 - c) * x + c * y
    g = (1 - c) * y + c * x
    p = z * 4 + lane2
    used = [0, 0]
    pending = []

    stage = [None]

    def mark(name):
        if stage[0] is not None:
            stage[0].__exit__(None, None, None)
        stage[0] = jax.named_scope(name) if name else None
        if name:
            stage[0].__enter__()

    def ids(n):
        used[0] += n
        return used[0] - n

    def out_id():
        used[1] += 1
        return used[1] - 1

    def chip(zz_, xx_, yy_, cc_):
        return (zz_ * 4 + xx_, yy_ * 2 + cc_)

    def dev(q, gg):
        second = q % 4
        return chip(q // 4, (1 - c) * second + c * gg, (1 - c) * gg + c * second, c)

    partner = chip(z, x, y, 1 - c)

    def rcopy(src, dst, s_id, r_id, where):
        return pltpu.make_async_remote_copy(
            src_ref=src, dst_ref=dst, send_sem=ssem.at[s_id], recv_sem=rsem.at[r_id],
            device_id=where, device_id_type=MESH,
        )

    def send(src, dst, s_id, r_id, where):
        rcopy(src, dst, s_id, r_id, where).start()

    def arrived(ref, r_id):
        rcopy(ref, ref, 0, r_id, partner).wait_recv()

    def sent(ref, s_id):
        pending.append(rcopy(ref, ref, s_id, 0, partner))

    def ds(start, size, unit):
        return pl.ds(pl.multiple_of(start, unit), size)

    mark("entry")
    fetched = [
        pltpu.make_async_copy(a, b, lsem.at[k])
        for k, (a, b) in enumerate(zip((tr_any, *tables_any), (tr, *tables)))
    ]
    for copy in fetched:
        copy.start()
    base_c, base_s, mul_c, mul_s, ibase_c, ibase_s, imul_c, imul_s = tables
    barrier = pltpu.get_barrier_semaphore()

    def greet(where):
        pl.semaphore_signal(barrier, inc=1, device_id=where, device_id_type=MESH)

    greet(partner)
    for d in (1, 2, 3):
        greet(dev(p, (g + d) % 4))
    for d in (1, 3):
        greet(dev((z + d) % 4 * 4 + lane2, g))
        greet(dev(z * 4 + (lane2 + d) % 4, g))
    crossed = jnp.logical_and(c == 1, x != y)

    @pl.when(crossed)
    def _():
        greet(chip(z, y, x, 0))
        greet(chip(z, y, x, 1))

    @pl.when(x != y)
    def _():
        pl.semaphore_wait(barrier, 9)

    @pl.when(x == y)
    def _():
        pl.semaphore_wait(barrier, 8)

    mark("swap")
    own_rows = ds(128 * p, 128, 128)
    fetched[0].wait()
    swap, swap_s = ids(2), [out_id(), out_id()]
    landing = tf.at[:, ds(128 * src, 128, 128), ds(256 * c, 256, 256)]
    to_first = rcopy(tr.at[0], landing, swap_s[0], swap + c, chip(z, x, y, 0))
    to_second = rcopy(tr.at[1], landing, swap_s[1], swap + c, chip(z, y, x, 1))
    stays = jnp.logical_and(c == 1, x == y)

    @pl.when(jnp.logical_not(stays))
    def _():
        to_second.start()

    @pl.when(c == 1)
    def _():
        to_first.start()

    @pl.when(c == 0)
    def _():
        landing[...] = tr[0]

    @pl.when(stays)
    def _():
        landing[...] = tr[1]

    @pl.when(c == 1)
    def _():
        arrived(tf.at[:, own_rows, 0:256], swap)

    @pl.when(jnp.logical_not(stays))
    def _():
        arrived(tf.at[:, own_rows, 256:512], swap + 1)

    root = 1.0 / math.sqrt(N)
    wr = wave[c, 0] * root
    wi = wave[c, 1] * root

    def dot(a, b):
        return lax.dot_general(a, b, (((1,), (0,)), ((), ())), preferred_element_type=F32)

    def dot_nt(a, b):
        return lax.dot_general(a, b, (((1,), (1,)), ((), ())), preferred_element_type=F32)

    def back_rows(n):
        errors = mf[...].reshape(256, 512)
        here = ds(n * 512, 512, 512)
        a, b = dot_nt(tf[0, here, :], errors), dot_nt(tf[1, here, :], errors)
        br, bi = a[:, :128] + b[:, 128:], a[:, 128:] - b[:, :128]
        pg[0, here, :] = -(wr * br + wi * bi)
        pg[1, here, :] = -(wr * bi - wi * br)

    def back_start():
        for part in range(2):
            mf[part] = tf[part, own_rows, :]

    def shift(at, axis, d):
        zz_, xx_ = at
        return ((zz_ + d + 4) % 4, xx_) if axis == 0 else (zz_, (xx_ + d + 4) % 4)

    def neighbour(axis, d):
        a, b = shift((z, lane2), axis, d)
        return dev(a * 4 + b, g)

    def block(at, kind, part=None):
        start = (at[0] * 4 + at[1]) * 128 + 32 * kind
        if part is not None:
            return tf.at[:, ds(start + 16 * part, 16, 16), :]
        return tf.at[:, ds(start, 32, 16), :]

    gather_s = out_id()

    def ag_start(at, axis, half):
        r_id = ids(3)
        send(block(at, half), block(at, half), gather_s, r_id, neighbour(axis, 1))
        send(block(at, half), block(at, half), gather_s, r_id + 1, neighbour(axis, -1))
        return at, axis, half, r_id

    def ag_forward(item):
        at, axis, half, r_id = item
        left, right = shift(at, axis, -1), shift(at, axis, 1)
        arrived(block(left, half), r_id)
        send(block(left, half, 0), block(left, half, 0), gather_s, r_id + 2, neighbour(axis, 1))
        arrived(block(right, half), r_id + 1)
        send(block(right, half, 1), block(right, half, 1), gather_s, r_id + 2, neighbour(axis, -1))

    def ag_finish(item):
        at, axis, half, r_id = item
        arrived(block(shift(at, axis, 2), half), r_id + 2)

    def make_table(first, last):
        @pl.loop(first, last)
        def _(m):
            rows = ds(m * BASE, BASE, BASE)
            for col in range(0, N, 512):
                here = pl.ds(col, 512)
                bc, bs = base_c[:, here], base_s[:, here]
                mc, ms = mul_c[pl.ds(m, 1), here], mul_s[pl.ds(m, 1), here]
                tab_c[rows, here] = (bc * mc - bs * ms).astype(BF)
                tab_s[rows, here] = (bs * mc + bc * ms).astype(BF)
            mc, ms = imul_c[pl.ds(m, 1), :], imul_s[pl.ds(m, 1), :]
            for r in range(4):
                bc, bs = ibase_c[r * BASE : r * BASE + BASE], ibase_s[r * BASE : r * BASE + BASE]
                rows = ds(r * QUARTER + m * BASE, BASE, BASE)
                inv_c[rows, :] = (bc * mc - bs * ms).astype(BF)
                inv_s[rows, :] = (bs * mc + bc * ms).astype(BF)

    def make_order():
        row = lax.broadcasted_iota(jnp.int32, (512, 512), 0)
        col = lax.broadcasted_iota(jnp.int32, (512, 512), 1)
        perm[...] = jnp.where(col == 4 * (row % 128) + row // 128, 1.0, 0.0).astype(BF)

    mark("gather_a")
    home = (z, lane2)
    kinds = (0, 1, 2, 3)
    first_axis = (0, 0, 0, 1)
    first = [ag_start(home, first_axis[k], k) for k in kinds]
    own = [ag_start(home, 1, k) for k in (0, 1, 2)]
    for copy in fetched[1:]:
        copy.wait()
    make_table(0, 16)
    make_order()
    mark("gather_b")
    near = {}

    def pass_on(k, hops):
        near[k, hops] = [ag_start(shift(home, first_axis[k], d), 1 - first_axis[k], k) for d in hops]

    ag_forward(first[3])
    for k in (0, 1, 2):
        ag_forward(first[k])
        pass_on(k, (-1, 1))
        if k == 2:
            own.append(ag_start(home, 0, 3))
        ag_forward(own[k])
    pass_on(3, (-1, 1))
    ag_finish(first[3])
    for k in (0, 1, 2):
        ag_finish(first[k])
        pass_on(k, (2,))
    pass_on(3, (2,))
    ag_forward(own[3])
    mark("gather_c")
    for k in kinds:
        for item in near[k, (-1, 1)]:
            ag_forward(item)
    for k in kinds:
        ag_finish(own[k])
    mark("gather_back")
    back_start()
    back_rows(z)
    mark("gather_d")
    for k in kinds:
        ag_forward(near[k, (2,)][0])
    for k in kinds:
        for item in near[k, (-1, 1)]:
            ag_finish(item)
    mark("gather_back")
    back_rows((z + 3) % 4)
    back_rows((z + 1) % 4)
    mark("gather_e")
    for k in kinds:
        ag_finish(near[k, (2,)][0])
    sent(tf.at[:, 0:1920, :], gather_s)
    mark("gather_back")
    back_rows((z + 2) % 4)

    def quarters(load, ub):
        x = [[load(part, q) for part in range(2)] for q in range(4)]
        plus = [[x[h][k] + x[h + 2][k] for k in range(2)] for h in range(2)]
        less = [[x[h][k] - x[h + 2][k] for k in range(2)] for h in range(2)]
        for k in range(2):
            ub(0, k)[...] = (plus[0][k] + plus[1][k]).astype(BF)
            ub(2, k)[...] = (plus[0][k] - plus[1][k]).astype(BF)
        ub(1, 0)[...] = (less[0][0] + less[1][1]).astype(BF)
        ub(1, 1)[...] = (less[0][1] - less[1][0]).astype(BF)
        ub(3, 0)[...] = (less[0][0] - less[1][1]).astype(BF)
        ub(3, 1)[...] = (less[0][1] + less[1][0]).astype(BF)

    def forward(load, store):
        quarters(load, lambda r, part: ub.at[r, part])
        for r in range(4):
            rows = ub[r].reshape(64, QUARTER)
            here = pl.ds(r * QUARTER, QUARTER)
            a, b = dot(rows, tab_c[:, here]), dot(rows, tab_s[:, here])
            store(r, a[:32] + b[32:], a[32:] - b[:32])

    def inverse(load, half, store):
        for col in range(0, QUARTER, 256):
            e = []
            for r in range(4):
                rows = load(r)
                there = pl.ds(r * QUARTER, QUARTER)
                a = dot(rows, inv_c[there, col : col + 256])
                b = dot(rows, inv_s[there, col : col + 256])
                e.append((a[:half] - b[half:], b[:half] + a[half:]))
            plus = [[e[h][k] + e[h + 2][k] for k in range(2)] for h in range(2)]
            less = [[e[h][k] - e[h + 2][k] for k in range(2)] for h in range(2)]
            store(col, plus[0][0] + plus[1][0], plus[0][1] + plus[1][1])
            store(QUARTER + col, less[0][0] - less[1][1], less[0][1] + less[1][0])
            store(2 * QUARTER + col, plus[0][0] - plus[1][0], plus[0][1] - plus[1][1])
            store(3 * QUARTER + col, less[0][0] + less[1][1], less[0][1] - less[1][0])

    def residue(ref, q):
        return ref.at[:, q % 4, ds(32 * (q // 4), 32, 32), :]

    offsets = [(a, b) for a in range(4) for b in range(4) if a or b]
    offsets.sort(key=lambda o: -(min(o[0], 4 - o[0]) + min(o[1], 4 - o[1])))

    def place(a, b):
        return (z + a) % 4 * 4 + (lane2 + b) % 4

    def plane_exchange(source, landing, r_id, s_id):
        for a, b in offsets:
            q = place(a, b)
            rcopy(source(q), landing(p), s_id, r_id, dev(q, g)).start()

    def plane_wait(others, r_id, s_id):
        arrived(others, r_id)
        sent(others, s_id)

    totals = []
    for it in range(2):
        if it == 0:
            ref, imf = mf[0].astype(F32), mf[1].astype(F32)
            squares = jnp.sum(ref * ref + imf * imf)
        else:
            mark("g_left")
            def put_half(col, a, b):
                hb[0, :, col : col + 256] = a.astype(BF)
                hb[1, :, col : col + 256] = b.astype(BF)

            inverse(lambda r: cb[:, r].reshape(64, QUARTER), 32, put_half)

            mark("g_plane")
            wid, wid_s = ids(1), out_id()
            src_of = lambda q: hb.at[:, :, ds(128 * q, 128, 128)]
            dst_of = lambda q: residue(wt, q)
            plane_exchange(src_of, dst_of, wid, wid_s)
            residue(wt, p)[...] = hb[:, :, ds(128 * p, 128, 128)]
            plane_wait(hb.at[:, :, 0:1920], wid, wid_s)
            for part in range(2):
                for r in range(4):
                    hh[part, r, :, ds(128 * g, 128, 128)] = wt[part, r].astype(F32).T.astype(BF)
            mark("g_gather")
            gid, gid_s = ids(8), out_id()

            def held(gg, part, h=None):
                which = slice(None) if h is None else pl.ds(2 * h, 2)
                return hh.at[part, which, :, ds(128 * gg, 128, 128)]

            up, down, far = (g + 1) % 4, (g + 3) % 4, (g + 2) % 4

            def pass_held(gg, part, h, r_id, to):
                send(held(gg, part, h), held(gg, part, h), gid_s, gid + r_id, dev(p, to))

            for h in range(2):
                pass_held(g, 0, h, h, up)
                pass_held(g, 1, h, 2 + h, down)
            pass_held(g, 1, None, 4, up)
            pass_held(g, 0, None, 5, down)
            for h in range(2):
                arrived(held(down, 0, h), gid + h)
                pass_held(down, 0, h, 6, up)
                arrived(held(up, 1, h), gid + 2 + h)
                pass_held(up, 1, h, 7, down)
            arrived(held(down, 1), gid + 4)
            arrived(held(up, 0), gid + 5)
            arrived(held(far, 0), gid + 6)
            arrived(held(far, 1), gid + 7)
            sent(hh.at[:, 0:3], gid_s)

            mark("g_right")
            def put_model(col, a, b):
                mb[0, :, col : col + 256] = a.astype(BF)
                mb[1, :, col : col + 256] = b.astype(BF)

            inverse(lambda r: hh[:, r].reshape(256, QUARTER), 128, put_model)

            mark("misfit")
            squares = 0.0
            for n in range(2):
                rows = mb[...].reshape(256, N)
                some = pl.ds(n * 256, 256)
                a, b = dot(rows, tf[0, :, some]), dot(rows, tf[1, :, some])
                pr, pi = a[:128] - b[128:], b[:128] + a[128:]
                here = ds(512 * g + n * 256, 256, 256)
                mr = tf[0, own_rows, some].astype(F32) - mb[0, :, here].astype(F32)
                mi = tf[1, own_rows, some].astype(F32) - mb[1, :, here].astype(F32)
                mr = mr + (wr * pr - wi * pi)
                mi = mi + (wr * pi + wi * pr)
                squares = squares + jnp.sum(mr * mr + mi * mi)
                mf[0, :, n * 256 : n * 256 + 256] = mr.astype(BF)
                mf[1, :, n * 256 : n * 256 + 256] = mi.astype(BF)

        if it:
            mark("back")

            @pl.loop(0, 4)
            def _(n):
                back_rows(n)

        mine = ds(512 * g, 512, 512)
        for part in range(2):
            pg[part, mine, :] = pg[part, mine, :] + mf[part].astype(F32).T

        mark("f_right")
        quarters(
            lambda part, q: pg[part, q * QUARTER : q * QUARTER + QUARTER, :],
            lambda r, part: ubt.at[r, :, pl.ds(128 * part, 128)],
        )
        up, down, far = (g + 1) % 4, (g + 3) % 4, (g + 2) % 4
        rid, rid_s = ids(6), out_id()

        def piece(ref, gg, h, part):
            return ref.at[it, part, pl.ds(2 * h, 2), ds(128 * gg, 128, 128), :]

        def slot(ref, h, *part):
            return ref.at[(it, *part, pl.ds(2 * h, 2))]

        for r in range(4):
            there = pl.ds(r * QUARTER, QUARTER)
            a, b = dot(inv_c[there, :], ubt[r]), dot(inv_s[there, :], ubt[r])
            tr_, ti_ = a[:, :128] + b[:, 128:], a[:, 128:] - b[:, :128]
            tp[0, r] = tr_
            tp[1, r] = ti_
            sb[it, 0, r] = tr_.astype(BF)
            sb[it, 1, r] = ti_.astype(BF)
            if r % 2:
                h = r // 2
                send(piece(sb, far, h, 0), slot(ra, h), rid_s, rid + h, dev(p, up))
                send(piece(sb, far, h, 1), slot(rb, h), rid_s, rid + 2 + h, dev(p, down))

        mark("scatter")
        for h in range(2):
            send(piece(sb, up, h, 1), slot(dl, h, 1), rid_s, rid + 4, dev(p, up))
            send(piece(sb, down, h, 0), slot(dr, h, 0), rid_s, rid + 5, dev(p, down))
        for h in range(2):
            pair = pl.ds(2 * h, 2)
            arrived(slot(ra, h), rid + h)
            qa[it, pair] = (tp[0, pair, ds(128 * up, 128, 128), :] + ra[it, pair].astype(F32)).astype(BF)
            send(slot(qa, h), slot(dl, h, 0), rid_s, rid + 4, dev(p, up))
            arrived(slot(rb, h), rid + 2 + h)
            qb[it, pair] = (tp[1, pair, ds(128 * down, 128, 128), :] + rb[it, pair].astype(F32)).astype(BF)
            send(slot(qb, h), slot(dr, h, 1), rid_s, rid + 5, dev(p, down))
        arrived(dl.at[it], rid + 4)
        arrived(dr.at[it], rid + 5)
        sent(sb.at[it, :, 0:3], rid_s)
        total = tp[:, :, ds(128 * g, 128, 128), :] + dl[it].astype(F32)
        zt[it] = (total + dr[it].astype(F32)).astype(BF)
        mark("f_plane")
        xid, xid_s = ids(1), out_id()
        src_of = lambda q: residue(zt.at[it], q)
        dst_of = lambda q: xt.at[it, :, :, ds(128 * q, 128, 128)]
        plane_exchange(src_of, dst_of, xid, xid_s)
        dst_of(p)[...] = src_of(p)[...]
        plane_wait(xt.at[it, :, :, 0:1920], xid, xid_s)

        mark("f_left")
        peaks = []

        def put_trial(r, a, b):
            a, b = STEP * a, STEP * b
            if it:
                a, b = trial[0, r] + a, trial[1, r] + b
            trial[0, r] = a
            trial[1, r] = b
            peaks.append(jnp.max(jnp.sqrt(a * a + b * b)))

        forward(lambda part, q: xt[it, part, :, q * QUARTER : q * QUARTER + QUARTER].astype(F32), put_trial)
        peak = jnp.maximum(jnp.maximum(peaks[0], peaks[1]), jnp.maximum(peaks[2], peaks[3]))

        mark("stats")
        lane = lax.broadcasted_iota(jnp.int32, (1, 128), 1)
        st1[it] = jnp.where(lane < 64, peak, squares)
        sid, sid_s = ids(1), out_id()
        src_of = lambda q: st1.at[it]
        dst_of = lambda q: sr1.at[it, q]
        plane_exchange(src_of, dst_of, sid, sid_s)
        sr1[it, p] = st1[it]
        if it:
            mark("out_send")
            oid, oid_s = ids(1), out_id()
            for b in range(4):
                v = [trial[part, r, :, 128 * b : 128 * b + 128] for r in range(4) for part in range(2)]
                v = jnp.concatenate([jnp.concatenate(v[k::2], axis=1) for k in range(2)], axis=0)
                hi = v.astype(BF)
                rest = v - hi.astype(F32)
                mid = rest.astype(BF)
                low = (rest - mid.astype(F32)).astype(BF)
                order = perm[...]
                v = dot(hi, order) + dot(mid, order) + dot(low, order)
                cfo[0, :, 512 * b : 512 * b + 512] = v[:32]
                cfo[1, :, 512 * b : 512 * b + 512] = v[32:]
            out_src = lambda q: cfo.at[:, :, ds(128 * q, 128, 128)]
            out_dst = lambda q: ot.at[:, q]
            away = jnp.logical_and(c == 1, x != y)

            def out_copy(q):
                return rcopy(out_src(q), out_dst(p), oid_s, oid, chip(q // 4, q % 4, g, c))

            for a, b in offsets:
                out_copy(place(a, b)).start()

            @pl.when(away)
            def _():
                out_copy(p).start()

            @pl.when(jnp.logical_not(away))
            def _():
                out_dst(p)[...] = out_src(p)[...]

            mark("stats_wait")
        plane_wait(sr1.at[it, 0:15], sid, sid_s)
        def joined(all_of):
            return jnp.where(lane < 64, jnp.max(all_of, axis=0), jnp.sum(all_of, axis=0))

        st2[it] = joined(sr1[it])
        tid, tid_s = ids(1), out_id()
        for d in (2, 1, 3):
            send(st2.at[it], sr2.at[it, g], tid_s, tid, dev(p, (g + d) % 4))
        sr2[it, g] = st2[it]
        arrived(sr2.at[it, 0:3], tid)
        sent(sr2.at[it, 0:3], tid_s)
        both = joined(sr2[it])
        totals.append(jnp.max(jnp.where(lane < 64, 0.0, both)))
        mark("shrink")
        level = SHRINK * jnp.max(jnp.where(lane < 64, both, 0.0))

        def shrunk(a, b):
            size = jnp.sqrt(a * a + b * b)
            factor = jnp.maximum(1.0 - level / jnp.maximum(size, level), 0.0)
            return a * factor, b * factor

        if it == 0:
            for r in range(4):
                a, b = shrunk(trial[0, r], trial[1, r])
                trial[0, r] = a
                trial[1, r] = b
                cb[0, r] = a.astype(BF)
                cb[1, r] = b.astype(BF)

    mark("out_wait")
    nid, nid_s = ids(1), out_id()
    for it in range(2):
        nt[it] = jnp.sqrt(jnp.full((1, 128), totals[it], F32))
    send(nt, nr, nid_s, nid, partner)

    @pl.when(away)
    def _():
        rcopy(ot, ot, oid_s, oid, partner).wait_recv()

    @pl.when(jnp.logical_not(away))
    def _():
        rcopy(ot.at[:, 0:15], ot.at[:, 0:15], oid_s, oid, partner).wait_recv()

    mark("out_turn")
    for b in range(4):
        for r in range(4):
            a, d = shrunk(ot[0, 4 * b + r], ot[1, 4 * b + r])
            nat[0, b, pl.ds(r, 32, stride=4), :] = a
            nat[1, b, pl.ds(r, 32, stride=4), :] = d
    halves, halves_s = ids(1), out_id()

    def turned(part, half):
        return jnp.concatenate([nat[part, 2 * half + k].T for k in range(2)], axis=1)

    for part in range(2):
        keep[part] = turned(part, 1 - c)
    send(keep, got, halves_s, halves, partner)
    for part in range(2):
        out[c, part] = turned(part, c)
    mark("out_swap")
    arrived(nr, nid)
    for it in range(2):
        norms[it, c] = jnp.max(nt[it])
        norms[it, 1 - c] = jnp.max(nr[it])
    arrived(got, halves)
    out[1 - c] = got[...]
    for copy in pending:
        copy.wait_send()
    rcopy(nt, nt, nid_s, nid, partner).wait_send()
    rcopy(keep, keep, halves_s, halves, partner).wait_send()

    @pl.when(away)
    def _():
        rcopy(ot, ot, oid_s, oid, partner).wait_send()

    @pl.when(jnp.logical_not(away))
    def _():
        rcopy(ot.at[:, 0:15], ot.at[:, 0:15], oid_s, oid, partner).wait_send()

    @pl.when(jnp.logical_not(stays))
    def _():
        to_second.wait_send()

    @pl.when(c == 1)
    def _():
        to_first.wait_send()

    assert used == [RECEIVES, SENDS], used
    mark(None)


def scratch():
    v = lambda *shape, t=BF: pltpu.VMEM(shape, t)
    return [
        v(2, 2, 128, 256), *[v(*a.shape, t=F32) for a in table_parts()],
        v(2, N, 512), v(QUARTER, N), v(QUARTER, N), v(N, QUARTER), v(N, QUARTER), v(512, 512),
        v(2, N, 128, t=F32), v(4, QUARTER, 256), v(2, 4, QUARTER, 128, t=F32),
        v(2, 2, 4, QUARTER, 128), v(2, 4, 128, 128), v(2, 4, 128, 128), v(2, 4, 128, 128),
        v(2, 4, 128, 128), v(2, 2, 4, 128, 128), v(2, 2, 4, 128, 128), v(4, 2, 32, QUARTER),
        v(2, 2, 4, 128, 128), v(2, 2, 32, N),
        v(2, 4, 32, QUARTER, t=F32), v(2, 32, N, t=F32), v(2, 4, 32, QUARTER),
        v(2, 32, N), v(2, 4, 128, 128), v(2, 4, 128, QUARTER), v(2, 128, N), v(2, 128, 512),
        v(2, 16, 32, 128, t=F32), v(2, 4, 128, 128, t=F32),
        v(2, 128, 256, t=F32), v(2, 128, 256, t=F32),
        v(2, 1, 128, t=F32), v(2, 1, 128, t=F32), v(2, 16, 1, 128, t=F32), v(2, 4, 1, 128, t=F32),
        v(2, 1, 128, t=F32), v(2, 1, 128, t=F32),
        pltpu.SemaphoreType.DMA((SENDS,)), pltpu.SemaphoreType.DMA((RECEIVES,)),
        pltpu.SemaphoreType.DMA((9,)),
    ]


def hand_on(a, b, out, norms):
    out[...] = a[...]
    for i in range(2):
        for j in range(2):
            norms[i, j] = b[i, j]


def per_device(traces, wavelet):
    vm = pl.BlockSpec(memory_space=pltpu.VMEM)
    sm = pl.BlockSpec(memory_space=pltpu.SMEM)
    hbm = pl.BlockSpec(memory_space=pl.ANY)
    shapes = (jax.ShapeDtypeStruct((2, 2, 128, 256), F32), jax.ShapeDtypeStruct((2, 2), F32))
    parts = pl.pallas_call(
        kernel,
        out_shape=shapes,
        in_specs=[hbm, sm] + [hbm] * 8,
        out_specs=(vm, sm),
        scratch_shapes=scratch(),
        compiler_params=pltpu.CompilerParams(
            collective_id=0, has_side_effects=True, vmem_limit_bytes=60 * 1024 * 1024
        ),
        name="whole",
    )(traces, wavelet, *table_parts())
    return pl.pallas_call(
        hand_on, out_shape=shapes, in_specs=[vm, sm], out_specs=(vm, sm), name="hand_on"
    )(*parts)


def solution(mesh):
    return jax.shard_map(
        per_device,
        mesh=mesh,
        in_specs=(P(None, None, "src", "rcv"), P()),
        out_specs=(P(None, None, "src", "rcv"), P()),
        check_vma=False,
    )
```

```python
import functools
import math

import jax
import jax.numpy as jnp
import numpy as np
from jax import lax
from jax.experimental import pallas as pl
from jax.experimental.pallas import tpu as pltpu
from jax.sharding import PartitionSpec as P

MESH = pl.DeviceIdType.MESH
N = 2048
BASE = 32
RECEIVES = 90
SENDS = 14
QUARTER = N // 4
STEP = 0.4
SHRINK = 0.2
BF = jnp.bfloat16
F32 = jnp.float32


def table_parts():
    def both(left, right, scale):
        angle = 2.0 * math.pi * ((left[:, None] * right[None, :]) % N) / N
        return [(f(angle) * scale).astype(np.float32) for f in (np.cos, np.sin)]

    scale = 1.0 / math.sqrt(N)
    quarter = np.arange(QUARTER)
    residue = np.arange(4)
    order = (4 * quarter[None, :] + residue[:, None]).reshape(-1)
    first = (4 * np.arange(BASE)[None, :] + residue[:, None]).reshape(-1)
    later = BASE * np.arange(QUARTER // BASE)
    return [
        *both(np.arange(BASE), order, scale), *both(later, order, 1.0),
        *both(first, quarter, scale), *both(4 * later, quarter, 1.0),
    ]


def kernel(
    tr_any, wave, t0, t1, t2, t3, t4, t5, t6, t7, out, norms,
    tr, b0, b1, b2, b3, b4, b5, b6, b7,
    tf, tab_c, tab_s, inv_c, inv_s, perm, pg, ubt, tp, sb, ra, rb, qa, qb, dl, dr, ub, zt, xt,
    trial, cfo, cb, hb, wt, hh, mb, mf, ot, nat, keep, got, st1, sr1, nt, nr,
    ssem, rsem, lsem,
):
    tables_any = (t0, t1, t2, t3, t4, t5, t6, t7)
    tables = (b0, b1, b2, b3, b4, b5, b6, b7)
    src = lax.axis_index("src")
    rcv = lax.axis_index("rcv")
    y = rcv // 2
    c = rcv % 2
    z = src // 4
    x = src % 4
    lane2 = (1 - c) * x + c * y
    g = (1 - c) * y + c * x
    p = z * 4 + lane2
    used = [0, 0]
    pending = []

    stage = [None]

    def mark(name):
        if stage[0] is not None:
            stage[0].__exit__(None, None, None)
        stage[0] = jax.named_scope(name) if name else None
        if name:
            stage[0].__enter__()

    def ids(n):
        used[0] += n
        return used[0] - n

    def out_id():
        used[1] += 1
        return used[1] - 1

    def chip(zz_, xx_, yy_, cc_):
        return (zz_ * 4 + xx_, yy_ * 2 + cc_)

    def dev(q, gg):
        second = q % 4
        return chip(q // 4, (1 - c) * second + c * gg, (1 - c) * gg + c * second, c)

    partner = chip(z, x, y, 1 - c)

    def rcopy(src, dst, s_id, r_id, where):
        return pltpu.make_async_remote_copy(
            src_ref=src, dst_ref=dst, send_sem=ssem.at[s_id], recv_sem=rsem.at[r_id],
            device_id=where, device_id_type=MESH,
        )

    def send(src, dst, s_id, r_id, where):
        rcopy(src, dst, s_id, r_id, where).start()

    def arrived(ref, r_id):
        rcopy(ref, ref, 0, r_id, partner).wait_recv()

    def sent(ref, s_id):
        pending.append(rcopy(ref, ref, s_id, 0, partner))

    def ds(start, size, unit):
        return pl.ds(pl.multiple_of(start, unit), size)

    mark("entry")
    fetched = [
        pltpu.make_async_copy(a, b, lsem.at[k])
        for k, (a, b) in enumerate(zip((tr_any, *tables_any), (tr, *tables)))
    ]
    for copy in fetched:
        copy.start()
    base_c, base_s, mul_c, mul_s, ibase_c, ibase_s, imul_c, imul_s = tables
    barrier = pltpu.get_barrier_semaphore()

    def greet(where):
        pl.semaphore_signal(barrier, inc=1, device_id=where, device_id_type=MESH)

    greet(partner)
    for d in (1, 2, 3):
        greet(dev(p, (g + d) % 4))
    for d in (1, 3):
        greet(dev((z + d) % 4 * 4 + lane2, g))
        greet(dev(z * 4 + (lane2 + d) % 4, g))
    crossed = jnp.logical_and(c == 1, x != y)

    @pl.when(crossed)
    def _():
        greet(chip(z, y, x, 0))
        greet(chip(z, y, x, 1))

    @pl.when(x != y)
    def _():
        pl.semaphore_wait(barrier, 9)

    @pl.when(x == y)
    def _():
        pl.semaphore_wait(barrier, 8)

    mark("swap")
    own_rows = ds(128 * p, 128, 128)
    fetched[0].wait()
    swap, swap_s = ids(2), [out_id(), out_id()]
    landing = tf.at[:, ds(128 * src, 128, 128), ds(256 * c, 256, 256)]
    to_first = rcopy(tr.at[0], landing, swap_s[0], swap + c, chip(z, x, y, 0))
    to_second = rcopy(tr.at[1], landing, swap_s[1], swap + c, chip(z, y, x, 1))
    stays = jnp.logical_and(c == 1, x == y)

    @pl.when(jnp.logical_not(stays))
    def _():
        to_second.start()

    @pl.when(c == 1)
    def _():
        to_first.start()

    @pl.when(c == 0)
    def _():
        landing[...] = tr[0]

    @pl.when(stays)
    def _():
        landing[...] = tr[1]

    @pl.when(c == 1)
    def _():
        arrived(tf.at[:, own_rows, 0:256], swap)

    @pl.when(jnp.logical_not(stays))
    def _():
        arrived(tf.at[:, own_rows, 256:512], swap + 1)

    root = 1.0 / math.sqrt(N)
    wr = wave[c, 0] * root
    wi = wave[c, 1] * root

    def dot(a, b):
        return lax.dot_general(a, b, (((1,), (0,)), ((), ())), preferred_element_type=F32)

    def dot_nt(a, b):
        return lax.dot_general(a, b, (((1,), (1,)), ((), ())), preferred_element_type=F32)

    def back_rows(n):
        errors = mf[...].reshape(256, 512)
        here = ds(n * 512, 512, 512)
        a, b = dot_nt(tf[0, here, :], errors), dot_nt(tf[1, here, :], errors)
        br, bi = a[:, :128] + b[:, 128:], a[:, 128:] - b[:, :128]
        pg[0, here, :] = -(wr * br + wi * bi)
        pg[1, here, :] = -(wr * bi - wi * br)

    def back_start():
        for part in range(2):
            mf[part] = tf[part, own_rows, :]

    def shift(at, axis, d):
        zz_, xx_ = at
        return (zz_ + (1 - axis) * d + 4) % 4, (xx_ + axis * d + 4) % 4

    def neighbour(axis, d):
        a, b = shift((z, lane2), axis, d)
        return dev(a * 4 + b, g)

    def block(at, kind, part=None):
        start = (at[0] * 4 + at[1]) * 128 + 32 * kind
        if part is not None:
            return tf.at[:, ds(start + 16 * part, 16, 16), :]
        return tf.at[:, ds(start, 32, 16), :]

    gather_s = out_id()

    def ag_start(at, axis, half):
        r_id = ids(3)
        send(block(at, half), block(at, half), gather_s, r_id, neighbour(axis, 1))
        send(block(at, half), block(at, half), gather_s, r_id + 1, neighbour(axis, -1))
        return at, axis, half, r_id

    def ag_forward(item):
        at, axis, half, r_id = item
        left, right = shift(at, axis, -1), shift(at, axis, 1)
        arrived(block(left, half), r_id)
        send(block(left, half, 0), block(left, half, 0), gather_s, r_id + 2, neighbour(axis, 1))
        arrived(block(right, half), r_id + 1)
        send(block(right, half, 1), block(right, half, 1), gather_s, r_id + 2, neighbour(axis, -1))

    def ag_finish(item):
        at, axis, half, r_id = item
        arrived(block(shift(at, axis, 2), half), r_id + 2)

    def make_table(first, last):
        @pl.loop(first, last)
        def _(m):
            rows = ds(m * BASE, BASE, BASE)
            for col in range(0, N, 512):
                here = pl.ds(col, 512)
                bc, bs = base_c[:, here], base_s[:, here]
                mc, ms = mul_c[pl.ds(m, 1), here], mul_s[pl.ds(m, 1), here]
                tab_c[rows, here] = (bc * mc - bs * ms).astype(BF)
                tab_s[rows, here] = (bs * mc + bc * ms).astype(BF)
            mc, ms = imul_c[pl.ds(m, 1), :], imul_s[pl.ds(m, 1), :]
            for r in range(4):
                bc, bs = ibase_c[r * BASE : r * BASE + BASE], ibase_s[r * BASE : r * BASE + BASE]
                rows = ds(r * QUARTER + m * BASE, BASE, BASE)
                inv_c[rows, :] = (bc * mc - bs * ms).astype(BF)
                inv_s[rows, :] = (bs * mc + bc * ms).astype(BF)

    def make_order():
        row = lax.broadcasted_iota(jnp.int32, (512, 512), 0)
        col = lax.broadcasted_iota(jnp.int32, (512, 512), 1)
        perm[...] = jnp.where(col == 4 * (row % 128) + row // 128, 1.0, 0.0).astype(BF)

    mark("gather_a")
    home = (z, lane2)
    kinds = (0, 1, 2, 3)
    first_axis = (0, 0, 1 - c, 1 - c)
    first, own = {}, {}
    for k in (0, 2, 1, 3):
        first[k] = ag_start(home, first_axis[k], k)
    for k in (0, 2, 1, 3):
        own[k] = ag_start(home, 1 - first_axis[k], k)
    for copy in fetched[1:]:
        copy.wait()
    make_table(0, 16)
    make_order()
    mark("gather_b")
    near = {}

    def pass_on(k, hops):
        near[k, hops] = [ag_start(shift(home, first_axis[k], d), 1 - first_axis[k], k) for d in hops]

    for k in (0, 2, 1, 3):
        ag_forward(first[k])
    for k in (0, 2, 1, 3):
        pass_on(k, (-1, 1))
        ag_forward(own[k])
    for k in (0, 2, 1, 3):
        ag_finish(first[k])
        pass_on(k, (2,))
    mark("gather_c")
    for k in (0, 2, 1, 3):
        for item in near[k, (-1, 1)]:
            ag_forward(item)
    for k in kinds:
        ag_finish(own[k])
    mark("gather_back")
    back_start()
    back_rows(z)
    mark("gather_d")
    for k in (0, 2, 1, 3):
        ag_forward(near[k, (2,)][0])
    for k in kinds:
        for item in near[k, (-1, 1)]:
            ag_finish(item)
    mark("gather_back")
    back_rows((z + 3) % 4)
    back_rows((z + 1) % 4)
    mark("gather_e")
    for k in kinds:
        ag_finish(near[k, (2,)][0])
    sent(tf.at[:, 0:1920, :], gather_s)
    mark("gather_back")
    back_rows((z + 2) % 4)

    def quarters(load, ub):
        x = [[load(part, q) for part in range(2)] for q in range(4)]
        plus = [[x[h][k] + x[h + 2][k] for k in range(2)] for h in range(2)]
        less = [[x[h][k] - x[h + 2][k] for k in range(2)] for h in range(2)]
        for k in range(2):
            ub(0, k)[...] = (plus[0][k] + plus[1][k]).astype(BF)
            ub(2, k)[...] = (plus[0][k] - plus[1][k]).astype(BF)
        ub(1, 0)[...] = (less[0][0] + less[1][1]).astype(BF)
        ub(1, 1)[...] = (less[0][1] - less[1][0]).astype(BF)
        ub(3, 0)[...] = (less[0][0] - less[1][1]).astype(BF)
        ub(3, 1)[...] = (less[0][1] + less[1][0]).astype(BF)

    def forward(load, store):
        quarters(load, lambda r, part: ub.at[r, part])
        for r in range(4):
            rows = ub[r].reshape(64, QUARTER)
            here = pl.ds(r * QUARTER, QUARTER)
            a, b = dot(rows, tab_c[:, here]), dot(rows, tab_s[:, here])
            store(r, a[:32] + b[32:], a[32:] - b[:32])

    def inverse(load, half, store):
        for col in range(0, QUARTER, 256):
            e = []
            for r in range(4):
                rows = load(r)
                there = pl.ds(r * QUARTER, QUARTER)
                a = dot(rows, inv_c[there, col : col + 256])
                b = dot(rows, inv_s[there, col : col + 256])
                e.append((a[:half] - b[half:], b[:half] + a[half:]))
            plus = [[e[h][k] + e[h + 2][k] for k in range(2)] for h in range(2)]
            less = [[e[h][k] - e[h + 2][k] for k in range(2)] for h in range(2)]
            store(col, plus[0][0] + plus[1][0], plus[0][1] + plus[1][1])
            store(QUARTER + col, less[0][0] - less[1][1], less[0][1] + less[1][0])
            store(2 * QUARTER + col, plus[0][0] - plus[1][0], plus[0][1] - plus[1][1])
            store(3 * QUARTER + col, less[0][0] + less[1][1], less[0][1] - less[1][0])

    def residue(ref, q):
        return ref.at[:, q % 4, ds(32 * (q // 4), 32, 32), :]

    offsets = [(a, b) for a in range(4) for b in range(4) if a or b]
    offsets.sort(key=lambda o: -(min(o[0], 4 - o[0]) + min(o[1], 4 - o[1])))

    everyone = [(a, b, d) for a in range(4) for b in range(4) for d in range(4) if a or b or d]
    everyone.sort(key=lambda o: -sum(min(i, 4 - i) for i in o))

    def place(a, b):
        return (z + a) % 4 * 4 + (lane2 + b) % 4

    def plane_exchange(source, landing, r_id, s_id):
        for a, b in offsets:
            q = place(a, b)
            rcopy(source(q), landing(p), s_id, r_id, dev(q, g)).start()

    def plane_wait(others, r_id, s_id):
        arrived(others, r_id)
        sent(others, s_id)

    totals = []
    for it in range(2):
        if it == 0:
            ref, imf = mf[0].astype(F32), mf[1].astype(F32)
            squares = jnp.sum(ref * ref + imf * imf)
        else:
            mark("g_left")
            def put_half(col, a, b):
                hb[0, :, col : col + 256] = a.astype(BF)
                hb[1, :, col : col + 256] = b.astype(BF)

            inverse(lambda r: cb[:, r].reshape(64, QUARTER), 32, put_half)

            mark("g_plane")
            wid, wid_s = ids(1), out_id()
            src_of = lambda q: hb.at[:, :, ds(128 * q, 128, 128)]
            dst_of = lambda q: residue(wt, q)
            plane_exchange(src_of, dst_of, wid, wid_s)
            residue(wt, p)[...] = hb[:, :, ds(128 * p, 128, 128)]
            plane_wait(hb.at[:, :, 0:1920], wid, wid_s)
            for part in range(2):
                for r in range(4):
                    hh[part, r, :, ds(128 * g, 128, 128)] = wt[part, r].astype(F32).T.astype(BF)
            mark("g_gather")
            gid, gid_s = ids(8), out_id()

            def held(gg, part, h=None):
                which = slice(None) if h is None else pl.ds(2 * h, 2)
                return hh.at[part, which, :, ds(128 * gg, 128, 128)]

            up, down, far = (g + 1) % 4, (g + 3) % 4, (g + 2) % 4

            def pass_held(gg, part, h, r_id, to):
                send(held(gg, part, h), held(gg, part, h), gid_s, gid + r_id, dev(p, to))

            for h in range(2):
                pass_held(g, 0, h, h, up)
                pass_held(g, 1, h, 2 + h, down)
            pass_held(g, 1, None, 4, up)
            pass_held(g, 0, None, 5, down)
            for h in range(2):
                arrived(held(down, 0, h), gid + h)
                pass_held(down, 0, h, 6, up)
                arrived(held(up, 1, h), gid + 2 + h)
                pass_held(up, 1, h, 7, down)
            arrived(held(down, 1), gid + 4)
            arrived(held(up, 0), gid + 5)
            arrived(held(far, 0), gid + 6)
            arrived(held(far, 1), gid + 7)
            sent(hh.at[:, 0:3], gid_s)

            mark("g_right")
            def put_model(col, a, b):
                mb[0, :, col : col + 256] = a.astype(BF)
                mb[1, :, col : col + 256] = b.astype(BF)

            inverse(lambda r: hh[:, r].reshape(256, QUARTER), 128, put_model)

            mark("misfit")
            squares = 0.0
            for n in range(2):
                rows = mb[...].reshape(256, N)
                some = pl.ds(n * 256, 256)
                a, b = dot(rows, tf[0, :, some]), dot(rows, tf[1, :, some])
                pr, pi = a[:128] - b[128:], b[:128] + a[128:]
                here = ds(512 * g + n * 256, 256, 256)
                mr = tf[0, own_rows, some].astype(F32) - mb[0, :, here].astype(F32)
                mi = tf[1, own_rows, some].astype(F32) - mb[1, :, here].astype(F32)
                mr = mr + (wr * pr - wi * pi)
                mi = mi + (wr * pi + wi * pr)
                squares = squares + jnp.sum(mr * mr + mi * mi)
                mf[0, :, n * 256 : n * 256 + 256] = mr.astype(BF)
                mf[1, :, n * 256 : n * 256 + 256] = mi.astype(BF)

        if it:
            mark("back")

            @pl.loop(0, 4)
            def _(n):
                back_rows(n)

        mine = ds(512 * g, 512, 512)
        for part in range(2):
            pg[part, mine, :] = pg[part, mine, :] + mf[part].astype(F32).T

        mark("f_right")
        quarters(
            lambda part, q: pg[part, q * QUARTER : q * QUARTER + QUARTER, :],
            lambda r, part: ubt.at[r, :, pl.ds(128 * part, 128)],
        )
        up, down, far = (g + 1) % 4, (g + 3) % 4, (g + 2) % 4
        rid, rid_s = ids(6), out_id()

        def piece(ref, gg, h, part):
            return ref.at[it, part, pl.ds(2 * h, 2), ds(128 * gg, 128, 128), :]

        def slot(ref, h, *part):
            return ref.at[(it, *part, pl.ds(2 * h, 2))]

        for r in range(4):
            there = pl.ds(r * QUARTER, QUARTER)
            a, b = dot(inv_c[there, :], ubt[r]), dot(inv_s[there, :], ubt[r])
            tr_, ti_ = a[:, :128] + b[:, 128:], a[:, 128:] - b[:, :128]
            tp[0, r] = tr_
            tp[1, r] = ti_
            sb[it, 0, r] = tr_.astype(BF)
            sb[it, 1, r] = ti_.astype(BF)
            if r % 2:
                h = r // 2
                send(piece(sb, far, h, 0), slot(ra, h), rid_s, rid + h, dev(p, up))
                send(piece(sb, far, h, 1), slot(rb, h), rid_s, rid + 2 + h, dev(p, down))

        mark("scatter")
        for h in range(2):
            send(piece(sb, up, h, 1), slot(dl, h, 1), rid_s, rid + 4, dev(p, up))
            send(piece(sb, down, h, 0), slot(dr, h, 0), rid_s, rid + 5, dev(p, down))
        for h in range(2):
            pair = pl.ds(2 * h, 2)
            arrived(slot(ra, h), rid + h)
            qa[it, pair] = (tp[0, pair, ds(128 * up, 128, 128), :] + ra[it, pair].astype(F32)).astype(BF)
            send(slot(qa, h), slot(dl, h, 0), rid_s, rid + 4, dev(p, up))
            arrived(slot(rb, h), rid + 2 + h)
            qb[it, pair] = (tp[1, pair, ds(128 * down, 128, 128), :] + rb[it, pair].astype(F32)).astype(BF)
            send(slot(qb, h), slot(dr, h, 1), rid_s, rid + 5, dev(p, down))
        arrived(dl.at[it], rid + 4)
        arrived(dr.at[it], rid + 5)
        sent(sb.at[it, :, 0:3], rid_s)
        total = tp[:, :, ds(128 * g, 128, 128), :] + dl[it].astype(F32)
        zt[it] = (total + dr[it].astype(F32)).astype(BF)
        mark("f_plane")
        xid, xid_s = ids(1), out_id()
        src_of = lambda q: residue(zt.at[it], q)
        dst_of = lambda q: xt.at[it, :, :, ds(128 * q, 128, 128)]
        plane_exchange(src_of, dst_of, xid, xid_s)
        dst_of(p)[...] = src_of(p)[...]
        plane_wait(xt.at[it, :, :, 0:1920], xid, xid_s)

        mark("f_left")
        peaks = []

        def put_trial(r, a, b):
            a, b = STEP * a, STEP * b
            if it:
                a, b = trial[0, r] + a, trial[1, r] + b
            trial[0, r] = a
            trial[1, r] = b
            peaks.append(jnp.max(jnp.sqrt(a * a + b * b)))

        forward(lambda part, q: xt[it, part, :, q * QUARTER : q * QUARTER + QUARTER].astype(F32), put_trial)
        peak = jnp.maximum(jnp.maximum(peaks[0], peaks[1]), jnp.maximum(peaks[2], peaks[3]))

        mark("stats")
        lane = lax.broadcasted_iota(jnp.int32, (1, 128), 1)
        st1[it] = jnp.where(lane < 64, peak, squares)
        sid, sid_s = ids(1), out_id()
        for k, (a, b, d) in enumerate(everyone):
            send(st1.at[it], sr1.at[it, k], sid_s, sid, dev(place(a, b), (g + d) % 4))
        sr1[it, 63] = st1[it]
        if it:
            mark("out_send")
            oid, oid_s = ids(1), out_id()
            for b in range(4):
                v = [trial[part, r, :, 128 * b : 128 * b + 128] for r in range(4) for part in range(2)]
                v = jnp.concatenate([jnp.concatenate(v[k::2], axis=1) for k in range(2)], axis=0)
                hi = v.astype(BF)
                rest = v - hi.astype(F32)
                mid = rest.astype(BF)
                low = (rest - mid.astype(F32)).astype(BF)
                order = perm[...]
                v = dot(hi, order) + dot(mid, order) + dot(low, order)
                cfo[0, :, 512 * b : 512 * b + 512] = v[:32]
                cfo[1, :, 512 * b : 512 * b + 512] = v[32:]
            out_src = lambda q: cfo.at[:, :, ds(128 * q, 128, 128)]
            out_dst = lambda q: ot.at[:, q]
            away = jnp.logical_and(c == 1, x != y)

            def out_copy(q):
                return rcopy(out_src(q), out_dst(p), oid_s, oid, chip(q // 4, q % 4, g, c))

            for a, b in offsets:
                out_copy(place(a, b)).start()

            @pl.when(away)
            def _():
                out_copy(p).start()

            @pl.when(jnp.logical_not(away))
            def _():
                out_dst(p)[...] = out_src(p)[...]

            mark("stats_wait")
        plane_wait(sr1.at[it, 0:63], sid, sid_s)
        found = sr1[it]
        both = jnp.where(lane < 64, jnp.max(found, axis=0), jnp.sum(found, axis=0))
        totals.append(jnp.max(jnp.where(lane < 64, 0.0, both)))
        mark("shrink")
        level = SHRINK * jnp.max(jnp.where(lane < 64, both, 0.0))

        def shrunk(a, b):
            size = jnp.sqrt(a * a + b * b)
            factor = jnp.maximum(1.0 - level / jnp.maximum(size, level), 0.0)
            return a * factor, b * factor

        if it == 0:
            for r in range(4):
                a, b = shrunk(trial[0, r], trial[1, r])
                trial[0, r] = a
                trial[1, r] = b
                cb[0, r] = a.astype(BF)
                cb[1, r] = b.astype(BF)

    mark("out_wait")
    nid, nid_s = ids(1), out_id()
    for it in range(2):
        nt[it] = jnp.sqrt(jnp.full((1, 128), totals[it], F32))
    send(nt, nr, nid_s, nid, partner)

    @pl.when(away)
    def _():
        rcopy(ot, ot, oid_s, oid, partner).wait_recv()

    @pl.when(jnp.logical_not(away))
    def _():
        rcopy(ot.at[:, 0:15], ot.at[:, 0:15], oid_s, oid, partner).wait_recv()

    mark("out_turn")
    for b in range(4):
        for r in range(4):
            a, d = shrunk(ot[0, 4 * b + r], ot[1, 4 * b + r])
            nat[0, b, pl.ds(r, 32, stride=4), :] = a
            nat[1, b, pl.ds(r, 32, stride=4), :] = d
    halves, halves_s = ids(1), out_id()

    def turned(part, half):
        return jnp.concatenate([nat[part, 2 * half + k].T for k in range(2)], axis=1)

    for part in range(2):
        keep[part] = turned(part, 1 - c)
    send(keep, got, halves_s, halves, partner)
    for part in range(2):
        out[c, part] = turned(part, c)
    mark("out_swap")
    arrived(nr, nid)
    for it in range(2):
        norms[it, c] = jnp.max(nt[it])
        norms[it, 1 - c] = jnp.max(nr[it])
    arrived(got, halves)
    out[1 - c] = got[...]
    for copy in pending:
        copy.wait_send()
    rcopy(nt, nt, nid_s, nid, partner).wait_send()
    rcopy(keep, keep, halves_s, halves, partner).wait_send()

    @pl.when(away)
    def _():
        rcopy(ot, ot, oid_s, oid, partner).wait_send()

    @pl.when(jnp.logical_not(away))
    def _():
        rcopy(ot.at[:, 0:15], ot.at[:, 0:15], oid_s, oid, partner).wait_send()

    @pl.when(jnp.logical_not(stays))
    def _():
        to_second.wait_send()

    @pl.when(c == 1)
    def _():
        to_first.wait_send()

    assert used == [RECEIVES, SENDS], used
    mark(None)


def scratch():
    v = lambda *shape, t=BF: pltpu.VMEM(shape, t)
    return [
        v(2, 2, 128, 256), *[v(*a.shape, t=F32) for a in table_parts()],
        v(2, N, 512), v(QUARTER, N), v(QUARTER, N), v(N, QUARTER), v(N, QUARTER), v(512, 512),
        v(2, N, 128, t=F32), v(4, QUARTER, 256), v(2, 4, QUARTER, 128, t=F32),
        v(2, 2, 4, QUARTER, 128), v(2, 4, 128, 128), v(2, 4, 128, 128), v(2, 4, 128, 128),
        v(2, 4, 128, 128), v(2, 2, 4, 128, 128), v(2, 2, 4, 128, 128), v(4, 2, 32, QUARTER),
        v(2, 2, 4, 128, 128), v(2, 2, 32, N),
        v(2, 4, 32, QUARTER, t=F32), v(2, 32, N, t=F32), v(2, 4, 32, QUARTER),
        v(2, 32, N), v(2, 4, 128, 128), v(2, 4, 128, QUARTER), v(2, 128, N), v(2, 128, 512),
        v(2, 16, 32, 128, t=F32), v(2, 4, 128, 128, t=F32),
        v(2, 128, 256, t=F32), v(2, 128, 256, t=F32),
        v(2, 1, 128, t=F32), v(2, 64, 1, 128, t=F32),
        v(2, 1, 128, t=F32), v(2, 1, 128, t=F32),
        pltpu.SemaphoreType.DMA((SENDS,)), pltpu.SemaphoreType.DMA((RECEIVES,)),
        pltpu.SemaphoreType.DMA((9,)),
    ]


def hand_on(a, b, out, norms):
    out[...] = a[...]
    for i in range(2):
        for j in range(2):
            norms[i, j] = b[i, j]


def per_device(traces, wavelet):
    vm = pl.BlockSpec(memory_space=pltpu.VMEM)
    sm = pl.BlockSpec(memory_space=pltpu.SMEM)
    hbm = pl.BlockSpec(memory_space=pl.ANY)
    shapes = (jax.ShapeDtypeStruct((2, 2, 128, 256), F32), jax.ShapeDtypeStruct((2, 2), F32))
    parts = pl.pallas_call(
        kernel,
        out_shape=shapes,
        in_specs=[hbm, sm] + [hbm] * 8,
        out_specs=(vm, sm),
        scratch_shapes=scratch(),
        compiler_params=pltpu.CompilerParams(
            collective_id=0, has_side_effects=True, vmem_limit_bytes=60 * 1024 * 1024
        ),
        name="whole",
    )(traces, wavelet, *table_parts())
    return pl.pallas_call(
        hand_on, out_shape=shapes, in_specs=[vm, sm], out_specs=(vm, sm), name="hand_on"
    )(*parts)


def solution(mesh):
    return jax.shard_map(
        per_device,
        mesh=mesh,
        in_specs=(P(None, None, "src", "rcv"), P()),
        out_specs=(P(None, None, "src", "rcv"), P()),
        check_vma=False,
    )
```

```python
import functools
import math

import jax
import jax.numpy as jnp
import numpy as np
from jax import lax
from jax.experimental import pallas as pl
from jax.experimental.pallas import tpu as pltpu
from jax.sharding import PartitionSpec as P

MESH = pl.DeviceIdType.MESH
N = 2048
BASE = 32
RECEIVES = 90
SENDS = 14
QUARTER = N // 4
STEP = 0.4
SHRINK = 0.2
BF = jnp.bfloat16
F32 = jnp.float32


def table_parts():
    def both(left, right, scale):
        angle = 2.0 * math.pi * ((left[:, None] * right[None, :]) % N) / N
        return [(f(angle) * scale).astype(np.float32) for f in (np.cos, np.sin)]

    scale = 1.0 / math.sqrt(N)
    quarter = np.arange(QUARTER)
    residue = np.arange(4)
    order = (4 * quarter[None, :] + residue[:, None]).reshape(-1)
    first = (4 * np.arange(BASE)[None, :] + residue[:, None]).reshape(-1)
    later = BASE * np.arange(QUARTER // BASE)
    return [
        *both(np.arange(BASE), order, scale), *both(later, order, 1.0),
        *both(first, quarter, scale), *both(4 * later, quarter, 1.0),
    ]


def kernel(
    tr_any, wave, t0, t1, t2, t3, t4, t5, t6, t7, out, norms,
    tr, b0, b1, b2, b3, b4, b5, b6, b7,
    tf, tab_c, tab_s, inv_c, inv_s, perm, pg, ubt, tp, sb, ra, rb, qa, qb, dl, dr, ub, zt, xt,
    trial, cfo, cb, hb, wt, hh, mb, mf, ot, nat, keep, got, st1, sr1, nt, nr,
    ssem, rsem, lsem,
):
    tables_any = (t0, t1, t2, t3, t4, t5, t6, t7)
    tables = (b0, b1, b2, b3, b4, b5, b6, b7)
    src = lax.axis_index("src")
    rcv = lax.axis_index("rcv")
    y = rcv // 2
    c = rcv % 2
    z = src // 4
    x = src % 4
    lane2 = (1 - c) * x + c * y
    g = (1 - c) * y + c * x
    p = z * 4 + lane2
    used = [0, 0]
    pending = []

    stage = [None]

    def mark(name):
        if stage[0] is not None:
            stage[0].__exit__(None, None, None)
        stage[0] = jax.named_scope(name) if name else None
        if name:
            stage[0].__enter__()

    def ids(n):
        used[0] += n
        return used[0] - n

    def out_id():
        used[1] += 1
        return used[1] - 1

    def chip(zz_, xx_, yy_, cc_):
        return (zz_ * 4 + xx_, yy_ * 2 + cc_)

    def dev(q, gg):
        second = q % 4
        return chip(q // 4, (1 - c) * second + c * gg, (1 - c) * gg + c * second, c)

    partner = chip(z, x, y, 1 - c)

    def rcopy(src, dst, s_id, r_id, where):
        return pltpu.make_async_remote_copy(
            src_ref=src, dst_ref=dst, send_sem=ssem.at[s_id], recv_sem=rsem.at[r_id],
            device_id=where, device_id_type=MESH,
        )

    def send(src, dst, s_id, r_id, where):
        rcopy(src, dst, s_id, r_id, where).start()

    def arrived(ref, r_id):
        rcopy(ref, ref, 0, r_id, partner).wait_recv()

    def sent(ref, s_id):
        pending.append(rcopy(ref, ref, s_id, 0, partner))

    def ds(start, size, unit):
        return pl.ds(pl.multiple_of(start, unit), size)

    mark("entry")
    fetched = [
        pltpu.make_async_copy(a, b, lsem.at[k])
        for k, (a, b) in enumerate(zip((tr_any, *tables_any), (tr, *tables)))
    ]
    for copy in fetched:
        copy.start()
    base_c, base_s, mul_c, mul_s, ibase_c, ibase_s, imul_c, imul_s = tables
    barrier = pltpu.get_barrier_semaphore()

    def greet(where):
        pl.semaphore_signal(barrier, inc=1, device_id=where, device_id_type=MESH)

    greet(partner)
    for d in (1, 2, 3):
        greet(dev(p, (g + d) % 4))
    for d in (1, 3):
        greet(dev((z + d) % 4 * 4 + lane2, g))
        greet(dev(z * 4 + (lane2 + d) % 4, g))
    crossed = jnp.logical_and(c == 1, x != y)

    @pl.when(crossed)
    def _():
        greet(chip(z, y, x, 0))
        greet(chip(z, y, x, 1))

    @pl.when(x != y)
    def _():
        pl.semaphore_wait(barrier, 9)

    @pl.when(x == y)
    def _():
        pl.semaphore_wait(barrier, 8)

    mark("swap")
    own_rows = ds(128 * p, 128, 128)
    fetched[0].wait()
    swap, swap_s = ids(2), [out_id(), out_id()]
    landing = tf.at[:, ds(128 * src, 128, 128), ds(256 * c, 256, 256)]
    to_first = rcopy(tr.at[0], landing, swap_s[0], swap + c, chip(z, x, y, 0))
    to_second = rcopy(tr.at[1], landing, swap_s[1], swap + c, chip(z, y, x, 1))
    stays = jnp.logical_and(c == 1, x == y)

    @pl.when(jnp.logical_not(stays))
    def _():
        to_second.start()

    @pl.when(c == 1)
    def _():
        to_first.start()

    @pl.when(c == 0)
    def _():
        landing[...] = tr[0]

    @pl.when(stays)
    def _():
        landing[...] = tr[1]

    @pl.when(c == 1)
    def _():
        arrived(tf.at[:, own_rows, 0:256], swap)

    @pl.when(jnp.logical_not(stays))
    def _():
        arrived(tf.at[:, own_rows, 256:512], swap + 1)

    root = 1.0 / math.sqrt(N)
    wr = wave[c, 0] * root
    wi = wave[c, 1] * root

    def dot(a, b):
        return lax.dot_general(a, b, (((1,), (0,)), ((), ())), preferred_element_type=F32)

    def dot_nt(a, b):
        return lax.dot_general(a, b, (((1,), (1,)), ((), ())), preferred_element_type=F32)

    def back_rows(n):
        errors = mf[...].reshape(256, 512)
        here = ds(n * 512, 512, 512)
        a, b = dot_nt(tf[0, here, :], errors), dot_nt(tf[1, here, :], errors)
        br, bi = a[:, :128] + b[:, 128:], a[:, 128:] - b[:, :128]
        pg[0, here, :] = -(wr * br + wi * bi)
        pg[1, here, :] = -(wr * bi - wi * br)

    def back_start():
        for part in range(2):
            mf[part] = tf[part, own_rows, :]

    def shift(at, axis, d):
        zz_, xx_ = at
        return (zz_ + (1 - axis) * d + 4) % 4, (xx_ + axis * d + 4) % 4

    def neighbour(axis, d):
        a, b = shift((z, lane2), axis, d)
        return dev(a * 4 + b, g)

    def block(at, kind, part=None):
        start = (at[0] * 4 + at[1]) * 128 + 32 * kind
        if part is not None:
            return tf.at[:, ds(start + 16 * part, 16, 16), :]
        return tf.at[:, ds(start, 32, 16), :]

    gather_s = out_id()

    def ag_start(at, axis, half):
        r_id = ids(3)
        send(block(at, half), block(at, half), gather_s, r_id, neighbour(axis, 1))
        send(block(at, half), block(at, half), gather_s, r_id + 1, neighbour(axis, -1))
        return at, axis, half, r_id

    def ag_forward(item):
        at, axis, half, r_id = item
        left, right = shift(at, axis, -1), shift(at, axis, 1)
        arrived(block(left, half), r_id)
        send(block(left, half, 0), block(left, half, 0), gather_s, r_id + 2, neighbour(axis, 1))
        arrived(block(right, half), r_id + 1)
        send(block(right, half, 1), block(right, half, 1), gather_s, r_id + 2, neighbour(axis, -1))

    def ag_finish(item):
        at, axis, half, r_id = item
        arrived(block(shift(at, axis, 2), half), r_id + 2)

    def make_table(first, last):
        @pl.loop(first, last)
        def _(m):
            rows = ds(m * BASE, BASE, BASE)
            for col in range(0, N, 512):
                here = pl.ds(col, 512)
                bc, bs = base_c[:, here], base_s[:, here]
                mc, ms = mul_c[pl.ds(m, 1), here], mul_s[pl.ds(m, 1), here]
                tab_c[rows, here] = (bc * mc - bs * ms).astype(BF)
                tab_s[rows, here] = (bs * mc + bc * ms).astype(BF)
            mc, ms = imul_c[pl.ds(m, 1), :], imul_s[pl.ds(m, 1), :]
            for r in range(4):
                bc, bs = ibase_c[r * BASE : r * BASE + BASE], ibase_s[r * BASE : r * BASE + BASE]
                rows = ds(r * QUARTER + m * BASE, BASE, BASE)
                inv_c[rows, :] = (bc * mc - bs * ms).astype(BF)
                inv_s[rows, :] = (bs * mc + bc * ms).astype(BF)

    def make_order():
        row = lax.broadcasted_iota(jnp.int32, (512, 512), 0)
        col = lax.broadcasted_iota(jnp.int32, (512, 512), 1)
        perm[...] = jnp.where(col == 4 * (row % 128) + row // 128, 1.0, 0.0).astype(BF)

    mark("gather_a")
    home = (z, lane2)
    kinds = (0, 1, 2, 3)
    first_axis = (0, 0, 1, 0)
    first, own = {}, {}
    for k in (0, 2, 1, 3):
        first[k] = ag_start(home, first_axis[k], k)
    for k in (0, 2, 1, 3):
        own[k] = ag_start(home, 1 - first_axis[k], k)
    for copy in fetched[1:]:
        copy.wait()
    make_table(0, 16)
    make_order()
    mark("gather_b")
    near = {}

    def pass_on(k, hops):
        near[k, hops] = [ag_start(shift(home, first_axis[k], d), 1 - first_axis[k], k) for d in hops]

    for k in (0, 2, 1, 3):
        ag_forward(first[k])
    for k in (0, 2, 1, 3):
        pass_on(k, (-1, 1))
        ag_forward(own[k])
    for k in (0, 2, 1, 3):
        ag_finish(first[k])
        pass_on(k, (2,))
    mark("gather_c")
    for k in (0, 2, 1, 3):
        for item in near[k, (-1, 1)]:
            ag_forward(item)
    for k in kinds:
        ag_finish(own[k])
    mark("gather_back")
    back_start()
    back_rows(z)
    mark("gather_d")
    for k in (0, 2, 1, 3):
        ag_forward(near[k, (2,)][0])
    for k in kinds:
        for item in near[k, (-1, 1)]:
            ag_finish(item)
    mark("gather_back")
    back_rows((z + 3) % 4)
    back_rows((z + 1) % 4)
    mark("gather_e")
    for k in kinds:
        ag_finish(near[k, (2,)][0])
    sent(tf.at[:, 0:1920, :], gather_s)
    mark("gather_back")
    back_rows((z + 2) % 4)

    def quarters(load, ub):
        x = [[load(part, q) for part in range(2)] for q in range(4)]
        plus = [[x[h][k] + x[h + 2][k] for k in range(2)] for h in range(2)]
        less = [[x[h][k] - x[h + 2][k] for k in range(2)] for h in range(2)]
        for k in range(2):
            ub(0, k)[...] = (plus[0][k] + plus[1][k]).astype(BF)
            ub(2, k)[...] = (plus[0][k] - plus[1][k]).astype(BF)
        ub(1, 0)[...] = (less[0][0] + less[1][1]).astype(BF)
        ub(1, 1)[...] = (less[0][1] - less[1][0]).astype(BF)
        ub(3, 0)[...] = (less[0][0] - less[1][1]).astype(BF)
        ub(3, 1)[...] = (less[0][1] + less[1][0]).astype(BF)

    def forward(load, store):
        quarters(load, lambda r, part: ub.at[r, part])
        for r in range(4):
            rows = ub[r].reshape(64, QUARTER)
            here = pl.ds(r * QUARTER, QUARTER)
            a, b = dot(rows, tab_c[:, here]), dot(rows, tab_s[:, here])
            store(r, a[:32] + b[32:], a[32:] - b[:32])

    def inverse(load, half, store):
        for col in range(0, QUARTER, 256):
            e = []
            for r in range(4):
                rows = load(r)
                there = pl.ds(r * QUARTER, QUARTER)
                a = dot(rows, inv_c[there, col : col + 256])
                b = dot(rows, inv_s[there, col : col + 256])
                e.append((a[:half] - b[half:], b[:half] + a[half:]))
            plus = [[e[h][k] + e[h + 2][k] for k in range(2)] for h in range(2)]
            less = [[e[h][k] - e[h + 2][k] for k in range(2)] for h in range(2)]
            store(col, plus[0][0] + plus[1][0], plus[0][1] + plus[1][1])
            store(QUARTER + col, less[0][0] - less[1][1], less[0][1] + less[1][0])
            store(2 * QUARTER + col, plus[0][0] - plus[1][0], plus[0][1] - plus[1][1])
            store(3 * QUARTER + col, less[0][0] + less[1][1], less[0][1] - less[1][0])

    def residue(ref, q):
        return ref.at[:, q % 4, ds(32 * (q // 4), 32, 32), :]

    offsets = [(a, b) for a in range(4) for b in range(4) if a or b]
    offsets.sort(key=lambda o: -(min(o[0], 4 - o[0]) + min(o[1], 4 - o[1])))

    everyone = [(a, b, d) for a in range(4) for b in range(4) for d in range(4) if a or b or d]
    everyone.sort(key=lambda o: -sum(min(i, 4 - i) for i in o))

    def place(a, b):
        return (z + a) % 4 * 4 + (lane2 + b) % 4

    def plane_exchange(source, landing, r_id, s_id):
        for a, b in offsets:
            q = place(a, b)
            rcopy(source(q), landing(p), s_id, r_id, dev(q, g)).start()

    def plane_wait(others, r_id, s_id):
        arrived(others, r_id)
        sent(others, s_id)

    totals = []
    for it in range(2):
        if it == 0:
            ref, imf = mf[0].astype(F32), mf[1].astype(F32)
            squares = jnp.sum(ref * ref + imf * imf)
        else:
            mark("g_left")
            def put_half(col, a, b):
                hb[0, :, col : col + 256] = a.astype(BF)
                hb[1, :, col : col + 256] = b.astype(BF)

            inverse(lambda r: cb[:, r].reshape(64, QUARTER), 32, put_half)

            mark("g_plane")
            wid, wid_s = ids(1), out_id()
            src_of = lambda q: hb.at[:, :, ds(128 * q, 128, 128)]
            dst_of = lambda q: residue(wt, q)
            plane_exchange(src_of, dst_of, wid, wid_s)
            residue(wt, p)[...] = hb[:, :, ds(128 * p, 128, 128)]
            plane_wait(hb.at[:, :, 0:1920], wid, wid_s)
            for part in range(2):
                for r in range(4):
                    hh[part, r, :, ds(128 * g, 128, 128)] = wt[part, r].astype(F32).T.astype(BF)
            mark("g_gather")
            gid, gid_s = ids(8), out_id()

            def held(gg, part, h=None):
                which = slice(None) if h is None else pl.ds(2 * h, 2)
                return hh.at[part, which, :, ds(128 * gg, 128, 128)]

            up, down, far = (g + 1) % 4, (g + 3) % 4, (g + 2) % 4

            def pass_held(gg, part, h, r_id, to):
                send(held(gg, part, h), held(gg, part, h), gid_s, gid + r_id, dev(p, to))

            for h in range(2):
                pass_held(g, 0, h, h, up)
                pass_held(g, 1, h, 2 + h, down)
            pass_held(g, 1, None, 4, up)
            pass_held(g, 0, None, 5, down)
            for h in range(2):
                arrived(held(down, 0, h), gid + h)
                pass_held(down, 0, h, 6, up)
                arrived(held(up, 1, h), gid + 2 + h)
                pass_held(up, 1, h, 7, down)
            arrived(held(down, 1), gid + 4)
            arrived(held(up, 0), gid + 5)
            arrived(held(far, 0), gid + 6)
            arrived(held(far, 1), gid + 7)
            sent(hh.at[:, 0:3], gid_s)

            mark("g_right")
            def put_model(col, a, b):
                mb[0, :, col : col + 256] = a.astype(BF)
                mb[1, :, col : col + 256] = b.astype(BF)

            inverse(lambda r: hh[:, r].reshape(256, QUARTER), 128, put_model)

            mark("misfit")
            squares = 0.0
            for n in range(2):
                rows = mb[...].reshape(256, N)
                some = pl.ds(n * 256, 256)
                a, b = dot(rows, tf[0, :, some]), dot(rows, tf[1, :, some])
                pr, pi = a[:128] - b[128:], b[:128] + a[128:]
                here = ds(512 * g + n * 256, 256, 256)
                mr = tf[0, own_rows, some].astype(F32) - mb[0, :, here].astype(F32)
                mi = tf[1, own_rows, some].astype(F32) - mb[1, :, here].astype(F32)
                mr = mr + (wr * pr - wi * pi)
                mi = mi + (wr * pi + wi * pr)
                squares = squares + jnp.sum(mr * mr + mi * mi)
                mf[0, :, n * 256 : n * 256 + 256] = mr.astype(BF)
                mf[1, :, n * 256 : n * 256 + 256] = mi.astype(BF)

        if it:
            mark("back")

            @pl.loop(0, 4)
            def _(n):
                back_rows(n)

        mine = ds(512 * g, 512, 512)
        for part in range(2):
            pg[part, mine, :] = pg[part, mine, :] + mf[part].astype(F32).T

        mark("f_right")
        quarters(
            lambda part, q: pg[part, q * QUARTER : q * QUARTER + QUARTER, :],
            lambda r, part: ubt.at[r, :, pl.ds(128 * part, 128)],
        )
        up, down, far = (g + 1) % 4, (g + 3) % 4, (g + 2) % 4
        rid, rid_s = ids(6), out_id()

        def piece(ref, gg, h, part):
            return ref.at[it, part, pl.ds(2 * h, 2), ds(128 * gg, 128, 128), :]

        def slot(ref, h, *part):
            return ref.at[(it, *part, pl.ds(2 * h, 2))]

        for r in range(4):
            there = pl.ds(r * QUARTER, QUARTER)
            a, b = dot(inv_c[there, :], ubt[r]), dot(inv_s[there, :], ubt[r])
            tr_, ti_ = a[:, :128] + b[:, 128:], a[:, 128:] - b[:, :128]
            tp[0, r] = tr_
            tp[1, r] = ti_
            sb[it, 0, r] = tr_.astype(BF)
            sb[it, 1, r] = ti_.astype(BF)
            if r % 2:
                h = r // 2
                send(piece(sb, far, h, 0), slot(ra, h), rid_s, rid + h, dev(p, up))
                send(piece(sb, far, h, 1), slot(rb, h), rid_s, rid + 2 + h, dev(p, down))

        mark("scatter")
        for h in range(2):
            send(piece(sb, up, h, 1), slot(dl, h, 1), rid_s, rid + 4, dev(p, up))
            send(piece(sb, down, h, 0), slot(dr, h, 0), rid_s, rid + 5, dev(p, down))
        for h in range(2):
            pair = pl.ds(2 * h, 2)
            arrived(slot(ra, h), rid + h)
            qa[it, pair] = (tp[0, pair, ds(128 * up, 128, 128), :] + ra[it, pair].astype(F32)).astype(BF)
            send(slot(qa, h), slot(dl, h, 0), rid_s, rid + 4, dev(p, up))
            arrived(slot(rb, h), rid + 2 + h)
            qb[it, pair] = (tp[1, pair, ds(128 * down, 128, 128), :] + rb[it, pair].astype(F32)).astype(BF)
            send(slot(qb, h), slot(dr, h, 1), rid_s, rid + 5, dev(p, down))
        arrived(dl.at[it], rid + 4)
        arrived(dr.at[it], rid + 5)
        sent(sb.at[it, :, 0:3], rid_s)
        total = tp[:, :, ds(128 * g, 128, 128), :] + dl[it].astype(F32)
        zt[it] = (total + dr[it].astype(F32)).astype(BF)
        mark("f_plane")
        xid, xid_s = ids(1), out_id()
        src_of = lambda q: residue(zt.at[it], q)
        dst_of = lambda q: xt.at[it, :, :, ds(128 * q, 128, 128)]
        plane_exchange(src_of, dst_of, xid, xid_s)
        dst_of(p)[...] = src_of(p)[...]
        plane_wait(xt.at[it, :, :, 0:1920], xid, xid_s)

        mark("f_left")
        peaks = []

        def put_trial(r, a, b):
            a, b = STEP * a, STEP * b
            if it:
                a, b = trial[0, r] + a, trial[1, r] + b
            trial[0, r] = a
            trial[1, r] = b
            peaks.append(jnp.max(jnp.sqrt(a * a + b * b)))

        forward(lambda part, q: xt[it, part, :, q * QUARTER : q * QUARTER + QUARTER].astype(F32), put_trial)
        peak = jnp.maximum(jnp.maximum(peaks[0], peaks[1]), jnp.maximum(peaks[2], peaks[3]))

        mark("stats")
        lane = lax.broadcasted_iota(jnp.int32, (1, 128), 1)
        st1[it] = jnp.where(lane < 64, peak, squares)
        sid, sid_s = ids(1), out_id()
        for k, (a, b, d) in enumerate(everyone):
            send(st1.at[it], sr1.at[it, k], sid_s, sid, dev(place(a, b), (g + d) % 4))
        sr1[it, 63] = st1[it]
        if it:
            mark("out_send")
            oid, oid_s = ids(1), out_id()
            for b in range(4):
                v = [trial[part, r, :, 128 * b : 128 * b + 128] for r in range(4) for part in range(2)]
                v = jnp.concatenate([jnp.concatenate(v[k::2], axis=1) for k in range(2)], axis=0)
                hi = v.astype(BF)
                rest = v - hi.astype(F32)
                mid = rest.astype(BF)
                low = (rest - mid.astype(F32)).astype(BF)
                order = perm[...]
                v = dot(hi, order) + dot(mid, order) + dot(low, order)
                cfo[0, :, 512 * b : 512 * b + 512] = v[:32]
                cfo[1, :, 512 * b : 512 * b + 512] = v[32:]
            out_src = lambda q: cfo.at[:, :, ds(128 * q, 128, 128)]
            out_dst = lambda q: ot.at[:, q]
            away = jnp.logical_and(c == 1, x != y)

            def out_copy(q):
                return rcopy(out_src(q), out_dst(p), oid_s, oid, chip(q // 4, q % 4, g, c))

            for a, b in offsets:
                out_copy(place(a, b)).start()

            @pl.when(away)
            def _():
                out_copy(p).start()

            @pl.when(jnp.logical_not(away))
            def _():
                out_dst(p)[...] = out_src(p)[...]

            mark("stats_wait")
        plane_wait(sr1.at[it, 0:63], sid, sid_s)
        found = sr1[it]
        both = jnp.where(lane < 64, jnp.max(found, axis=0), jnp.sum(found, axis=0))
        totals.append(jnp.max(jnp.where(lane < 64, 0.0, both)))
        mark("shrink")
        level = SHRINK * jnp.max(jnp.where(lane < 64, both, 0.0))

        def shrunk(a, b):
            size = jnp.sqrt(a * a + b * b)
            factor = jnp.maximum(1.0 - level / jnp.maximum(size, level), 0.0)
            return a * factor, b * factor

        if it == 0:
            for r in range(4):
                a, b = shrunk(trial[0, r], trial[1, r])
                trial[0, r] = a
                trial[1, r] = b
                cb[0, r] = a.astype(BF)
                cb[1, r] = b.astype(BF)

    mark("out_wait")
    nid, nid_s = ids(1), out_id()
    for it in range(2):
        nt[it] = jnp.sqrt(jnp.full((1, 128), totals[it], F32))
    send(nt, nr, nid_s, nid, partner)

    @pl.when(away)
    def _():
        rcopy(ot, ot, oid_s, oid, partner).wait_recv()

    @pl.when(jnp.logical_not(away))
    def _():
        rcopy(ot.at[:, 0:15], ot.at[:, 0:15], oid_s, oid, partner).wait_recv()

    mark("out_turn")
    for b in range(4):
        for r in range(4):
            a, d = shrunk(ot[0, 4 * b + r], ot[1, 4 * b + r])
            nat[0, b, pl.ds(r, 32, stride=4), :] = a
            nat[1, b, pl.ds(r, 32, stride=4), :] = d
    halves, halves_s = ids(1), out_id()

    def turned(part, half):
        return jnp.concatenate([nat[part, 2 * half + k].T for k in range(2)], axis=1)

    for part in range(2):
        keep[part] = turned(part, 1 - c)
    send(keep, got, halves_s, halves, partner)
    for part in range(2):
        out[c, part] = turned(part, c)
    mark("out_swap")
    arrived(nr, nid)
    for it in range(2):
        norms[it, c] = jnp.max(nt[it])
        norms[it, 1 - c] = jnp.max(nr[it])
    arrived(got, halves)
    out[1 - c] = got[...]
    for copy in pending:
        copy.wait_send()
    rcopy(nt, nt, nid_s, nid, partner).wait_send()
    rcopy(keep, keep, halves_s, halves, partner).wait_send()

    @pl.when(away)
    def _():
        rcopy(ot, ot, oid_s, oid, partner).wait_send()

    @pl.when(jnp.logical_not(away))
    def _():
        rcopy(ot.at[:, 0:15], ot.at[:, 0:15], oid_s, oid, partner).wait_send()

    @pl.when(jnp.logical_not(stays))
    def _():
        to_second.wait_send()

    @pl.when(c == 1)
    def _():
        to_first.wait_send()

    assert used == [RECEIVES, SENDS], used
    mark(None)


def scratch():
    v = lambda *shape, t=BF: pltpu.VMEM(shape, t)
    return [
        v(2, 2, 128, 256), *[v(*a.shape, t=F32) for a in table_parts()],
        v(2, N, 512), v(QUARTER, N), v(QUARTER, N), v(N, QUARTER), v(N, QUARTER), v(512, 512),
        v(2, N, 128, t=F32), v(4, QUARTER, 256), v(2, 4, QUARTER, 128, t=F32),
        v(2, 2, 4, QUARTER, 128), v(2, 4, 128, 128), v(2, 4, 128, 128), v(2, 4, 128, 128),
        v(2, 4, 128, 128), v(2, 2, 4, 128, 128), v(2, 2, 4, 128, 128), v(4, 2, 32, QUARTER),
        v(2, 2, 4, 128, 128), v(2, 2, 32, N),
        v(2, 4, 32, QUARTER, t=F32), v(2, 32, N, t=F32), v(2, 4, 32, QUARTER),
        v(2, 32, N), v(2, 4, 128, 128), v(2, 4, 128, QUARTER), v(2, 128, N), v(2, 128, 512),
        v(2, 16, 32, 128, t=F32), v(2, 4, 128, 128, t=F32),
        v(2, 128, 256, t=F32), v(2, 128, 256, t=F32),
        v(2, 1, 128, t=F32), v(2, 64, 1, 128, t=F32),
        v(2, 1, 128, t=F32), v(2, 1, 128, t=F32),
        pltpu.SemaphoreType.DMA((SENDS,)), pltpu.SemaphoreType.DMA((RECEIVES,)),
        pltpu.SemaphoreType.DMA((9,)),
    ]


def hand_on(a, b, out, norms):
    out[...] = a[...]
    for i in range(2):
        for j in range(2):
            norms[i, j] = b[i, j]


def per_device(traces, wavelet):
    vm = pl.BlockSpec(memory_space=pltpu.VMEM)
    sm = pl.BlockSpec(memory_space=pltpu.SMEM)
    hbm = pl.BlockSpec(memory_space=pl.ANY)
    shapes = (jax.ShapeDtypeStruct((2, 2, 128, 256), F32), jax.ShapeDtypeStruct((2, 2), F32))
    parts = pl.pallas_call(
        kernel,
        out_shape=shapes,
        in_specs=[hbm, sm] + [hbm] * 8,
        out_specs=(vm, sm),
        scratch_shapes=scratch(),
        compiler_params=pltpu.CompilerParams(
            collective_id=0, has_side_effects=True, vmem_limit_bytes=60 * 1024 * 1024
        ),
        name="whole",
    )(traces, wavelet, *table_parts())
    return pl.pallas_call(
        hand_on, out_shape=shapes, in_specs=[vm, sm], out_specs=(vm, sm), name="hand_on"
    )(*parts)


def solution(mesh):
    return jax.shard_map(
        per_device,
        mesh=mesh,
        in_specs=(P(None, None, "src", "rcv"), P()),
        out_specs=(P(None, None, "src", "rcv"), P()),
        check_vma=False,
    )
```

```python
import functools
import math

import jax
import jax.numpy as jnp
import numpy as np
from jax import lax
from jax.experimental import pallas as pl
from jax.experimental.pallas import tpu as pltpu
from jax.sharding import PartitionSpec as P

MESH = pl.DeviceIdType.MESH
N = 2048
BASE = 32
RECEIVES = 102
SENDS = 14
QUARTER = N // 4
STEP = 0.4
SHRINK = 0.2
BF = jnp.bfloat16
F32 = jnp.float32


def table_parts():
    def both(left, right, scale):
        angle = 2.0 * math.pi * ((left[:, None] * right[None, :]) % N) / N
        return [(f(angle) * scale).astype(np.float32) for f in (np.cos, np.sin)]

    scale = 1.0 / math.sqrt(N)
    quarter = np.arange(QUARTER)
    residue = np.arange(4)
    order = (4 * quarter[None, :] + residue[:, None]).reshape(-1)
    first = (4 * np.arange(BASE)[None, :] + residue[:, None]).reshape(-1)
    later = BASE * np.arange(QUARTER // BASE)
    return [
        *both(np.arange(BASE), order, scale), *both(later, order, 1.0),
        *both(first, quarter, scale), *both(4 * later, quarter, 1.0),
    ]


def kernel(
    tr_any, wave, t0, t1, t2, t3, t4, t5, t6, t7, out, norms,
    tr, b0, b1, b2, b3, b4, b5, b6, b7,
    tf, tab_c, tab_s, inv_c, inv_s, perm, pg, ubt, tp, sb, ra, rb, qa, qb, dl, dr, ub, zt, xt,
    trial, cfo, cb, hb, wt, hh, mb, mf, ot, nat, keep, got, st1, sr1, nt, nr,
    ssem, rsem, lsem,
):
    tables_any = (t0, t1, t2, t3, t4, t5, t6, t7)
    tables = (b0, b1, b2, b3, b4, b5, b6, b7)
    src = lax.axis_index("src")
    rcv = lax.axis_index("rcv")
    y = rcv // 2
    c = rcv % 2
    z = src // 4
    x = src % 4
    lane2 = (1 - c) * x + c * y
    g = (1 - c) * y + c * x
    p = z * 4 + lane2
    used = [0, 0]
    pending = []

    stage = [None]

    def mark(name):
        if stage[0] is not None:
            stage[0].__exit__(None, None, None)
        stage[0] = jax.named_scope(name) if name else None
        if name:
            stage[0].__enter__()

    def ids(n):
        used[0] += n
        return used[0] - n

    def out_id():
        used[1] += 1
        return used[1] - 1

    def chip(zz_, xx_, yy_, cc_):
        return (zz_ * 4 + xx_, yy_ * 2 + cc_)

    def dev(q, gg):
        second = q % 4
        return chip(q // 4, (1 - c) * second + c * gg, (1 - c) * gg + c * second, c)

    partner = chip(z, x, y, 1 - c)

    def rcopy(src, dst, s_id, r_id, where):
        return pltpu.make_async_remote_copy(
            src_ref=src, dst_ref=dst, send_sem=ssem.at[s_id], recv_sem=rsem.at[r_id],
            device_id=where, device_id_type=MESH,
        )

    def send(src, dst, s_id, r_id, where):
        rcopy(src, dst, s_id, r_id, where).start()

    def arrived(ref, r_id):
        rcopy(ref, ref, 0, r_id, partner).wait_recv()

    def sent(ref, s_id):
        pending.append(rcopy(ref, ref, s_id, 0, partner))

    def ds(start, size, unit):
        return pl.ds(pl.multiple_of(start, unit), size)

    mark("entry")
    fetched = [
        pltpu.make_async_copy(a, b, lsem.at[k])
        for k, (a, b) in enumerate(zip((tr_any, *tables_any), (tr, *tables)))
    ]
    for copy in fetched:
        copy.start()
    base_c, base_s, mul_c, mul_s, ibase_c, ibase_s, imul_c, imul_s = tables
    barrier = pltpu.get_barrier_semaphore()

    def greet(where):
        pl.semaphore_signal(barrier, inc=1, device_id=where, device_id_type=MESH)

    greet(partner)
    for d in (1, 2, 3):
        greet(dev(p, (g + d) % 4))
    for d in (1, 3):
        greet(dev((z + d) % 4 * 4 + lane2, g))
        greet(dev(z * 4 + (lane2 + d) % 4, g))
    crossed = jnp.logical_and(c == 1, x != y)

    @pl.when(crossed)
    def _():
        greet(chip(z, y, x, 0))
        greet(chip(z, y, x, 1))

    @pl.when(x != y)
    def _():
        pl.semaphore_wait(barrier, 9)

    @pl.when(x == y)
    def _():
        pl.semaphore_wait(barrier, 8)

    mark("swap")
    own_rows = ds(128 * p, 128, 128)
    fetched[0].wait()
    swap, swap_s = ids(2), [out_id(), out_id()]
    landing = tf.at[:, ds(128 * src, 128, 128), ds(256 * c, 256, 256)]
    to_first = rcopy(tr.at[0], landing, swap_s[0], swap + c, chip(z, x, y, 0))
    to_second = rcopy(tr.at[1], landing, swap_s[1], swap + c, chip(z, y, x, 1))
    stays = jnp.logical_and(c == 1, x == y)

    @pl.when(jnp.logical_not(stays))
    def _():
        to_second.start()

    @pl.when(c == 1)
    def _():
        to_first.start()

    @pl.when(c == 0)
    def _():
        landing[...] = tr[0]

    @pl.when(stays)
    def _():
        landing[...] = tr[1]

    @pl.when(c == 1)
    def _():
        arrived(tf.at[:, own_rows, 0:256], swap)

    @pl.when(jnp.logical_not(stays))
    def _():
        arrived(tf.at[:, own_rows, 256:512], swap + 1)

    root = 1.0 / math.sqrt(N)
    wr = wave[c, 0] * root
    wi = wave[c, 1] * root

    def dot(a, b):
        return lax.dot_general(a, b, (((1,), (0,)), ((), ())), preferred_element_type=F32)

    def dot_nt(a, b):
        return lax.dot_general(a, b, (((1,), (1,)), ((), ())), preferred_element_type=F32)

    def back_rows(n):
        errors = mf[...].reshape(256, 512)
        here = ds(n * 512, 512, 512)
        a, b = dot_nt(tf[0, here, :], errors), dot_nt(tf[1, here, :], errors)
        br, bi = a[:, :128] + b[:, 128:], a[:, 128:] - b[:, :128]
        pg[0, here, :] = -(wr * br + wi * bi)
        pg[1, here, :] = -(wr * bi - wi * br)

    def back_start():
        for part in range(2):
            mf[part] = tf[part, own_rows, :]

    def shift(at, axis, d):
        zz_, xx_ = at
        return (zz_ + (1 - axis) * d + 4) % 4, (xx_ + axis * d + 4) % 4

    def neighbour(axis, d):
        a, b = shift((z, lane2), axis, d)
        return dev(a * 4 + b, g)

    def block(at, kind, part=None):
        start = (at[0] * 4 + at[1]) * 128 + 32 * kind
        if part is not None:
            return tf.at[:, ds(start + 16 * part, 16, 16), :]
        return tf.at[:, ds(start, 32, 16), :]

    gather_s = out_id()

    def ag_start(at, axis, half):
        r_id = ids(3)
        send(block(at, half), block(at, half), gather_s, r_id, neighbour(axis, 1))
        send(block(at, half), block(at, half), gather_s, r_id + 1, neighbour(axis, -1))
        return at, axis, half, r_id

    def ag_forward(item):
        at, axis, half, r_id = item
        left, right = shift(at, axis, -1), shift(at, axis, 1)
        arrived(block(left, half), r_id)
        send(block(left, half, 0), block(left, half, 0), gather_s, r_id + 2, neighbour(axis, 1))
        arrived(block(right, half), r_id + 1)
        send(block(right, half, 1), block(right, half, 1), gather_s, r_id + 2, neighbour(axis, -1))

    def ag_finish(item):
        at, axis, half, r_id = item
        arrived(block(shift(at, axis, 2), half), r_id + 2)

    def make_table(first, last):
        @pl.loop(first, last)
        def _(m):
            rows = ds(m * BASE, BASE, BASE)
            for col in range(0, N, 512):
                here = pl.ds(col, 512)
                bc, bs = base_c[:, here], base_s[:, here]
                mc, ms = mul_c[pl.ds(m, 1), here], mul_s[pl.ds(m, 1), here]
                tab_c[rows, here] = (bc * mc - bs * ms).astype(BF)
                tab_s[rows, here] = (bs * mc + bc * ms).astype(BF)
            mc, ms = imul_c[pl.ds(m, 1), :], imul_s[pl.ds(m, 1), :]
            for r in range(4):
                bc, bs = ibase_c[r * BASE : r * BASE + BASE], ibase_s[r * BASE : r * BASE + BASE]
                rows = ds(r * QUARTER + m * BASE, BASE, BASE)
                inv_c[rows, :] = (bc * mc - bs * ms).astype(BF)
                inv_s[rows, :] = (bs * mc + bc * ms).astype(BF)

    def make_order():
        row = lax.broadcasted_iota(jnp.int32, (512, 512), 0)
        col = lax.broadcasted_iota(jnp.int32, (512, 512), 1)
        perm[...] = jnp.where(col == 4 * (row % 128) + row // 128, 1.0, 0.0).astype(BF)

    mark("gather_a")
    home = (z, lane2)
    kinds = (0, 1, 2, 3)
    first_axis = (0, 0, 1, 0)
    first, own = {}, {}
    for k in (0, 2, 1, 3):
        first[k] = ag_start(home, first_axis[k], k)
    for k in (0, 2, 1, 3):
        own[k] = ag_start(home, 1 - first_axis[k], k)
    for copy in fetched[1:]:
        copy.wait()
    make_table(0, 16)
    make_order()
    mark("gather_b")
    near = {}

    def pass_on(k, hops):
        near[k, hops] = [ag_start(shift(home, first_axis[k], d), 1 - first_axis[k], k) for d in hops]

    for k in (0, 2, 1, 3):
        ag_forward(first[k])
    for k in (0, 2, 1, 3):
        pass_on(k, (-1, 1))
        ag_forward(own[k])
    for k in (0, 2, 1, 3):
        ag_finish(first[k])
        pass_on(k, (2,))
    mark("gather_c")
    for k in (0, 2, 1, 3):
        for item in near[k, (-1, 1)]:
            ag_forward(item)
    for k in kinds:
        ag_finish(own[k])
    mark("gather_back")
    back_start()
    back_rows(z)
    mark("gather_d")
    for k in (0, 2, 1, 3):
        ag_forward(near[k, (2,)][0])
    for k in kinds:
        for item in near[k, (-1, 1)]:
            ag_finish(item)
    mark("gather_back")
    back_rows((z + 3) % 4)
    back_rows((z + 1) % 4)
    mark("gather_e")
    for k in kinds:
        ag_finish(near[k, (2,)][0])
    sent(tf.at[:, 0:1920, :], gather_s)
    mark("gather_back")
    back_rows((z + 2) % 4)

    def quarters(load, ub):
        x = [[load(part, q) for part in range(2)] for q in range(4)]
        plus = [[x[h][k] + x[h + 2][k] for k in range(2)] for h in range(2)]
        less = [[x[h][k] - x[h + 2][k] for k in range(2)] for h in range(2)]
        for k in range(2):
            ub(0, k)[...] = (plus[0][k] + plus[1][k]).astype(BF)
            ub(2, k)[...] = (plus[0][k] - plus[1][k]).astype(BF)
        ub(1, 0)[...] = (less[0][0] + less[1][1]).astype(BF)
        ub(1, 1)[...] = (less[0][1] - less[1][0]).astype(BF)
        ub(3, 0)[...] = (less[0][0] - less[1][1]).astype(BF)
        ub(3, 1)[...] = (less[0][1] + less[1][0]).astype(BF)

    def forward(load, store):
        quarters(load, lambda r, part: ub.at[r, part])
        for r in range(4):
            rows = ub[r].reshape(64, QUARTER)
            here = pl.ds(r * QUARTER, QUARTER)
            a, b = dot(rows, tab_c[:, here]), dot(rows, tab_s[:, here])
            store(r, a[:32] + b[32:], a[32:] - b[:32])

    def inverse(load, half, store):
        for col in range(0, QUARTER, 256):
            e = []
            for r in range(4):
                rows = load(r)
                there = pl.ds(r * QUARTER, QUARTER)
                a = dot(rows, inv_c[there, col : col + 256])
                b = dot(rows, inv_s[there, col : col + 256])
                e.append((a[:half] - b[half:], b[:half] + a[half:]))
            plus = [[e[h][k] + e[h + 2][k] for k in range(2)] for h in range(2)]
            less = [[e[h][k] - e[h + 2][k] for k in range(2)] for h in range(2)]
            store(col, plus[0][0] + plus[1][0], plus[0][1] + plus[1][1])
            store(QUARTER + col, less[0][0] - less[1][1], less[0][1] + less[1][0])
            store(2 * QUARTER + col, plus[0][0] - plus[1][0], plus[0][1] - plus[1][1])
            store(3 * QUARTER + col, less[0][0] + less[1][1], less[0][1] - less[1][0])

    def residue(ref, q):
        return ref.at[:, q % 4, ds(32 * (q // 4), 32, 32), :]

    offsets = [(a, b) for a in range(4) for b in range(4) if a or b]
    offsets.sort(key=lambda o: -(min(o[0], 4 - o[0]) + min(o[1], 4 - o[1])))

    everyone = [(a, b, d) for a in range(4) for b in range(4) for d in range(4) if a or b or d]
    everyone.sort(key=lambda o: -sum(min(i, 4 - i) for i in o))

    def place(a, b):
        return (z + a) % 4 * 4 + (lane2 + b) % 4

    def plane_exchange(source, landing, r_id, s_id):
        for a, b in offsets:
            q = place(a, b)
            rcopy(source(q), landing(p), s_id, r_id, dev(q, g)).start()

    def plane_wait(others, r_id, s_id):
        arrived(others, r_id)
        sent(others, s_id)

    totals = []
    for it in range(2):
        if it == 0:
            ref, imf = mf[0].astype(F32), mf[1].astype(F32)
            squares = jnp.sum(ref * ref + imf * imf)
        else:
            mark("g_left")
            def put_half(col, a, b):
                hb[0, :, col : col + 256] = a.astype(BF)
                hb[1, :, col : col + 256] = b.astype(BF)

            inverse(lambda r: cb[:, r].reshape(64, QUARTER), 32, put_half)

            mark("g_plane")
            wid, wid_s = ids(1), out_id()
            src_of = lambda q: hb.at[:, :, ds(128 * q, 128, 128)]
            dst_of = lambda q: residue(wt, q)
            plane_exchange(src_of, dst_of, wid, wid_s)
            residue(wt, p)[...] = hb[:, :, ds(128 * p, 128, 128)]
            plane_wait(hb.at[:, :, 0:1920], wid, wid_s)
            for part in range(2):
                for r in range(4):
                    hh[part, r, :, ds(128 * g, 128, 128)] = wt[part, r].astype(F32).T.astype(BF)
            mark("g_gather")
            gid, gid_s = ids(12), out_id()

            def held(gg, part, h=None):
                which = slice(None) if h is None else pl.ds(h, 1)
                return hh.at[part, which, :, ds(128 * gg, 128, 128)]

            up, down, far = (g + 1) % 4, (g + 3) % 4, (g + 2) % 4

            def pass_held(gg, part, h, r_id, to):
                send(held(gg, part, h), held(gg, part, h), gid_s, gid + r_id, dev(p, to))

            for h in range(4):
                pass_held(g, 0, h, h, up)
                pass_held(g, 1, h, 4 + h, down)
            pass_held(g, 1, None, 8, up)
            pass_held(g, 0, None, 9, down)
            for h in range(4):
                arrived(held(down, 0, h), gid + h)
                pass_held(down, 0, h, 10, up)
                arrived(held(up, 1, h), gid + 4 + h)
                pass_held(up, 1, h, 11, down)
            arrived(held(down, 1), gid + 8)
            arrived(held(up, 0), gid + 9)
            arrived(held(far, 0), gid + 10)
            arrived(held(far, 1), gid + 11)
            sent(hh.at[:, 0:3], gid_s)

            mark("g_right")
            def put_model(col, a, b):
                mb[0, :, col : col + 256] = a.astype(BF)
                mb[1, :, col : col + 256] = b.astype(BF)

            inverse(lambda r: hh[:, r].reshape(256, QUARTER), 128, put_model)

            mark("misfit")
            squares = 0.0
            for n in range(2):
                rows = mb[...].reshape(256, N)
                some = pl.ds(n * 256, 256)
                a, b = dot(rows, tf[0, :, some]), dot(rows, tf[1, :, some])
                pr, pi = a[:128] - b[128:], b[:128] + a[128:]
                here = ds(512 * g + n * 256, 256, 256)
                mr = tf[0, own_rows, some].astype(F32) - mb[0, :, here].astype(F32)
                mi = tf[1, own_rows, some].astype(F32) - mb[1, :, here].astype(F32)
                mr = mr + (wr * pr - wi * pi)
                mi = mi + (wr * pi + wi * pr)
                squares = squares + jnp.sum(mr * mr + mi * mi)
                mf[0, :, n * 256 : n * 256 + 256] = mr.astype(BF)
                mf[1, :, n * 256 : n * 256 + 256] = mi.astype(BF)

        if it:
            mark("back")

            @pl.loop(0, 4)
            def _(n):
                back_rows(n)

        mine = ds(512 * g, 512, 512)
        for part in range(2):
            pg[part, mine, :] = pg[part, mine, :] + mf[part].astype(F32).T

        mark("f_right")
        quarters(
            lambda part, q: pg[part, q * QUARTER : q * QUARTER + QUARTER, :],
            lambda r, part: ubt.at[r, :, pl.ds(128 * part, 128)],
        )
        up, down, far = (g + 1) % 4, (g + 3) % 4, (g + 2) % 4
        rid, rid_s = ids(10), out_id()

        def piece(ref, gg, part, r=None):
            which = slice(None) if r is None else pl.ds(r, 1)
            return ref.at[it, part, which, ds(128 * gg, 128, 128), :]

        for r in range(4):
            there = pl.ds(r * QUARTER, QUARTER)
            a, b = dot(inv_c[there, :], ubt[r]), dot(inv_s[there, :], ubt[r])
            tr_, ti_ = a[:, :128] + b[:, 128:], a[:, 128:] - b[:, :128]
            tp[0, r] = tr_
            tp[1, r] = ti_
            sb[it, 0, r] = tr_.astype(BF)
            sb[it, 1, r] = ti_.astype(BF)
            send(piece(sb, far, 0, r), ra.at[it, pl.ds(r, 1)], rid_s, rid + r, dev(p, up))
            send(piece(sb, far, 1, r), rb.at[it, pl.ds(r, 1)], rid_s, rid + 4 + r, dev(p, down))

        mark("scatter")
        send(piece(sb, up, 1), dl.at[it, 1], rid_s, rid + 8, dev(p, up))
        send(piece(sb, down, 0), dr.at[it, 0], rid_s, rid + 9, dev(p, down))
        for r in range(4):
            one = pl.ds(r, 1)
            arrived(ra.at[it, one], rid + r)
            qa[it, r] = (tp[0, r, ds(128 * up, 128, 128), :] + ra[it, r].astype(F32)).astype(BF)
            send(qa.at[it, one], dl.at[it, 0, one], rid_s, rid + 8, dev(p, up))
            arrived(rb.at[it, one], rid + 4 + r)
            qb[it, r] = (tp[1, r, ds(128 * down, 128, 128), :] + rb[it, r].astype(F32)).astype(BF)
            send(qb.at[it, one], dr.at[it, 1, one], rid_s, rid + 9, dev(p, down))
        arrived(dl.at[it], rid + 8)
        arrived(dr.at[it], rid + 9)
        sent(sb.at[it, :, 0:3], rid_s)
        total = tp[:, :, ds(128 * g, 128, 128), :] + dl[it].astype(F32)
        zt[it] = (total + dr[it].astype(F32)).astype(BF)
        mark("f_plane")
        xid, xid_s = ids(1), out_id()
        src_of = lambda q: residue(zt.at[it], q)
        dst_of = lambda q: xt.at[it, :, :, ds(128 * q, 128, 128)]
        plane_exchange(src_of, dst_of, xid, xid_s)
        dst_of(p)[...] = src_of(p)[...]
        plane_wait(xt.at[it, :, :, 0:1920], xid, xid_s)

        mark("f_left")
        peaks = []

        def put_trial(r, a, b):
            a, b = STEP * a, STEP * b
            if it:
                a, b = trial[0, r] + a, trial[1, r] + b
            trial[0, r] = a
            trial[1, r] = b
            v = a * a + b * b
            v = jnp.maximum(jnp.maximum(v[:, :128], v[:, 128:256]), jnp.maximum(v[:, 256:384], v[:, 384:]))
            peaks.append(v)

        forward(lambda part, q: xt[it, part, :, q * QUARTER : q * QUARTER + QUARTER].astype(F32), put_trial)
        peak = jnp.maximum(jnp.maximum(peaks[0], peaks[1]), jnp.maximum(peaks[2], peaks[3]))
        peak = jnp.max(jnp.sqrt(peak))

        mark("stats")
        lane = lax.broadcasted_iota(jnp.int32, (1, 128), 1)
        st1[it] = jnp.where(lane < 64, peak, squares)
        sid, sid_s = ids(1), out_id()
        for k, (a, b, d) in enumerate(everyone):
            send(st1.at[it], sr1.at[it, k], sid_s, sid, dev(place(a, b), (g + d) % 4))
        sr1[it, 63] = st1[it]
        if it:
            mark("out_send")
            oid, oid_s = ids(1), out_id()
            away = jnp.logical_and(c == 1, x != y)
            out_src = lambda q: cfo.at[:, :, ds(128 * q, 128, 128)]
            out_dst = lambda q: ot.at[:, q]

            def out_copy(q):
                return rcopy(out_src(q), out_dst(p), oid_s, oid, chip(q // 4, q % 4, g, c))

            order = perm[...]
            for dz in (2, 1, 3, 0):
                b = (z + dz) % 4
                part_of = lambda part, r: trial[part, r, :, ds(128 * b, 128, 128)]
                v = [jnp.concatenate([part_of(part, r) for r in range(4)], axis=1) for part in range(2)]
                v = jnp.concatenate(v, axis=0)
                hi = v.astype(BF)
                rest = v - hi.astype(F32)
                mid = rest.astype(BF)
                low = (rest - mid.astype(F32)).astype(BF)
                v = dot(hi, order) + dot(mid, order) + dot(low, order)
                cfo[0, :, ds(512 * b, 512, 512)] = v[:32]
                cfo[1, :, ds(512 * b, 512, 512)] = v[32:]
                for dx in (2, 1, 3, 0):
                    if dz or dx:
                        out_copy(place(dz, dx)).start()

            @pl.when(away)
            def _():
                out_copy(p).start()

            @pl.when(jnp.logical_not(away))
            def _():
                out_dst(p)[...] = out_src(p)[...]

            mark("stats_wait")
        plane_wait(sr1.at[it, 0:63], sid, sid_s)
        found = sr1[it]
        both = jnp.where(lane < 64, jnp.max(found, axis=0), jnp.sum(found, axis=0))
        totals.append(jnp.max(jnp.where(lane < 64, 0.0, both)))
        mark("shrink")
        level = SHRINK * jnp.max(jnp.where(lane < 64, both, 0.0))

        def shrunk(a, b):
            size = jnp.sqrt(a * a + b * b)
            factor = jnp.maximum(1.0 - level / jnp.maximum(size, level), 0.0)
            return a * factor, b * factor

        if it == 0:
            for r in range(4):
                a, b = shrunk(trial[0, r], trial[1, r])
                trial[0, r] = a
                trial[1, r] = b
                cb[0, r] = a.astype(BF)
                cb[1, r] = b.astype(BF)

    mark("out_wait")
    nid, nid_s = ids(1), out_id()
    for it in range(2):
        nt[it] = jnp.sqrt(jnp.full((1, 128), totals[it], F32))
    send(nt, nr, nid_s, nid, partner)

    @pl.when(away)
    def _():
        rcopy(ot, ot, oid_s, oid, partner).wait_recv()

    @pl.when(jnp.logical_not(away))
    def _():
        rcopy(ot.at[:, 0:15], ot.at[:, 0:15], oid_s, oid, partner).wait_recv()

    mark("out_turn")
    for b in range(4):
        for r in range(4):
            a, d = shrunk(ot[0, 4 * b + r], ot[1, 4 * b + r])
            nat[0, b, pl.ds(r, 32, stride=4), :] = a
            nat[1, b, pl.ds(r, 32, stride=4), :] = d
    halves, halves_s = ids(1), out_id()

    def turned(part, half):
        return jnp.concatenate([nat[part, 2 * half + k].T for k in range(2)], axis=1)

    for part in range(2):
        keep[part] = turned(part, 1 - c)
    send(keep, got, halves_s, halves, partner)
    for part in range(2):
        out[c, part] = turned(part, c)
    mark("out_swap")
    arrived(nr, nid)
    for it in range(2):
        norms[it, c] = jnp.max(nt[it])
        norms[it, 1 - c] = jnp.max(nr[it])
    arrived(got, halves)
    out[1 - c] = got[...]
    for copy in pending:
        copy.wait_send()
    rcopy(nt, nt, nid_s, nid, partner).wait_send()
    rcopy(keep, keep, halves_s, halves, partner).wait_send()

    @pl.when(away)
    def _():
        rcopy(ot, ot, oid_s, oid, partner).wait_send()

    @pl.when(jnp.logical_not(away))
    def _():
        rcopy(ot.at[:, 0:15], ot.at[:, 0:15], oid_s, oid, partner).wait_send()

    @pl.when(jnp.logical_not(stays))
    def _():
        to_second.wait_send()

    @pl.when(c == 1)
    def _():
        to_first.wait_send()

    assert used == [RECEIVES, SENDS], used
    mark(None)


def scratch():
    v = lambda *shape, t=BF: pltpu.VMEM(shape, t)
    return [
        v(2, 2, 128, 256), *[v(*a.shape, t=F32) for a in table_parts()],
        v(2, N, 512), v(QUARTER, N), v(QUARTER, N), v(N, QUARTER), v(N, QUARTER), v(512, 512),
        v(2, N, 128, t=F32), v(4, QUARTER, 256), v(2, 4, QUARTER, 128, t=F32),
        v(2, 2, 4, QUARTER, 128), v(2, 4, 128, 128), v(2, 4, 128, 128), v(2, 4, 128, 128),
        v(2, 4, 128, 128), v(2, 2, 4, 128, 128), v(2, 2, 4, 128, 128), v(4, 2, 32, QUARTER),
        v(2, 2, 4, 128, 128), v(2, 2, 32, N),
        v(2, 4, 32, QUARTER, t=F32), v(2, 32, N, t=F32), v(2, 4, 32, QUARTER),
        v(2, 32, N), v(2, 4, 128, 128), v(2, 4, 128, QUARTER), v(2, 128, N), v(2, 128, 512),
        v(2, 16, 32, 128, t=F32), v(2, 4, 128, 128, t=F32),
        v(2, 128, 256, t=F32), v(2, 128, 256, t=F32),
        v(2, 1, 128, t=F32), v(2, 64, 1, 128, t=F32),
        v(2, 1, 128, t=F32), v(2, 1, 128, t=F32),
        pltpu.SemaphoreType.DMA((SENDS,)), pltpu.SemaphoreType.DMA((RECEIVES,)),
        pltpu.SemaphoreType.DMA((9,)),
    ]


def hand_on(a, b, out, norms):
    out[...] = a[...]
    for i in range(2):
        for j in range(2):
            norms[i, j] = b[i, j]


def per_device(traces, wavelet):
    vm = pl.BlockSpec(memory_space=pltpu.VMEM)
    sm = pl.BlockSpec(memory_space=pltpu.SMEM)
    hbm = pl.BlockSpec(memory_space=pl.ANY)
    shapes = (jax.ShapeDtypeStruct((2, 2, 128, 256), F32), jax.ShapeDtypeStruct((2, 2), F32))
    parts = pl.pallas_call(
        kernel,
        out_shape=shapes,
        in_specs=[hbm, sm] + [hbm] * 8,
        out_specs=(vm, sm),
        scratch_shapes=scratch(),
        compiler_params=pltpu.CompilerParams(
            collective_id=0, has_side_effects=True, vmem_limit_bytes=60 * 1024 * 1024
        ),
        name="whole",
    )(traces, wavelet, *table_parts())
    return pl.pallas_call(
        hand_on, out_shape=shapes, in_specs=[vm, sm], out_specs=(vm, sm), name="hand_on"
    )(*parts)


def solution(mesh):
    return jax.shard_map(
        per_device,
        mesh=mesh,
        in_specs=(P(None, None, "src", "rcv"), P()),
        out_specs=(P(None, None, "src", "rcv"), P()),
        check_vma=False,
    )
```

```python
import functools
import math

import jax
import jax.numpy as jnp
import numpy as np
from jax import lax
from jax.experimental import pallas as pl
from jax.experimental.pallas import tpu as pltpu
from jax.sharding import PartitionSpec as P

MESH = pl.DeviceIdType.MESH
N = 2048
BASE = 32
RECEIVES = 89
SENDS = 14
QUARTER = N // 4
STEP = 0.4
SHRINK = 0.2
BF = jnp.bfloat16
F32 = jnp.float32


def table_parts():
    def both(left, right, scale):
        angle = 2.0 * math.pi * ((left[:, None] * right[None, :]) % N) / N
        return [(f(angle) * scale).astype(np.float32) for f in (np.cos, np.sin)]

    scale = 1.0 / math.sqrt(N)
    quarter = np.arange(QUARTER)
    residue = np.arange(4)
    order = (4 * quarter[None, :] + residue[:, None]).reshape(-1)
    first = (4 * np.arange(BASE)[None, :] + residue[:, None]).reshape(-1)
    later = BASE * np.arange(QUARTER // BASE)
    return [
        *both(np.arange(BASE), order, scale), *both(later, order, 1.0),
        *both(first, quarter, scale), *both(4 * later, quarter, 1.0),
    ]


def kernel(
    tr_any, wave, t0, t1, t2, t3, t4, t5, t6, t7, out, norms,
    tr, b0, b1, b2, b3, b4, b5, b6, b7,
    tf, tab_c, tab_s, inv_c, inv_s, perm, pg, ubt, tp, sb, ra, rb, qa, qb, dl, dr, ub, zt, xt,
    trial, cfo, cb, hb, wt, hh, mb, mf, ot, nat, keep, got, st1, sr1, nt, nr,
    ssem, rsem, lsem,
):
    tables_any = (t0, t1, t2, t3, t4, t5, t6, t7)
    tables = (b0, b1, b2, b3, b4, b5, b6, b7)
    src = lax.axis_index("src")
    rcv = lax.axis_index("rcv")
    y = rcv // 2
    c = rcv % 2
    z = src // 4
    x = src % 4
    lane2 = (1 - c) * x + c * y
    g = (1 - c) * y + c * x
    p = z * 4 + lane2
    used = [0, 0]
    pending = []

    stage = [None]

    def mark(name):
        if stage[0] is not None:
            stage[0].__exit__(None, None, None)
        stage[0] = jax.named_scope(name) if name else None
        if name:
            stage[0].__enter__()

    def ids(n):
        used[0] += n
        return used[0] - n

    def out_id():
        used[1] += 1
        return used[1] - 1

    def chip(zz_, xx_, yy_, cc_):
        return (zz_ * 4 + xx_, yy_ * 2 + cc_)

    def dev(q, gg):
        second = q % 4
        return chip(q // 4, (1 - c) * second + c * gg, (1 - c) * gg + c * second, c)

    partner = chip(z, x, y, 1 - c)

    def rcopy(src, dst, s_id, r_id, where):
        return pltpu.make_async_remote_copy(
            src_ref=src, dst_ref=dst, send_sem=ssem.at[s_id], recv_sem=rsem.at[r_id],
            device_id=where, device_id_type=MESH,
        )

    def send(src, dst, s_id, r_id, where):
        rcopy(src, dst, s_id, r_id, where).start()

    def arrived(ref, r_id):
        rcopy(ref, ref, 0, r_id, partner).wait_recv()

    def sent(ref, s_id):
        pending.append(rcopy(ref, ref, s_id, 0, partner))

    def ds(start, size, unit):
        return pl.ds(pl.multiple_of(start, unit), size)

    mark("entry")
    fetched = [
        pltpu.make_async_copy(a, b, lsem.at[k])
        for k, (a, b) in enumerate(zip((tr_any, *tables_any), (tr, *tables)))
    ]
    for copy in fetched:
        copy.start()
    base_c, base_s, mul_c, mul_s, ibase_c, ibase_s, imul_c, imul_s = tables
    barrier = pltpu.get_barrier_semaphore()

    def greet(where):
        pl.semaphore_signal(barrier, inc=1, device_id=where, device_id_type=MESH)

    greet(partner)
    for d in (1, 2, 3):
        greet(dev(p, (g + d) % 4))
    for d in (1, 3):
        greet(dev((z + d) % 4 * 4 + lane2, g))
        greet(dev(z * 4 + (lane2 + d) % 4, g))
    crossed = jnp.logical_and(c == 1, x != y)

    @pl.when(crossed)
    def _():
        greet(chip(z, y, x, 0))
        greet(chip(z, y, x, 1))

    @pl.when(x != y)
    def _():
        pl.semaphore_wait(barrier, 9)

    @pl.when(x == y)
    def _():
        pl.semaphore_wait(barrier, 8)

    mark("swap")
    own_rows = ds(128 * p, 128, 128)
    fetched[0].wait()
    swap, swap_s = ids(2), [out_id(), out_id()]
    landing = tf.at[:, ds(128 * src, 128, 128), ds(256 * c, 256, 256)]
    to_first = rcopy(tr.at[0], landing, swap_s[0], swap + c, chip(z, x, y, 0))
    to_second = rcopy(tr.at[1], landing, swap_s[1], swap + c, chip(z, y, x, 1))
    stays = jnp.logical_and(c == 1, x == y)

    @pl.when(jnp.logical_not(stays))
    def _():
        to_second.start()

    @pl.when(c == 1)
    def _():
        to_first.start()

    @pl.when(c == 0)
    def _():
        landing[...] = tr[0]

    @pl.when(stays)
    def _():
        landing[...] = tr[1]

    @pl.when(c == 1)
    def _():
        arrived(tf.at[:, own_rows, 0:256], swap)

    @pl.when(jnp.logical_not(stays))
    def _():
        arrived(tf.at[:, own_rows, 256:512], swap + 1)

    root = 1.0 / math.sqrt(N)
    wr = wave[c, 0] * root
    wi = wave[c, 1] * root

    def dot(a, b):
        return lax.dot_general(a, b, (((1,), (0,)), ((), ())), preferred_element_type=F32)

    def dot_nt(a, b):
        return lax.dot_general(a, b, (((1,), (1,)), ((), ())), preferred_element_type=F32)

    def back_rows(n):
        errors = mf[...].reshape(256, 512)
        here = ds(n * 512, 512, 512)
        a, b = dot_nt(tf[0, here, :], errors), dot_nt(tf[1, here, :], errors)
        br, bi = a[:, :128] + b[:, 128:], a[:, 128:] - b[:, :128]
        pg[0, here, :] = -(wr * br + wi * bi)
        pg[1, here, :] = -(wr * bi - wi * br)

    def back_start():
        for part in range(2):
            mf[part] = tf[part, own_rows, :]

    def shift(at, axis, d):
        zz_, xx_ = at
        return (zz_ + (1 - axis) * d + 4) % 4, (xx_ + axis * d + 4) % 4

    def neighbour(axis, d):
        a, b = shift((z, lane2), axis, d)
        return dev(a * 4 + b, g)

    def block(at, kind, part=None):
        start = (at[0] * 4 + at[1]) * 128 + 32 * kind
        if part is not None:
            return tf.at[:, ds(start + 16 * part, 16, 16), :]
        return tf.at[:, ds(start, 32, 16), :]

    gather_s = out_id()

    def ag_start(at, axis, half, done):
        r_id = ids(2)
        send(block(at, half), block(at, half), gather_s, r_id, neighbour(axis, 1))
        send(block(at, half), block(at, half), gather_s, r_id + 1, neighbour(axis, -1))
        return at, axis, half, r_id, done

    def ag_forward(item):
        at, axis, half, r_id, done = item
        left, right = shift(at, axis, -1), shift(at, axis, 1)
        arrived(block(left, half), r_id)
        send(block(left, half, 0), block(left, half, 0), gather_s, done, neighbour(axis, 1))
        arrived(block(right, half), r_id + 1)
        send(block(right, half, 1), block(right, half, 1), gather_s, done, neighbour(axis, -1))

    def ag_finish(item):
        at, axis, half, r_id, done = item
        arrived(block(shift(at, axis, 2), half), done)

    def all_done(items, done):
        arrived(tf.at[:, 0 : 32 * items, :], done)

    def make_table(first, last):
        @pl.loop(first, last)
        def _(m):
            rows = ds(m * BASE, BASE, BASE)
            for col in range(0, N, 512):
                here = pl.ds(col, 512)
                bc, bs = base_c[:, here], base_s[:, here]
                mc, ms = mul_c[pl.ds(m, 1), here], mul_s[pl.ds(m, 1), here]
                tab_c[rows, here] = (bc * mc - bs * ms).astype(BF)
                tab_s[rows, here] = (bs * mc + bc * ms).astype(BF)
            mc, ms = imul_c[pl.ds(m, 1), :], imul_s[pl.ds(m, 1), :]
            for r in range(4):
                bc, bs = ibase_c[r * BASE : r * BASE + BASE], ibase_s[r * BASE : r * BASE + BASE]
                rows = ds(r * QUARTER + m * BASE, BASE, BASE)
                inv_c[rows, :] = (bc * mc - bs * ms).astype(BF)
                inv_s[rows, :] = (bs * mc + bc * ms).astype(BF)

    def make_order():
        row = lax.broadcasted_iota(jnp.int32, (512, 512), 0)
        col = lax.broadcasted_iota(jnp.int32, (512, 512), 1)
        perm[...] = jnp.where(col == 4 * (row % 128) + row // 128, 1.0, 0.0).astype(BF)

    mark("gather_a")
    home = (z, lane2)
    kinds = (0, 1, 2, 3)
    first_axis = (0, 0, 1, 0)
    first, own = {}, {}
    for k in (0, 2, 1, 3):
        first[k] = ag_start(home, first_axis[k], k, ids(1))
    own_done, near_done, far_done = ids(1), ids(1), ids(1)
    for k in (0, 2, 1, 3):
        own[k] = ag_start(home, 1 - first_axis[k], k, own_done)
    for copy in fetched[1:]:
        copy.wait()
    make_table(0, 16)
    make_order()
    mark("gather_b")
    near = {}

    def pass_on(k, hops):
        done = far_done if hops == (2,) else near_done
        near[k, hops] = [
            ag_start(shift(home, first_axis[k], d), 1 - first_axis[k], k, done) for d in hops
        ]

    for k in (0, 2, 1, 3):
        ag_forward(first[k])
    for k in (0, 2, 1, 3):
        pass_on(k, (-1, 1))
        ag_forward(own[k])
    for k in (0, 2, 1, 3):
        ag_finish(first[k])
        pass_on(k, (2,))
    mark("gather_c")
    for k in (0, 2, 1, 3):
        for item in near[k, (-1, 1)]:
            ag_forward(item)
    all_done(4, own_done)
    mark("gather_back")
    back_start()
    back_rows(z)
    mark("gather_d")
    for k in (0, 2, 1, 3):
        ag_forward(near[k, (2,)][0])
    all_done(8, near_done)
    mark("gather_back")
    back_rows((z + 3) % 4)
    back_rows((z + 1) % 4)
    mark("gather_e")
    all_done(4, far_done)
    sent(tf.at[:, 0:1920, :], gather_s)
    mark("gather_back")
    back_rows((z + 2) % 4)

    def quarters(load, ub):
        x = [[load(part, q) for part in range(2)] for q in range(4)]
        plus = [[x[h][k] + x[h + 2][k] for k in range(2)] for h in range(2)]
        less = [[x[h][k] - x[h + 2][k] for k in range(2)] for h in range(2)]
        for k in range(2):
            ub(0, k)[...] = (plus[0][k] + plus[1][k]).astype(BF)
            ub(2, k)[...] = (plus[0][k] - plus[1][k]).astype(BF)
        ub(1, 0)[...] = (less[0][0] + less[1][1]).astype(BF)
        ub(1, 1)[...] = (less[0][1] - less[1][0]).astype(BF)
        ub(3, 0)[...] = (less[0][0] - less[1][1]).astype(BF)
        ub(3, 1)[...] = (less[0][1] + less[1][0]).astype(BF)

    def forward(load, store):
        quarters(load, lambda r, part: ub.at[r, part])
        for r in range(4):
            rows = ub[r].reshape(64, QUARTER)
            here = pl.ds(r * QUARTER, QUARTER)
            a, b = dot(rows, tab_c[:, here]), dot(rows, tab_s[:, here])
            store(r, a[:32] + b[32:], a[32:] - b[:32])

    def inverse(load, half, store):
        for col in range(0, QUARTER, 256):
            e = []
            for r in range(4):
                rows = load(r)
                there = pl.ds(r * QUARTER, QUARTER)
                a = dot(rows, inv_c[there, col : col + 256])
                b = dot(rows, inv_s[there, col : col + 256])
                e.append((a[:half] - b[half:], b[:half] + a[half:]))
            plus = [[e[h][k] + e[h + 2][k] for k in range(2)] for h in range(2)]
            less = [[e[h][k] - e[h + 2][k] for k in range(2)] for h in range(2)]
            store(col, plus[0][0] + plus[1][0], plus[0][1] + plus[1][1])
            store(QUARTER + col, less[0][0] - less[1][1], less[0][1] + less[1][0])
            store(2 * QUARTER + col, plus[0][0] - plus[1][0], plus[0][1] - plus[1][1])
            store(3 * QUARTER + col, less[0][0] + less[1][1], less[0][1] - less[1][0])

    def residue(ref, q):
        return ref.at[:, q % 4, ds(32 * (q // 4), 32, 32), :]

    offsets = [(a, b) for a in range(4) for b in range(4) if a or b]
    offsets.sort(key=lambda o: -(min(o[0], 4 - o[0]) + min(o[1], 4 - o[1])))

    everyone = [(a, b, d) for a in range(4) for b in range(4) for d in range(4) if a or b or d]
    everyone.sort(key=lambda o: -sum(min(i, 4 - i) for i in o))

    def place(a, b):
        return (z + a) % 4 * 4 + (lane2 + b) % 4

    def plane_exchange(source, landing, r_id, s_id):
        for a, b in offsets:
            q = place(a, b)
            rcopy(source(q), landing(p), s_id, r_id, dev(q, g)).start()

    def plane_wait(others, r_id, s_id):
        arrived(others, r_id)
        sent(others, s_id)

    totals = []
    for it in range(2):
        if it == 0:
            ref, imf = mf[0].astype(F32), mf[1].astype(F32)
            squares = jnp.sum(ref * ref + imf * imf)
        else:
            mark("g_left")
            def put_half(col, a, b):
                hb[0, :, col : col + 256] = a.astype(BF)
                hb[1, :, col : col + 256] = b.astype(BF)

            inverse(lambda r: cb[:, r].reshape(64, QUARTER), 32, put_half)

            mark("g_plane")
            wid, wid_s = ids(1), out_id()
            src_of = lambda q: hb.at[:, :, ds(128 * q, 128, 128)]
            dst_of = lambda q: residue(wt, q)
            plane_exchange(src_of, dst_of, wid, wid_s)
            residue(wt, p)[...] = hb[:, :, ds(128 * p, 128, 128)]
            plane_wait(hb.at[:, :, 0:1920], wid, wid_s)
            for part in range(2):
                for r in range(4):
                    hh[part, r, :, ds(128 * g, 128, 128)] = wt[part, r].astype(F32).T.astype(BF)
            mark("g_gather")
            gid, gid_s = ids(12), out_id()

            def held(gg, part, h=None):
                which = slice(None) if h is None else pl.ds(h, 1)
                return hh.at[part, which, :, ds(128 * gg, 128, 128)]

            up, down, far = (g + 1) % 4, (g + 3) % 4, (g + 2) % 4

            def pass_held(gg, part, h, r_id, to):
                send(held(gg, part, h), held(gg, part, h), gid_s, gid + r_id, dev(p, to))

            for h in range(4):
                pass_held(g, 0, h, h, up)
                pass_held(g, 1, h, 4 + h, down)
            pass_held(g, 1, None, 8, up)
            pass_held(g, 0, None, 9, down)
            for h in range(4):
                arrived(held(down, 0, h), gid + h)
                pass_held(down, 0, h, 10, up)
                arrived(held(up, 1, h), gid + 4 + h)
                pass_held(up, 1, h, 11, down)
            arrived(held(down, 1), gid + 8)
            arrived(held(up, 0), gid + 9)
            arrived(held(far, 0), gid + 10)
            arrived(held(far, 1), gid + 11)
            sent(hh.at[:, 0:3], gid_s)

            mark("g_right")
            def put_model(col, a, b):
                mb[0, :, col : col + 256] = a.astype(BF)
                mb[1, :, col : col + 256] = b.astype(BF)

            inverse(lambda r: hh[:, r].reshape(256, QUARTER), 128, put_model)

            mark("misfit")
            squares = 0.0
            for n in range(2):
                rows = mb[...].reshape(256, N)
                some = pl.ds(n * 256, 256)
                a, b = dot(rows, tf[0, :, some]), dot(rows, tf[1, :, some])
                pr, pi = a[:128] - b[128:], b[:128] + a[128:]
                here = ds(512 * g + n * 256, 256, 256)
                mr = tf[0, own_rows, some].astype(F32) - mb[0, :, here].astype(F32)
                mi = tf[1, own_rows, some].astype(F32) - mb[1, :, here].astype(F32)
                mr = mr + (wr * pr - wi * pi)
                mi = mi + (wr * pi + wi * pr)
                squares = squares + jnp.sum(mr * mr + mi * mi)
                mf[0, :, n * 256 : n * 256 + 256] = mr.astype(BF)
                mf[1, :, n * 256 : n * 256 + 256] = mi.astype(BF)

        if it:
            mark("back")

            @pl.loop(0, 4)
            def _(n):
                back_rows(n)

        mine = ds(512 * g, 512, 512)
        for part in range(2):
            pg[part, mine, :] = pg[part, mine, :] + mf[part].astype(F32).T

        mark("f_right")
        quarters(
            lambda part, q: pg[part, q * QUARTER : q * QUARTER + QUARTER, :],
            lambda r, part: ubt.at[r, :, pl.ds(128 * part, 128)],
        )
        up, down, far = (g + 1) % 4, (g + 3) % 4, (g + 2) % 4
        rid, rid_s = ids(10), out_id()

        def piece(ref, gg, part, r=None):
            which = slice(None) if r is None else pl.ds(r, 1)
            return ref.at[it, part, which, ds(128 * gg, 128, 128), :]

        for r in range(4):
            there = pl.ds(r * QUARTER, QUARTER)
            a, b = dot(inv_c[there, :], ubt[r]), dot(inv_s[there, :], ubt[r])
            tr_, ti_ = a[:, :128] + b[:, 128:], a[:, 128:] - b[:, :128]
            tp[0, r] = tr_
            tp[1, r] = ti_
            sb[it, 0, r] = tr_.astype(BF)
            sb[it, 1, r] = ti_.astype(BF)
            send(piece(sb, far, 0, r), ra.at[it, pl.ds(r, 1)], rid_s, rid + r, dev(p, up))
            send(piece(sb, far, 1, r), rb.at[it, pl.ds(r, 1)], rid_s, rid + 4 + r, dev(p, down))

        mark("scatter")
        send(piece(sb, up, 1), dl.at[it, 1], rid_s, rid + 8, dev(p, up))
        send(piece(sb, down, 0), dr.at[it, 0], rid_s, rid + 9, dev(p, down))
        for r in range(4):
            one = pl.ds(r, 1)
            arrived(ra.at[it, one], rid + r)
            qa[it, r] = (tp[0, r, ds(128 * up, 128, 128), :] + ra[it, r].astype(F32)).astype(BF)
            send(qa.at[it, one], dl.at[it, 0, one], rid_s, rid + 8, dev(p, up))
            arrived(rb.at[it, one], rid + 4 + r)
            qb[it, r] = (tp[1, r, ds(128 * down, 128, 128), :] + rb[it, r].astype(F32)).astype(BF)
            send(qb.at[it, one], dr.at[it, 1, one], rid_s, rid + 9, dev(p, down))
        arrived(dl.at[it], rid + 8)
        arrived(dr.at[it], rid + 9)
        sent(sb.at[it, :, 0:3], rid_s)
        total = tp[:, :, ds(128 * g, 128, 128), :] + dl[it].astype(F32)
        zt[it] = (total + dr[it].astype(F32)).astype(BF)
        mark("f_plane")
        xid, xid_s = ids(1), out_id()
        src_of = lambda q: residue(zt.at[it], q)
        dst_of = lambda q: xt.at[it, :, :, ds(128 * q, 128, 128)]
        plane_exchange(src_of, dst_of, xid, xid_s)
        dst_of(p)[...] = src_of(p)[...]
        plane_wait(xt.at[it, :, :, 0:1920], xid, xid_s)

        mark("f_left")
        peaks = []

        def put_trial(r, a, b):
            a, b = STEP * a, STEP * b
            if it:
                a, b = trial[0, r] + a, trial[1, r] + b
            trial[0, r] = a
            trial[1, r] = b
            v = a * a + b * b
            v = jnp.maximum(jnp.maximum(v[:, :128], v[:, 128:256]), jnp.maximum(v[:, 256:384], v[:, 384:]))
            peaks.append(v)

        forward(lambda part, q: xt[it, part, :, q * QUARTER : q * QUARTER + QUARTER].astype(F32), put_trial)
        peak = jnp.maximum(jnp.maximum(peaks[0], peaks[1]), jnp.maximum(peaks[2], peaks[3]))
        peak = jnp.max(jnp.sqrt(peak))

        mark("stats")
        lane = lax.broadcasted_iota(jnp.int32, (1, 128), 1)
        st1[it] = jnp.where(lane < 64, peak, squares)
        sid, sid_s = ids(1), out_id()
        for k, (a, b, d) in enumerate(everyone):
            send(st1.at[it], sr1.at[it, k], sid_s, sid, dev(place(a, b), (g + d) % 4))
        sr1[it, 63] = st1[it]
        if it:
            mark("out_send")
            oid, oid_s = ids(1), out_id()
            away = jnp.logical_and(c == 1, x != y)
            out_src = lambda q: cfo.at[:, :, ds(128 * q, 128, 128)]
            out_dst = lambda q: ot.at[:, q]

            def out_copy(q):
                return rcopy(out_src(q), out_dst(p), oid_s, oid, chip(q // 4, q % 4, g, c))

            order = perm[...]
            for dz in (2, 1, 3, 0):
                b = (z + dz) % 4
                part_of = lambda part, r: trial[part, r, :, ds(128 * b, 128, 128)]
                v = [jnp.concatenate([part_of(part, r) for r in range(4)], axis=1) for part in range(2)]
                v = jnp.concatenate(v, axis=0)
                hi = v.astype(BF)
                rest = v - hi.astype(F32)
                mid = rest.astype(BF)
                low = (rest - mid.astype(F32)).astype(BF)
                v = dot(hi, order) + dot(mid, order) + dot(low, order)
                cfo[0, :, ds(512 * b, 512, 512)] = v[:32]
                cfo[1, :, ds(512 * b, 512, 512)] = v[32:]
                for dx in (2, 1, 3, 0):
                    if dz or dx:
                        out_copy(place(dz, dx)).start()

            @pl.when(away)
            def _():
                out_copy(p).start()

            @pl.when(jnp.logical_not(away))
            def _():
                out_dst(p)[...] = out_src(p)[...]

            mark("stats_wait")
        plane_wait(sr1.at[it, 0:63], sid, sid_s)
        found = sr1[it]
        both = jnp.where(lane < 64, jnp.max(found, axis=0), jnp.sum(found, axis=0))
        totals.append(jnp.max(jnp.where(lane < 64, 0.0, both)))
        mark("shrink")
        level = SHRINK * jnp.max(jnp.where(lane < 64, both, 0.0))

        def shrunk(a, b):
            size = jnp.sqrt(a * a + b * b)
            factor = jnp.maximum(1.0 - level / jnp.maximum(size, level), 0.0)
            return a * factor, b * factor

        if it == 0:
            for r in range(4):
                a, b = shrunk(trial[0, r], trial[1, r])
                trial[0, r] = a
                trial[1, r] = b
                cb[0, r] = a.astype(BF)
                cb[1, r] = b.astype(BF)

    mark("out_wait")
    nid, nid_s = ids(1), out_id()
    for it in range(2):
        nt[it] = jnp.sqrt(jnp.full((1, 128), totals[it], F32))
    send(nt, nr, nid_s, nid, partner)

    @pl.when(away)
    def _():
        rcopy(ot, ot, oid_s, oid, partner).wait_recv()

    @pl.when(jnp.logical_not(away))
    def _():
        rcopy(ot.at[:, 0:15], ot.at[:, 0:15], oid_s, oid, partner).wait_recv()

    mark("out_turn")
    for b in range(4):
        for r in range(4):
            a, d = shrunk(ot[0, 4 * b + r], ot[1, 4 * b + r])
            nat[0, b, pl.ds(r, 32, stride=4), :] = a
            nat[1, b, pl.ds(r, 32, stride=4), :] = d
    halves, halves_s = ids(1), out_id()

    def turned(part, half):
        return jnp.concatenate([nat[part, 2 * half + k].T for k in range(2)], axis=1)

    for part in range(2):
        keep[part] = turned(part, 1 - c)
    send(keep, got, halves_s, halves, partner)
    for part in range(2):
        out[c, part] = turned(part, c)
    mark("out_swap")
    arrived(nr, nid)
    for it in range(2):
        norms[it, c] = jnp.max(nt[it])
        norms[it, 1 - c] = jnp.max(nr[it])
    arrived(got, halves)
    out[1 - c] = got[...]
    for copy in pending:
        copy.wait_send()
    rcopy(nt, nt, nid_s, nid, partner).wait_send()
    rcopy(keep, keep, halves_s, halves, partner).wait_send()

    @pl.when(away)
    def _():
        rcopy(ot, ot, oid_s, oid, partner).wait_send()

    @pl.when(jnp.logical_not(away))
    def _():
        rcopy(ot.at[:, 0:15], ot.at[:, 0:15], oid_s, oid, partner).wait_send()

    @pl.when(jnp.logical_not(stays))
    def _():
        to_second.wait_send()

    @pl.when(c == 1)
    def _():
        to_first.wait_send()

    assert used == [RECEIVES, SENDS], used
    mark(None)


def scratch():
    v = lambda *shape, t=BF: pltpu.VMEM(shape, t)
    return [
        v(2, 2, 128, 256), *[v(*a.shape, t=F32) for a in table_parts()],
        v(2, N, 512), v(QUARTER, N), v(QUARTER, N), v(N, QUARTER), v(N, QUARTER), v(512, 512),
        v(2, N, 128, t=F32), v(4, QUARTER, 256), v(2, 4, QUARTER, 128, t=F32),
        v(2, 2, 4, QUARTER, 128), v(2, 4, 128, 128), v(2, 4, 128, 128), v(2, 4, 128, 128),
        v(2, 4, 128, 128), v(2, 2, 4, 128, 128), v(2, 2, 4, 128, 128), v(4, 2, 32, QUARTER),
        v(2, 2, 4, 128, 128), v(2, 2, 32, N),
        v(2, 4, 32, QUARTER, t=F32), v(2, 32, N, t=F32), v(2, 4, 32, QUARTER),
        v(2, 32, N), v(2, 4, 128, 128), v(2, 4, 128, QUARTER), v(2, 128, N), v(2, 128, 512),
        v(2, 16, 32, 128, t=F32), v(2, 4, 128, 128, t=F32),
        v(2, 128, 256, t=F32), v(2, 128, 256, t=F32),
        v(2, 1, 128, t=F32), v(2, 64, 1, 128, t=F32),
        v(2, 1, 128, t=F32), v(2, 1, 128, t=F32),
        pltpu.SemaphoreType.DMA((SENDS,)), pltpu.SemaphoreType.DMA((RECEIVES,)),
        pltpu.SemaphoreType.DMA((9,)),
    ]


def hand_on(a, b, out, norms):
    out[...] = a[...]
    for i in range(2):
        for j in range(2):
            norms[i, j] = b[i, j]


def per_device(traces, wavelet):
    vm = pl.BlockSpec(memory_space=pltpu.VMEM)
    sm = pl.BlockSpec(memory_space=pltpu.SMEM)
    hbm = pl.BlockSpec(memory_space=pl.ANY)
    block = pl.BlockSpec((1, 2, 128, 256), lambda i: (i, 0, 0, 0))
    shapes = (jax.ShapeDtypeStruct((2, 2, 128, 256), F32), jax.ShapeDtypeStruct((2, 2), F32))
    parts = pl.pallas_call(
        kernel,
        out_shape=shapes,
        in_specs=[hbm, sm] + [hbm] * 8,
        out_specs=(vm, sm),
        scratch_shapes=scratch(),
        compiler_params=pltpu.CompilerParams(
            collective_id=0, has_side_effects=True, vmem_limit_bytes=60 * 1024 * 1024
        ),
        name="whole",
    )(traces, wavelet, *table_parts())
    return pl.pallas_call(
        hand_on, out_shape=shapes, grid=(2,), in_specs=[block, sm], out_specs=(block, sm), name="hand_on"
    )(*parts)


def solution(mesh):
    return jax.shard_map(
        per_device,
        mesh=mesh,
        in_specs=(P(None, None, "src", "rcv"), P()),
        out_specs=(P(None, None, "src", "rcv"), P()),
        check_vma=False,
    )
```

```python
import functools
import math

import jax
import jax.numpy as jnp
import numpy as np
from jax import lax
from jax.experimental import pallas as pl
from jax.experimental.pallas import tpu as pltpu
from jax.sharding import PartitionSpec as P

MESH = pl.DeviceIdType.MESH
N = 2048
BASE = 32
RECEIVES = 89
SENDS = 14
QUARTER = N // 4
STEP = 0.4
SHRINK = 0.2
BF = jnp.bfloat16
F32 = jnp.float32


def table_parts():
    def both(left, right, scale):
        angle = 2.0 * math.pi * ((left[:, None] * right[None, :]) % N) / N
        return [(f(angle) * scale).astype(np.float32) for f in (np.cos, np.sin)]

    scale = 1.0 / math.sqrt(N)
    quarter = np.arange(QUARTER)
    residue = np.arange(4)
    order = (4 * quarter[None, :] + residue[:, None]).reshape(-1)
    first = (4 * np.arange(BASE)[None, :] + residue[:, None]).reshape(-1)
    later = BASE * np.arange(QUARTER // BASE)
    return [
        *both(np.arange(BASE), order, scale), *both(later, order, 1.0),
        *both(first, quarter, scale), *both(4 * later, quarter, 1.0),
    ]


def kernel(
    tr_any, wave, t0, t1, t2, t3, t4, t5, t6, t7, out, norms,
    tr, b0, b1, b2, b3, b4, b5, b6, b7,
    tf, tab_c, tab_s, inv_c, inv_s, perm, pg, ubt, tp, sb, ra, rb, qa, qb, dl, dr, ub, zt, xt,
    trial, cfo, cb, hb, wt, hh, mb, mf, ot, nat, keep, got, st1, sr1, nt, nr,
    ssem, rsem, lsem,
):
    tables_any = (t0, t1, t2, t3, t4, t5, t6, t7)
    tables = (b0, b1, b2, b3, b4, b5, b6, b7)
    src = lax.axis_index("src")
    rcv = lax.axis_index("rcv")
    y = rcv // 2
    c = rcv % 2
    z = src // 4
    x = src % 4
    lane2 = (1 - c) * x + c * y
    g = (1 - c) * y + c * x
    p = z * 4 + lane2
    used = [0, 0]
    pending = []

    stage = [None]

    def mark(name):
        if stage[0] is not None:
            stage[0].__exit__(None, None, None)
        stage[0] = jax.named_scope(name) if name else None
        if name:
            stage[0].__enter__()

    def ids(n):
        used[0] += n
        return used[0] - n

    def out_id():
        used[1] += 1
        return used[1] - 1

    def chip(zz_, xx_, yy_, cc_):
        return (zz_ * 4 + xx_, yy_ * 2 + cc_)

    def dev(q, gg):
        second = q % 4
        return chip(q // 4, (1 - c) * second + c * gg, (1 - c) * gg + c * second, c)

    partner = chip(z, x, y, 1 - c)

    def rcopy(src, dst, s_id, r_id, where):
        return pltpu.make_async_remote_copy(
            src_ref=src, dst_ref=dst, send_sem=ssem.at[s_id], recv_sem=rsem.at[r_id],
            device_id=where, device_id_type=MESH,
        )

    def send(src, dst, s_id, r_id, where):
        rcopy(src, dst, s_id, r_id, where).start()

    def arrived(ref, r_id):
        rcopy(ref, ref, 0, r_id, partner).wait_recv()

    def sent(ref, s_id):
        pending.append(rcopy(ref, ref, s_id, 0, partner))

    def ds(start, size, unit):
        return pl.ds(pl.multiple_of(start, unit), size)

    mark("entry")
    fetched = [
        pltpu.make_async_copy(a, b, lsem.at[k])
        for k, (a, b) in enumerate(zip((tr_any, *tables_any), (tr, *tables)))
    ]
    for copy in fetched:
        copy.start()
    base_c, base_s, mul_c, mul_s, ibase_c, ibase_s, imul_c, imul_s = tables
    barrier = pltpu.get_barrier_semaphore()

    def greet(where):
        pl.semaphore_signal(barrier, inc=1, device_id=where, device_id_type=MESH)

    greet(partner)
    for d in (1, 2, 3):
        greet(dev(p, (g + d) % 4))
    for d in (1, 3):
        greet(dev((z + d) % 4 * 4 + lane2, g))
        greet(dev(z * 4 + (lane2 + d) % 4, g))
    crossed = jnp.logical_and(c == 1, x != y)

    @pl.when(crossed)
    def _():
        greet(chip(z, y, x, 0))
        greet(chip(z, y, x, 1))

    @pl.when(x != y)
    def _():
        pl.semaphore_wait(barrier, 9)

    @pl.when(x == y)
    def _():
        pl.semaphore_wait(barrier, 8)

    mark("swap")
    own_rows = ds(128 * p, 128, 128)
    fetched[0].wait()
    swap, swap_s = ids(2), [out_id(), out_id()]
    landing = tf.at[:, ds(128 * src, 128, 128), ds(256 * c, 256, 256)]
    to_first = rcopy(tr.at[0], landing, swap_s[0], swap + c, chip(z, x, y, 0))
    to_second = rcopy(tr.at[1], landing, swap_s[1], swap + c, chip(z, y, x, 1))
    stays = jnp.logical_and(c == 1, x == y)

    @pl.when(c == 1)
    def _():
        to_first.start()

    @pl.when(jnp.logical_not(stays))
    def _():
        to_second.start()

    @pl.when(c == 0)
    def _():
        landing[...] = tr[0]

    @pl.when(stays)
    def _():
        landing[...] = tr[1]

    @pl.when(c == 1)
    def _():
        arrived(tf.at[:, own_rows, 0:256], swap)

    @pl.when(jnp.logical_not(stays))
    def _():
        arrived(tf.at[:, own_rows, 256:512], swap + 1)

    root = 1.0 / math.sqrt(N)
    wr = wave[c, 0] * root
    wi = wave[c, 1] * root

    def dot(a, b):
        return lax.dot_general(a, b, (((1,), (0,)), ((), ())), preferred_element_type=F32)

    def dot_nt(a, b):
        return lax.dot_general(a, b, (((1,), (1,)), ((), ())), preferred_element_type=F32)

    def back_rows(n):
        errors = mf[...].reshape(256, 512)
        here = ds(n * 512, 512, 512)
        a, b = dot_nt(tf[0, here, :], errors), dot_nt(tf[1, here, :], errors)
        br, bi = a[:, :128] + b[:, 128:], a[:, 128:] - b[:, :128]
        pg[0, here, :] = -(wr * br + wi * bi)
        pg[1, here, :] = -(wr * bi - wi * br)

    def back_start():
        for part in range(2):
            mf[part] = tf[part, own_rows, :]

    def shift(at, axis, d):
        zz_, xx_ = at
        return (zz_ + (1 - axis) * d + 4) % 4, (xx_ + axis * d + 4) % 4

    def neighbour(axis, d):
        a, b = shift((z, lane2), axis, d)
        return dev(a * 4 + b, g)

    def block(at, kind, part=None):
        start = (at[0] * 4 + at[1]) * 128 + 32 * kind
        if part is not None:
            return tf.at[:, ds(start + 16 * part, 16, 16), :]
        return tf.at[:, ds(start, 32, 16), :]

    gather_s = out_id()

    def ag_start(at, axis, half, done):
        r_id = ids(2)
        send(block(at, half), block(at, half), gather_s, r_id, neighbour(axis, 1))
        send(block(at, half), block(at, half), gather_s, r_id + 1, neighbour(axis, -1))
        return at, axis, half, r_id, done

    def ag_forward(item):
        at, axis, half, r_id, done = item
        left, right = shift(at, axis, -1), shift(at, axis, 1)
        arrived(block(left, half), r_id)
        send(block(left, half, 0), block(left, half, 0), gather_s, done, neighbour(axis, 1))
        arrived(block(right, half), r_id + 1)
        send(block(right, half, 1), block(right, half, 1), gather_s, done, neighbour(axis, -1))

    def ag_finish(item):
        at, axis, half, r_id, done = item
        arrived(block(shift(at, axis, 2), half), done)

    def all_done(items, done):
        arrived(tf.at[:, 0 : 32 * items, :], done)

    def make_table(first, last):
        @pl.loop(first, last)
        def _(m):
            rows = ds(m * BASE, BASE, BASE)
            for col in range(0, N, 512):
                here = pl.ds(col, 512)
                bc, bs = base_c[:, here], base_s[:, here]
                mc, ms = mul_c[pl.ds(m, 1), here], mul_s[pl.ds(m, 1), here]
                tab_c[rows, here] = (bc * mc - bs * ms).astype(BF)
                tab_s[rows, here] = (bs * mc + bc * ms).astype(BF)
            mc, ms = imul_c[pl.ds(m, 1), :], imul_s[pl.ds(m, 1), :]
            for r in range(4):
                bc, bs = ibase_c[r * BASE : r * BASE + BASE], ibase_s[r * BASE : r * BASE + BASE]
                rows = ds(r * QUARTER + m * BASE, BASE, BASE)
                inv_c[rows, :] = (bc * mc - bs * ms).astype(BF)
                inv_s[rows, :] = (bs * mc + bc * ms).astype(BF)

    def make_order():
        row = lax.broadcasted_iota(jnp.int32, (512, 512), 0)
        col = lax.broadcasted_iota(jnp.int32, (512, 512), 1)
        perm[...] = jnp.where(col == 4 * (row % 128) + row // 128, 1.0, 0.0).astype(BF)

    mark("gather_a")
    home = (z, lane2)
    kinds = (0, 1, 2, 3)
    first_axis = (0, 0, 1, 0)
    first, own = {}, {}
    for k in (0, 2, 1, 3):
        first[k] = ag_start(home, first_axis[k], k, ids(1))
    own_done, near_done, far_done = ids(1), ids(1), ids(1)
    for k in (0, 2, 1, 3):
        own[k] = ag_start(home, 1 - first_axis[k], k, own_done)
    for copy in fetched[1:]:
        copy.wait()
    make_table(0, 16)
    make_order()
    mark("gather_b")
    near = {}

    def pass_on(k, hops):
        done = far_done if hops == (2,) else near_done
        near[k, hops] = [
            ag_start(shift(home, first_axis[k], d), 1 - first_axis[k], k, done) for d in hops
        ]

    for k in (0, 2, 1, 3):
        ag_forward(first[k])
    for k in (0, 2, 1, 3):
        pass_on(k, (-1, 1))
        ag_forward(own[k])
    for k in (0, 2, 1, 3):
        ag_finish(first[k])
        pass_on(k, (2,))
    mark("gather_c")
    for k in (0, 2, 1, 3):
        for item in near[k, (-1, 1)]:
            ag_forward(item)
    all_done(4, own_done)
    mark("gather_back")
    back_start()
    back_rows(z)
    mark("gather_d")
    for k in (0, 2, 1, 3):
        ag_forward(near[k, (2,)][0])
    all_done(8, near_done)
    mark("gather_back")
    back_rows((z + 3) % 4)
    back_rows((z + 1) % 4)
    mark("gather_e")
    all_done(4, far_done)
    sent(tf.at[:, 0:1920, :], gather_s)
    mark("gather_back")
    back_rows((z + 2) % 4)

    def quarters(load, ub):
        x = [[load(part, q) for part in range(2)] for q in range(4)]
        plus = [[x[h][k] + x[h + 2][k] for k in range(2)] for h in range(2)]
        less = [[x[h][k] - x[h + 2][k] for k in range(2)] for h in range(2)]
        for k in range(2):
            ub(0, k)[...] = (plus[0][k] + plus[1][k]).astype(BF)
            ub(2, k)[...] = (plus[0][k] - plus[1][k]).astype(BF)
        ub(1, 0)[...] = (less[0][0] + less[1][1]).astype(BF)
        ub(1, 1)[...] = (less[0][1] - less[1][0]).astype(BF)
        ub(3, 0)[...] = (less[0][0] - less[1][1]).astype(BF)
        ub(3, 1)[...] = (less[0][1] + less[1][0]).astype(BF)

    def forward(load, store):
        quarters(load, lambda r, part: ub.at[r, part])
        for r in range(4):
            rows = ub[r].reshape(64, QUARTER)
            here = pl.ds(r * QUARTER, QUARTER)
            a, b = dot(rows, tab_c[:, here]), dot(rows, tab_s[:, here])
            store(r, a[:32] + b[32:], a[32:] - b[:32])

    def inverse(load, half, store):
        for col in range(0, QUARTER, 256):
            e = []
            for r in range(4):
                rows = load(r)
                there = pl.ds(r * QUARTER, QUARTER)
                a = dot(rows, inv_c[there, col : col + 256])
                b = dot(rows, inv_s[there, col : col + 256])
                e.append((a[:half] - b[half:], b[:half] + a[half:]))
            plus = [[e[h][k] + e[h + 2][k] for k in range(2)] for h in range(2)]
            less = [[e[h][k] - e[h + 2][k] for k in range(2)] for h in range(2)]
            store(col, plus[0][0] + plus[1][0], plus[0][1] + plus[1][1])
            store(QUARTER + col, less[0][0] - less[1][1], less[0][1] + less[1][0])
            store(2 * QUARTER + col, plus[0][0] - plus[1][0], plus[0][1] - plus[1][1])
            store(3 * QUARTER + col, less[0][0] + less[1][1], less[0][1] - less[1][0])

    def residue(ref, q):
        return ref.at[:, q % 4, ds(32 * (q // 4), 32, 32), :]

    offsets = [(a, b) for a in range(4) for b in range(4) if a or b]
    offsets.sort(key=lambda o: -(min(o[0], 4 - o[0]) + min(o[1], 4 - o[1])))

    everyone = [(a, b, d) for a in range(4) for b in range(4) for d in range(4) if a or b or d]
    everyone.sort(key=lambda o: -sum(min(i, 4 - i) for i in o))

    def place(a, b):
        return (z + a) % 4 * 4 + (lane2 + b) % 4

    def plane_exchange(source, landing, r_id, s_id):
        for a, b in offsets:
            q = place(a, b)
            rcopy(source(q), landing(p), s_id, r_id, dev(q, g)).start()

    def plane_wait(others, r_id, s_id):
        arrived(others, r_id)
        sent(others, s_id)

    totals = []
    for it in range(2):
        if it == 0:
            ref, imf = mf[0].astype(F32), mf[1].astype(F32)
            squares = jnp.sum(ref * ref + imf * imf)
        else:
            mark("g_left")
            def put_half(col, a, b):
                hb[0, :, col : col + 256] = a.astype(BF)
                hb[1, :, col : col + 256] = b.astype(BF)

            inverse(lambda r: cb[:, r].reshape(64, QUARTER), 32, put_half)

            mark("g_plane")
            wid, wid_s = ids(1), out_id()
            src_of = lambda q: hb.at[:, :, ds(128 * q, 128, 128)]
            dst_of = lambda q: residue(wt, q)
            plane_exchange(src_of, dst_of, wid, wid_s)
            residue(wt, p)[...] = hb[:, :, ds(128 * p, 128, 128)]
            plane_wait(hb.at[:, :, 0:1920], wid, wid_s)
            for part in range(2):
                for r in range(4):
                    hh[part, r, :, ds(128 * g, 128, 128)] = wt[part, r].astype(F32).T.astype(BF)
            mark("g_gather")
            gid, gid_s = ids(12), out_id()

            def held(gg, part, h=None):
                which = slice(None) if h is None else pl.ds(h, 1)
                return hh.at[part, which, :, ds(128 * gg, 128, 128)]

            up, down, far = (g + 1) % 4, (g + 3) % 4, (g + 2) % 4

            def pass_held(gg, part, h, r_id, to):
                send(held(gg, part, h), held(gg, part, h), gid_s, gid + r_id, dev(p, to))

            for h in range(4):
                pass_held(g, 0, h, h, up)
                pass_held(g, 1, h, 4 + h, down)
            pass_held(g, 1, None, 8, up)
            pass_held(g, 0, None, 9, down)
            for h in range(4):
                arrived(held(down, 0, h), gid + h)
                pass_held(down, 0, h, 10, up)
                arrived(held(up, 1, h), gid + 4 + h)
                pass_held(up, 1, h, 11, down)
            arrived(held(down, 1), gid + 8)
            arrived(held(up, 0), gid + 9)
            arrived(held(far, 0), gid + 10)
            arrived(held(far, 1), gid + 11)
            sent(hh.at[:, 0:3], gid_s)

            mark("g_right")
            def put_model(col, a, b):
                mb[0, :, col : col + 256] = a.astype(BF)
                mb[1, :, col : col + 256] = b.astype(BF)

            inverse(lambda r: hh[:, r].reshape(256, QUARTER), 128, put_model)

            mark("misfit")
            squares = 0.0
            for n in range(2):
                rows = mb[...].reshape(256, N)
                some = pl.ds(n * 256, 256)
                a, b = dot(rows, tf[0, :, some]), dot(rows, tf[1, :, some])
                pr, pi = a[:128] - b[128:], b[:128] + a[128:]
                here = ds(512 * g + n * 256, 256, 256)
                mr = tf[0, own_rows, some].astype(F32) - mb[0, :, here].astype(F32)
                mi = tf[1, own_rows, some].astype(F32) - mb[1, :, here].astype(F32)
                mr = mr + (wr * pr - wi * pi)
                mi = mi + (wr * pi + wi * pr)
                squares = squares + jnp.sum(mr * mr + mi * mi)
                mf[0, :, n * 256 : n * 256 + 256] = mr.astype(BF)
                mf[1, :, n * 256 : n * 256 + 256] = mi.astype(BF)

        if it:
            mark("back")

            @pl.loop(0, 4)
            def _(n):
                back_rows(n)

        mine = ds(512 * g, 512, 512)
        for part in range(2):
            pg[part, mine, :] = pg[part, mine, :] + mf[part].astype(F32).T

        mark("f_right")
        quarters(
            lambda part, q: pg[part, q * QUARTER : q * QUARTER + QUARTER, :],
            lambda r, part: ubt.at[r, :, pl.ds(128 * part, 128)],
        )
        up, down, far = (g + 1) % 4, (g + 3) % 4, (g + 2) % 4
        rid, rid_s = ids(10), out_id()

        def piece(ref, gg, part, r=None):
            which = slice(None) if r is None else pl.ds(r, 1)
            return ref.at[it, part, which, ds(128 * gg, 128, 128), :]

        for r in range(4):
            there = pl.ds(r * QUARTER, QUARTER)
            a, b = dot(inv_c[there, :], ubt[r]), dot(inv_s[there, :], ubt[r])
            tr_, ti_ = a[:, :128] + b[:, 128:], a[:, 128:] - b[:, :128]
            tp[0, r] = tr_
            tp[1, r] = ti_
            sb[it, 0, r] = tr_.astype(BF)
            sb[it, 1, r] = ti_.astype(BF)
            send(piece(sb, far, 0, r), ra.at[it, pl.ds(r, 1)], rid_s, rid + r, dev(p, up))
            send(piece(sb, far, 1, r), rb.at[it, pl.ds(r, 1)], rid_s, rid + 4 + r, dev(p, down))

        mark("scatter")
        send(piece(sb, up, 1), dl.at[it, 1], rid_s, rid + 8, dev(p, up))
        send(piece(sb, down, 0), dr.at[it, 0], rid_s, rid + 9, dev(p, down))
        for r in range(4):
            one = pl.ds(r, 1)
            arrived(ra.at[it, one], rid + r)
            qa[it, r] = (tp[0, r, ds(128 * up, 128, 128), :] + ra[it, r].astype(F32)).astype(BF)
            send(qa.at[it, one], dl.at[it, 0, one], rid_s, rid + 8, dev(p, up))
            arrived(rb.at[it, one], rid + 4 + r)
            qb[it, r] = (tp[1, r, ds(128 * down, 128, 128), :] + rb[it, r].astype(F32)).astype(BF)
            send(qb.at[it, one], dr.at[it, 1, one], rid_s, rid + 9, dev(p, down))
        arrived(dl.at[it], rid + 8)
        arrived(dr.at[it], rid + 9)
        sent(sb.at[it, :, 0:3], rid_s)
        total = tp[:, :, ds(128 * g, 128, 128), :] + dl[it].astype(F32)
        zt[it] = (total + dr[it].astype(F32)).astype(BF)
        mark("f_plane")
        xid, xid_s = ids(1), out_id()
        src_of = lambda q: residue(zt.at[it], q)
        dst_of = lambda q: xt.at[it, :, :, ds(128 * q, 128, 128)]
        plane_exchange(src_of, dst_of, xid, xid_s)
        dst_of(p)[...] = src_of(p)[...]
        plane_wait(xt.at[it, :, :, 0:1920], xid, xid_s)

        mark("f_left")
        peaks = []

        def put_trial(r, a, b):
            a, b = STEP * a, STEP * b
            if it:
                a, b = trial[0, r] + a, trial[1, r] + b
            trial[0, r] = a
            trial[1, r] = b
            v = a * a + b * b
            v = jnp.maximum(jnp.maximum(v[:, :128], v[:, 128:256]), jnp.maximum(v[:, 256:384], v[:, 384:]))
            peaks.append(v)

        forward(lambda part, q: xt[it, part, :, q * QUARTER : q * QUARTER + QUARTER].astype(F32), put_trial)
        peak = jnp.maximum(jnp.maximum(peaks[0], peaks[1]), jnp.maximum(peaks[2], peaks[3]))
        peak = jnp.max(jnp.sqrt(peak))

        mark("stats")
        lane = lax.broadcasted_iota(jnp.int32, (1, 128), 1)
        st1[it] = jnp.where(lane < 64, peak, squares)
        sid, sid_s = ids(1), out_id()
        for k, (a, b, d) in enumerate(everyone):
            send(st1.at[it], sr1.at[it, k], sid_s, sid, dev(place(a, b), (g + d) % 4))
        sr1[it, 63] = st1[it]
        if it:
            mark("out_send")
            oid, oid_s = ids(1), out_id()
            away = jnp.logical_and(c == 1, x != y)
            out_src = lambda q: cfo.at[:, :, ds(128 * q, 128, 128)]
            out_dst = lambda q: ot.at[:, q]

            def out_copy(q):
                return rcopy(out_src(q), out_dst(p), oid_s, oid, chip(q // 4, q % 4, g, c))

            order = perm[...]
            for dz in (2, 1, 3, 0):
                b = (z + dz) % 4
                part_of = lambda part, r: trial[part, r, :, ds(128 * b, 128, 128)]
                v = [jnp.concatenate([part_of(part, r) for r in range(4)], axis=1) for part in range(2)]
                v = jnp.concatenate(v, axis=0)
                hi = v.astype(BF)
                rest = v - hi.astype(F32)
                mid = rest.astype(BF)
                low = (rest - mid.astype(F32)).astype(BF)
                v = dot(hi, order) + dot(mid, order) + dot(low, order)
                cfo[0, :, ds(512 * b, 512, 512)] = v[:32]
                cfo[1, :, ds(512 * b, 512, 512)] = v[32:]
                for dx in (2, 1, 3, 0):
                    if dz or dx:
                        out_copy(place(dz, dx)).start()

            @pl.when(away)
            def _():
                out_copy(p).start()

            @pl.when(jnp.logical_not(away))
            def _():
                out_dst(p)[...] = out_src(p)[...]

            mark("stats_wait")
        plane_wait(sr1.at[it, 0:63], sid, sid_s)
        found = sr1[it]
        both = jnp.where(lane < 64, jnp.max(found, axis=0), jnp.sum(found, axis=0))
        totals.append(jnp.max(jnp.where(lane < 64, 0.0, both)))
        mark("shrink")
        level = SHRINK * jnp.max(jnp.where(lane < 64, both, 0.0))

        def shrunk(a, b):
            size = jnp.sqrt(a * a + b * b)
            factor = jnp.maximum(1.0 - level / jnp.maximum(size, level), 0.0)
            return a * factor, b * factor

        if it == 0:
            for r in range(4):
                a, b = shrunk(trial[0, r], trial[1, r])
                trial[0, r] = a
                trial[1, r] = b
                cb[0, r] = a.astype(BF)
                cb[1, r] = b.astype(BF)

    mark("out_wait")
    nid, nid_s = ids(1), out_id()
    for it in range(2):
        nt[it] = jnp.sqrt(jnp.full((1, 128), totals[it], F32))
    send(nt, nr, nid_s, nid, partner)

    @pl.when(away)
    def _():
        rcopy(ot, ot, oid_s, oid, partner).wait_recv()

    @pl.when(jnp.logical_not(away))
    def _():
        rcopy(ot.at[:, 0:15], ot.at[:, 0:15], oid_s, oid, partner).wait_recv()

    mark("out_turn")
    for b in range(4):
        for r in range(4):
            a, d = shrunk(ot[0, 4 * b + r], ot[1, 4 * b + r])
            nat[0, b, pl.ds(r, 32, stride=4), :] = a
            nat[1, b, pl.ds(r, 32, stride=4), :] = d
    halves, halves_s = ids(1), out_id()

    def turned(part, half):
        return jnp.concatenate([nat[part, 2 * half + k].T for k in range(2)], axis=1)

    for part in range(2):
        keep[part] = turned(part, 1 - c)
        send(keep.at[part], got.at[part], halves_s, halves, partner)
    for part in range(2):
        out[c, part] = turned(part, c)
    mark("out_swap")
    arrived(nr, nid)
    for it in range(2):
        norms[it, c] = jnp.max(nt[it])
        norms[it, 1 - c] = jnp.max(nr[it])
    arrived(got, halves)
    out[1 - c] = got[...]
    for copy in pending:
        copy.wait_send()
    rcopy(nt, nt, nid_s, nid, partner).wait_send()
    rcopy(keep, keep, halves_s, halves, partner).wait_send()

    @pl.when(away)
    def _():
        rcopy(ot, ot, oid_s, oid, partner).wait_send()

    @pl.when(jnp.logical_not(away))
    def _():
        rcopy(ot.at[:, 0:15], ot.at[:, 0:15], oid_s, oid, partner).wait_send()

    @pl.when(jnp.logical_not(stays))
    def _():
        to_second.wait_send()

    @pl.when(c == 1)
    def _():
        to_first.wait_send()

    assert used == [RECEIVES, SENDS], used
    mark(None)


def scratch():
    v = lambda *shape, t=BF: pltpu.VMEM(shape, t)
    return [
        v(2, 2, 128, 256), *[v(*a.shape, t=F32) for a in table_parts()],
        v(2, N, 512), v(QUARTER, N), v(QUARTER, N), v(N, QUARTER), v(N, QUARTER), v(512, 512),
        v(2, N, 128, t=F32), v(4, QUARTER, 256), v(2, 4, QUARTER, 128, t=F32),
        v(2, 2, 4, QUARTER, 128), v(2, 4, 128, 128), v(2, 4, 128, 128), v(2, 4, 128, 128),
        v(2, 4, 128, 128), v(2, 2, 4, 128, 128), v(2, 2, 4, 128, 128), v(4, 2, 32, QUARTER),
        v(2, 2, 4, 128, 128), v(2, 2, 32, N),
        v(2, 4, 32, QUARTER, t=F32), v(2, 32, N, t=F32), v(2, 4, 32, QUARTER),
        v(2, 32, N), v(2, 4, 128, 128), v(2, 4, 128, QUARTER), v(2, 128, N), v(2, 128, 512),
        v(2, 16, 32, 128, t=F32), v(2, 4, 128, 128, t=F32),
        v(2, 128, 256, t=F32), v(2, 128, 256, t=F32),
        v(2, 1, 128, t=F32), v(2, 64, 1, 128, t=F32),
        v(2, 1, 128, t=F32), v(2, 1, 128, t=F32),
        pltpu.SemaphoreType.DMA((SENDS,)), pltpu.SemaphoreType.DMA((RECEIVES,)),
        pltpu.SemaphoreType.DMA((9,)),
    ]


def hand_on(a, b, out, norms):
    out[...] = a[...]
    for i in range(2):
        for j in range(2):
            norms[i, j] = b[i, j]


def per_device(traces, wavelet):
    vm = pl.BlockSpec(memory_space=pltpu.VMEM)
    sm = pl.BlockSpec(memory_space=pltpu.SMEM)
    hbm = pl.BlockSpec(memory_space=pl.ANY)
    block = pl.BlockSpec((1, 2, 128, 256), lambda i: (i, 0, 0, 0))
    shapes = (jax.ShapeDtypeStruct((2, 2, 128, 256), F32), jax.ShapeDtypeStruct((2, 2), F32))
    parts = pl.pallas_call(
        kernel,
        out_shape=shapes,
        in_specs=[hbm, sm] + [hbm] * 8,
        out_specs=(vm, sm),
        scratch_shapes=scratch(),
        compiler_params=pltpu.CompilerParams(
            collective_id=0, has_side_effects=True, vmem_limit_bytes=60 * 1024 * 1024
        ),
        name="whole",
    )(traces, wavelet, *table_parts())
    return pl.pallas_call(
        hand_on, out_shape=shapes, grid=(2,), in_specs=[block, sm], out_specs=(block, sm), name="hand_on"
    )(*parts)


def solution(mesh):
    return jax.shard_map(
        per_device,
        mesh=mesh,
        in_specs=(P(None, None, "src", "rcv"), P()),
        out_specs=(P(None, None, "src", "rcv"), P()),
        check_vma=False,
    )
```
